128 devices in a mesh: dp: 8 (over y, core), seq: 16 (over x, z).
Axes of the slice: x: 4, y: 4, z: 4, core: 2. Of those that a mesh axis runs over, the one named last changes fastest.
Arguments:
- head_inputs: bfloat16 [8, 6144, 1024], P('dp', 'seq'), may hold values from -6 to 6
- gate_inputs: bfloat16 [8, 6144, 1024], P('dp', 'seq'), may hold values from -6 to 6
- state_proj: bfloat16 [8, 6144, 256], P('dp', 'seq'), may hold values from -2 to 2
- time_steps: float32 [8, 6144, 16], P('dp', 'seq'), may hold values from -4.7 to 4.7
- token_ids: int32 [8, 6144], P('dp', 'seq'), may hold values from 0 to 50279, as said below
- token_counts: int32 [8], replicated, may hold values from 3072 to 6144
- teacher_out: bfloat16 [8, 6144, 1024], P('dp', 'seq'), may hold values from -6 to 6
- out_weight: float32 [1024, 1024], P(('dp', 'seq')), may hold values from -0.1875 to 0.1875
- decay_log: float32 [16], replicated, may hold values from -6.5 to 1
- step_bias: float32 [16], replicated, may hold values from -5 to -3
- skip_gain: float32 [16], replicated, may hold values from 0.5 to 1.5
- norm_gain: float32 [1024], replicated, may hold values from 0.5 to 1.5
Outputs:
- losses: float32 [2], replicated
- new_weight: float32 [1024, 1024], P(('dp', 'seq'))
- new_decay: float32 [16], replicated
- new_bias: float32 [16], replicated
- new_skip: float32 [16], replicated
- new_gain: float32 [1024], replicated
The draws below stay inside these ranges and needn't reach their ends.
Inputs may be any that keep to these rules, and one draw needn't show every extreme that they name: `token_ids`: in each sequence exactly one position, never the first, holds id 0.
All inputs are finite; a program needn't handle non-finite values.
Results may differ from the reference program's by a relative error of at most 0.0003.
Values may be sent and summed in bfloat16 or wider, within the bound.
A program may use at most 192 MiB of HBM per device.

```python
import jax
import jax.numpy as jnp
from jax import lax

D = 1024
N = 128
VOCAB = 50280
H = 16
STEPS = 2
TOK_DEV = 384
SEQS = 8
LENGTH = 6144
DI = 1024
N_SEQ = 16


def draw_time_steps(key, part):
    noise_key, shift_key = jax.random.split(key)
    blocks = LENGTH // TOK_DEV
    offset = jax.random.uniform(shift_key, (SEQS, blocks, 1, H), jnp.float32, -0.7, 0.7)
    jitter = jnp.clip(jax.random.normal(noise_key, (SEQS, blocks, TOK_DEV, H), jnp.float32), -4.0, 4.0)
    return (jitter + offset).reshape(SEQS, LENGTH, H)


def draw_decay_log(key, part):
    pick_key, strong_key, weak_key = jax.random.split(key, 3)
    strong = jax.random.randint(pick_key, (H,), 0, 2) > 0
    slow_rate = jax.random.uniform(strong_key, (H,), jnp.float32, -6.5, -5.5)
    quick_rate = jax.random.uniform(weak_key, (H,), jnp.float32, 0.0, 1.0)
    return jnp.where(strong, slow_rate, quick_rate)


def draw_token_ids(key, part):
    token_key, reset_key = jax.random.split(key)
    token_draw = jax.random.randint(token_key, (SEQS, LENGTH), 1, VOCAB)
    reset_at = jax.random.randint(reset_key, (SEQS, 1), 1, LENGTH)
    return jnp.where(jnp.arange(LENGTH)[None, :] == reset_at, 0, token_draw).astype(jnp.int32)


def plant(drawn, stream_key, low, largest):
    place = [jax.random.randint(jax.random.fold_in(stream_key, axis), (), 0, length) for axis, length in enumerate(drawn.shape)]
    main_axis = drawn.shape.index(max(drawn.shape))
    beside = place[:main_axis] + [(place[main_axis] + 1) % drawn.shape[main_axis]] + place[main_axis + 1:]
    return drawn.at[tuple(place)].set(low).at[tuple(beside)].set(largest)


def spiked(result, own_key, source, target, parts, factor):
    owner, partner = [(jnp.arange(result.shape[axis_at]) // (result.shape[axis_at] // parts)).reshape([-1 if axis == axis_at else 1 for axis in range(result.ndim)]) for axis_at in (source, target)]
    chosen = jax.random.permutation(own_key, parts)[partner]
    strong = (owner == chosen) | (owner == (partner + parts // 2) % parts)
    return jnp.where(strong, factor * result, result)


def steps_of(own_key, dims, cuts, least, high):
    factor_of, own = 1.0, jax.random.fold_in(own_key, 6)
    for axis_at, blocks in cuts:
        steps = jnp.exp(jax.random.uniform(jax.random.fold_in(own, axis_at), (blocks,), jnp.float32, least / len(cuts), high / len(cuts)))
        factor_of = factor_of * jnp.repeat(steps, dims[axis_at] // blocks).reshape([-1 if axis == axis_at else 1 for axis in range(len(dims))])
    return factor_of


def scatter_about(stream_key, shape, scale, reach, cuts=(), kind=jnp.bfloat16):
    result = jax.random.normal(stream_key, shape, jnp.float32) * scale
    if len(cuts) > 0:
        result = steps_of(stream_key, shape, cuts, -0.22, 0.18) * result
    return jnp.clip(result, min=-reach, max=reach).astype(kind)


def gaussian_with(key, dims, scale, bound, cuts, heavy, dtype=jnp.bfloat16):
    entries = scale * jax.random.normal(key, dims, jnp.float32)
    if cuts:
        entries = entries * steps_of(key, dims, cuts, -0.22, 0.18)
    return jnp.clip(spiked(entries, jax.random.fold_in(key, 3), *heavy), -bound, bound).astype(dtype)


def setup_inputs(seed: int = 0) -> dict:
    arg_keys = jax.random.split(jax.random.key(seed), 13)
    return {
        "head_inputs": scatter_about(arg_keys[0], (SEQS, LENGTH, DI), 1.0, 6.0, ((0, 8), (1, 16))),
        "gate_inputs": gaussian_with(arg_keys[1], (SEQS, LENGTH, DI), 1.0, 6.0, ((0, 8), (1, 16)), (1, 2, 16, 2.0)),
        "state_proj": scatter_about(arg_keys[2], (SEQS, LENGTH, 2 * N), 0.3, 2.0, ((0, 8), (1, 16))),
        "time_steps": draw_time_steps(jax.random.fold_in(arg_keys[12], 71), 0),
        "token_ids": draw_token_ids(jax.random.fold_in(arg_keys[12], 71), 0),
        "token_counts": plant(jax.random.randint(arg_keys[5], (SEQS,), LENGTH // 2, LENGTH + 1), jax.random.fold_in(arg_keys[5], 1), LENGTH // 2, LENGTH).astype(jnp.int32),
        "teacher_out": scatter_about(arg_keys[6], (SEQS, LENGTH, D), 1.0, 6.0, ((0, 8), (1, 16))),
        "out_weight": scatter_about(arg_keys[7], (DI, D), DI ** -0.5, 0.1875, ((0, 128),), jnp.float32),
        "decay_log": draw_decay_log(jax.random.fold_in(arg_keys[12], 71), 0),
        "step_bias": jnp.clip(jax.random.uniform(arg_keys[9], (H,), jnp.float32, -5.0, -3.0), -5.0, -3.0),
        "skip_gain": jnp.clip(jax.random.uniform(arg_keys[10], (H,), jnp.float32, 0.5, 1.5), 0.5, 1.5),
        "norm_gain": jnp.clip(1.0 + 0.1 * jax.random.normal(arg_keys[11], (DI,), jnp.float32), 0.5, 1.5),
    }


norm_floor = 1.0
clip_limit = 1.0
learn_rate = 8.0
highest = lax.Precision.HIGHEST
masked_low = -10000.0

def step_sizes(decay_log, step_bias, step_raw):
    step_width = jax.nn.softplus(step_raw + step_bias[None, :])
    decay_sum = jnp.cumsum(step_width * (-jnp.exp(decay_log))[None, :], axis=0)
    return (step_width, decay_sum)

def mix_block(decay_log, step_bias, skip_gain, norm_gain, state_in, head_inputs, gate_inputs, b_proj, c_proj, step_raw, segment):
    positions = head_inputs.shape[0]
    head_count = decay_log.shape[0]
    step_width, decay_sum = step_sizes(decay_log, step_bias, step_raw)
    inputs_f = head_inputs.astype(jnp.float32).reshape(positions, head_count, -1)
    scaled = inputs_f * step_width[:, :, None]
    scores = jnp.dot(c_proj, b_proj.T, preferred_element_type=jnp.float32)
    position = jnp.arange(positions)
    allowed = (segment[:, None] == segment[None, :]) & (position[:, None] >= position[None, :])

    def one_head(head_data):
        head_sum, head_scaled = head_data
        spread = head_sum[:, None] - head_sum[None, :]
        decay_grid = jnp.exp(jnp.where(allowed, spread, masked_low))
        return jnp.dot(decay_grid * scores, head_scaled, precision=highest)
    intra_sum = jnp.transpose(lax.map(one_head, (decay_sum.T, jnp.transpose(scaled, (1, 0, 2)))), (1, 0, 2))
    entry_decay = jnp.exp(decay_sum) * (segment == 0)[:, None]
    carried = jnp.einsum('in,hpn->ihp', c_proj.astype(jnp.float32), state_in, precision=highest) * entry_decay[:, :, None]
    mixed_out = intra_sum + carried + skip_gain[None, :, None] * inputs_f
    gated = mixed_out.reshape(positions, -1) * jax.nn.silu(gate_inputs.astype(jnp.float32))
    mean_square = lax.optimization_barrier(jnp.mean(gated * gated, axis=1, keepdims=True))
    return gated * norm_gain[None, :] * lax.rsqrt(mean_square + norm_floor)

def state_block(decay_log, step_bias, head_inputs, b_proj, step_raw, segment):
    positions = head_inputs.shape[0]
    head_count = decay_log.shape[0]
    step_width, decay_sum = step_sizes(decay_log, step_bias, step_raw)
    final_sum = decay_sum[-1]
    same_doc = (segment == segment[-1])[:, None]
    tail_decay = jnp.exp(jnp.where(same_doc, final_sum[None, :] - decay_sum, masked_low))
    inputs_f = head_inputs.astype(jnp.float32).reshape(positions, head_count, -1)
    weighted = inputs_f * (step_width * tail_decay)[:, :, None]
    state_out = jnp.einsum('jhp,jn->hpn', weighted, b_proj.astype(jnp.float32), precision=highest)
    carry_out = jnp.exp(final_sum) * (segment[-1] == 0)
    return (carry_out, state_out)

def kahan_total(partials):

    def add_one(running, element):
        summed_up, correction = running
        adjusted = element - correction
        new_total = summed_up + adjusted
        correction = new_total - summed_up - adjusted
        return ((new_total, correction), None)
    (summed_up, correction), _ = lax.scan(add_one, (jnp.zeros((), jnp.float32), jnp.zeros((), jnp.float32)), partials)
    return summed_up

def reference(head_inputs, gate_inputs, state_proj, time_steps, token_ids, token_counts, teacher_out, out_weight, decay_log, step_bias, skip_gain, norm_gain):
    seq_count, length, inner_width = head_inputs.shape
    state_size = state_proj.shape[2] // 2
    model_width = teacher_out.shape[2]
    blocks = N_SEQ
    block_len = length // blocks
    head_count = decay_log.shape[0]
    head_size = inner_width // head_count

    def split_blocks(array):
        return array.reshape((seq_count, blocks, block_len) + array.shape[2:])
    starts = (token_ids == 0).astype(jnp.int32)
    segments = jnp.cumsum(split_blocks(starts), axis=2).astype(jnp.int32)
    position = jnp.arange(length).astype(jnp.int32)
    scored_all = (position[None, :] < token_counts[:, None]).astype(jnp.float32)
    total_count = jnp.sum(token_counts).astype(jnp.float32)
    pieces = (split_blocks(head_inputs), split_blocks(gate_inputs), split_blocks(state_proj), split_blocks(time_steps), segments)
    losses = []
    for step_index in range(STEPS):
        weight_b = out_weight.astype(jnp.bfloat16)
        params = (decay_log, step_bias, skip_gain, norm_gain)

        def one_sequence(running, seq_data):
            sequence, target_s, scored_s = seq_data

            def forward(params_in):

                def per_block(state_in, block_data):
                    inputs_b, gates_b, proj_b, raw_b, seg_b = block_data
                    normed_blk = mix_block(params_in[0], params_in[1], params_in[2], params_in[3], state_in, inputs_b, gates_b, proj_b[:, :state_size], proj_b[:, state_size:], raw_b, seg_b)
                    carry_out, state_out = state_block(params_in[0], params_in[1], inputs_b, proj_b[:, :state_size], raw_b, seg_b)
                    return (carry_out[:, None, None] * state_in + state_out, normed_blk)
                start_state = jnp.zeros((head_count, head_size, state_size), jnp.float32)
                _, normed_seq = lax.scan(jax.checkpoint(per_block), start_state, sequence)
                return normed_seq
            normed, pull_back = jax.vjp(forward, params)
            normed_b = normed.astype(jnp.bfloat16).reshape(-1, inner_width)
            output = jnp.dot(normed_b, weight_b, preferred_element_type=jnp.float32)
            residual = output - target_s.astype(jnp.float32)
            token_loss = lax.optimization_barrier(jnp.sum(residual * residual, axis=1)) * scored_s / model_width
            block_sums = lax.optimization_barrier(jnp.sum(token_loss.reshape(blocks, block_len), axis=1))
            out_grad = (residual * (2.0 / (model_width * total_count)) * scored_s[:, None]).astype(jnp.bfloat16)
            weight_part = jnp.dot(normed_b.T, out_grad, preferred_element_type=jnp.float32)
            normed_grad = jnp.dot(out_grad, weight_b.T, preferred_element_type=jnp.float32).reshape(normed.shape)
            small_part, = pull_back(normed_grad)
            new_running = (running[0] + weight_part, tuple((left + right for left, right in zip(running[1], small_part))))
            return (new_running, block_sums)
        start_running = (jnp.zeros(out_weight.shape, jnp.float32), tuple((jnp.zeros(member.shape, jnp.float32) for member in params)))
        (weight_grad, small_grads), partial_sums = lax.scan(one_sequence, start_running, (pieces, teacher_out, scored_all))
        losses.append(kahan_total(partial_sums.reshape(-1)) / total_count)
        norm_square = jnp.sum(weight_grad * weight_grad) + sum((jnp.sum(member * member) for member in small_grads))
        factor = clip_limit / jnp.maximum(jnp.sqrt(norm_square), clip_limit)
        out_weight = out_weight - learn_rate * factor * weight_grad
        decay_log = decay_log - learn_rate * factor * small_grads[0]
        step_bias = step_bias - learn_rate * factor * small_grads[1]
        skip_gain = skip_gain - learn_rate * factor * small_grads[2]
        norm_gain = norm_gain - learn_rate * factor * small_grads[3]
    return (jnp.stack(losses), out_weight, decay_log, step_bias, skip_gain, norm_gain)
```

```python
import jax
import jax.numpy as jnp
from jax import lax
from jax.experimental import pallas as pl
from jax.experimental.pallas import tpu as pltpu
from jax.sharding import PartitionSpec as P

STEPS = 2
DP, SEQ = "dp", "seq"
N_DP, N_SEQ, N_Y = 8, 16, 4
TOK, WIDE, STATE, HEADS, HEAD = 384, 1024, 128, 16, 64
CHUNK, CHUNKS, PAIRS = 128, 3, 8
HALF = WIDE // 2

norm_floor = 1.0
clip_limit = 1.0
learn_rate = 8.0
f32, bf16 = jnp.float32, jnp.bfloat16
highest = lax.Precision.HIGHEST


def dot(a, b):
    return jnp.dot(a, b, preferred_element_type=f32)


def dot_tn(a, b):
    return lax.dot_general(a, b, (((0,), (0,)), ((), ())), preferred_element_type=f32)


def dot_nt(a, b):
    return lax.dot_general(a, b, (((1,), (1,)), ((), ())), preferred_element_type=f32)


def iota(shape, dim):
    return lax.broadcasted_iota(jnp.int32, shape, dim)


def three_parts(v):
    high = v.astype(bf16).astype(f32)
    rest = v - high
    mid = rest.astype(bf16).astype(f32)
    low = rest - mid
    group = (iota(v.shape, 1) >> 4) & 3
    zero = jnp.zeros_like(v)
    return jnp.where(
        group == 0, high, jnp.where(group == 1, mid, jnp.where(group == 2, low, zero))
    ).astype(bf16)


def blocks_of(rows):
    left = rows[:, :HALF].reshape(N_SEQ, 1, 8, HALF)
    right = rows[:, HALF:].reshape(N_SEQ, 1, 8, HALF)
    return jnp.concatenate([left, right], axis=1).reshape(N_SEQ, 16, HALF)


def rows_of(blocks):
    count = blocks.shape[0]
    split = blocks.reshape(count, 2, 8, HALF)
    return split[:, 0].reshape(count * 8, HALF), split[:, 1].reshape(count * 8, HALF)


def kernel(
    x_ref, z_ref, bc_ref, raw_ref, ids_ref, cnt_ref, tgt_ref, w_ref, dec_in, bias_in, skip_in, gain_in,
    loss_out, w_out, dec_out, bias_out, skip_out, gain_out,
    ex, red, tri, par, gain, wown,
    rawt, wid, dec_s, ent, tail, chain, fcol, sc,
    xw, yin, eexp, silu, gstate, hst, apart, normb, ogb, gb, zin, ds1, accs,
    hs, hr, hp, hi, gs, gr, gp, gi, cs, cr,
    agb, wfull, wgp, pr, sb, rb,
    sa, sar, sb2, sbr, ta, tar, tb, tbr,
    s_send, s_recv, s_ag, s_agr, s_fs, s_fr, s_ps, s_pr, s_rs, s_rr,
):
    dp, seq = lax.axis_index(DP), lax.axis_index(SEQ)
    yy, core = dp // 2, dp % 2
    partner = dp + 1 - 2 * core
    own_q = yy * N_SEQ + seq
    own_b = dp * N_SEQ + seq
    MESH = pl.DeviceIdType.MESH

    def at(d, s):
        return {DP: d, SEQ: s}

    def remote(src, dst, ss, rs, d, s):
        return pltpu.make_async_remote_copy(
            src_ref=src, dst_ref=dst, send_sem=ss, recv_sem=rs, device_id=at(d, s), device_id_type=MESH
        )

    barrier = pltpu.get_barrier_semaphore()

    def greet_same(k, carry):
        q = (own_q + k) % 64
        pl.semaphore_signal(barrier, 1, device_id=at((q // 16) * 2 + core, q % 16), device_id_type=MESH)
        return carry

    lax.fori_loop(1, 64, greet_same, 0)

    def greet_other(k, carry):
        pl.semaphore_signal(barrier, 1, device_id=at(k * 2 + 1 - core, seq), device_id_type=MESH)
        return carry

    lax.fori_loop(0, N_Y, greet_other, 0)

    row = iota((CHUNK, WIDE), 0)
    col = iota((CHUNK, WIDE), 1)
    ex[...] = jnp.where(((row & 15) == (col >> 6)) & (row < 48), 1.0, 0.0).astype(bf16)
    rrow = iota((WIDE, 128), 0)
    rcol = iota((WIDE, 128), 1)
    red[...] = jnp.where((rrow >> 6) == (rcol & 15), 1.0, 0.0).astype(bf16)
    ti, tj = iota((CHUNK, CHUNK), 0), iota((CHUNK, CHUNK), 1)
    tri[...] = jnp.where(ti >= tj, 1.0, 0.0)
    rep = jnp.where(iota((HEADS, 128), 0) == (iota((HEADS, 128), 1) & 15), 1.0, 0.0)

    def tiled(ref):
        return jnp.dot(jnp.broadcast_to(ref[...], (8, HEADS)), rep, precision=highest, preferred_element_type=f32)

    par[0] = tiled(dec_in)
    par[1] = tiled(bias_in)
    par[2] = tiled(skip_in)
    gain[...] = gain_in[...]
    wown[...] = w_ref[...]
    rawt[...] = jnp.dot(raw_ref[...], rep, precision=highest, preferred_element_type=f32)

    def expand(v):
        return dot(three_parts(v), ex[...])

    def head_sum(v):
        high = v.astype(bf16)
        low = (v - high.astype(f32)).astype(bf16)
        return dot(high, red[...]) + dot(low, red[...])

    lane = iota((1, 128), 1)
    low_half = jnp.where(lane < HEAD, 1.0, 0.0).astype(bf16)
    high_half = jnp.where(lane < HEAD, 0.0, 1.0).astype(bf16)

    total = cnt_ref[0]
    for k in range(1, N_DP):
        total = total + cnt_ref[k]
    total_f = total.astype(f32)
    own_count = cnt_ref[dp]

    def rows(c):
        return pl.ds(pl.multiple_of(c * CHUNK, CHUNK), CHUNK)

    def prepare(c, carry):
        flag = jnp.where(ids_ref[0:1, rows(c)] == 0, 1.0, 0.0)
        flag_col = jnp.broadcast_to(flag, (CHUNK, CHUNK)).T
        seg = dot(tri[...], flag_col)
        seg_row = seg.T
        fcol[c] = seg
        scores = dot_nt(bc_ref[rows(c), STATE:], bc_ref[rows(c), :STATE])
        sc[c] = jnp.where((seg == seg_row) & (ti >= tj), scores, 0.0)
        return carry

    lax.fori_loop(0, CHUNKS, prepare, 0)

    def ag_start():
        block = jnp.concatenate([wown[:, :HALF], wown[:, HALF:]], axis=0).astype(bf16)
        agb[own_b] = block

        def send(k, carry):
            q = (own_q + k) % 64
            remote(agb.at[own_b], agb.at[own_b], s_ag, s_agr.at[yy], (q // 16) * 2 + core, q % 16).start()
            return carry

        lax.fori_loop(1, 64, send, 0)

    def ag_finish():
        copies = []
        for k in range(N_Y):
            y_k = (yy + k) % N_Y
            first = (y_k * 2 + core) * N_SEQ
            count = 15 if k == 0 else 16
            piece = agb.at[pl.ds(first, count)]
            remote(piece, piece, s_ag, s_agr.at[y_k], partner, seq).wait_recv()
            whole = agb.at[pl.ds(first, N_SEQ)]
            copy = remote(whole, whole, s_fs.at[k], s_fr.at[k], partner, seq)
            copy.start()
            copies.append(copy)
        for k in range(N_Y):
            y_k = (yy + k) % N_Y
            other = (y_k * 2 + 1 - core) * N_SEQ
            piece = agb.at[pl.ds(other, N_SEQ)]
            remote(piece, piece, s_fs.at[k], s_fr.at[k], partner, seq).wait_recv()
        sent = agb.at[pl.ds(0, 63)]
        remote(sent, sent, s_ag, s_agr.at[0], partner, seq).wait_send()
        for copy in copies:
            copy.wait_send()

        def unpack(d, carry):
            left, right = rows_of(agb[pl.ds(d * N_SEQ, N_SEQ)].astype(f32))
            wfull[rows(d), :HALF] = left.astype(bf16)
            wfull[rows(d), HALF:] = right.astype(bf16)
            return carry

        lax.fori_loop(0, N_DP, unpack, 0)

    def exchange_start(src, dst, n):
        def send(k, carry):
            peer = (seq + k) % N_SEQ
            remote(src.at[peer], dst.at[seq], s_send.at[n], s_recv.at[n], dp, peer).start()
            return carry

        lax.fori_loop(1, N_SEQ, send, 0)
        dst[seq] = src[seq]

    def spread_start(src, dst, n):
        def send(k, carry):
            peer = (seq + k) % N_SEQ
            remote(src, dst.at[seq], s_send.at[n], s_recv.at[n], dp, peer).start()
            return carry

        lax.fori_loop(1, N_SEQ, send, 0)
        dst[seq] = src[...]

    def cross_start(src, dst, n):
        def send(k, carry):
            peer = (dp + k) % N_DP
            remote(src, dst.at[dp], s_send.at[n], s_recv.at[n], peer, seq).start()
            return carry

        lax.fori_loop(1, N_DP, send, 0)
        dst[dp] = src[...]

    def recv_wait(dst, n, count):
        piece = dst.at[pl.ds(0, count)]
        remote(piece, piece, s_send.at[n], s_recv.at[n], partner, seq).wait_recv()

    def send_wait(dst, n, count):
        piece = dst.at[pl.ds(0, count)]
        remote(piece, piece, s_send.at[n], s_recv.at[n], partner, seq).wait_send()

    def one_step(step, losses):
        dec_t, bias_t, skip_t = par[0, 0:1], par[1, 0:1], par[2, 0:1]
        rate = jnp.exp(dec_t)

        hst[0] = jnp.zeros((STATE, WIDE), f32)

        def begin(c, carried):
            seg = fcol[c]
            pre = rawt[rows(c)] + bias_t
            u = jnp.exp(-jnp.abs(pre))
            v = 1.0 + u
            log1p = jnp.where(v == 1.0, u, jnp.log(v) * u / jnp.where(v == 1.0, 1.0, v - 1.0))
            width = jnp.maximum(pre, 0.0) + log1p
            s = jnp.dot(tri[...], -rate * width, precision=highest, preferred_element_type=f32)
            last = s[CHUNK - 1 : CHUNK]
            seg_last = seg[CHUNK - 1 : CHUNK]
            entering = jnp.exp(s) * jnp.where(seg == 0.0, 1.0, 0.0)
            leaving = jnp.exp(last - s) * jnp.where(seg == seg_last, 1.0, 0.0)
            through = jnp.exp(last) * jnp.where(seg_last == 0.0, 1.0, 0.0)
            wid[rows(c)] = width
            dec_s[rows(c)] = s
            tail[rows(c)] = leaving
            eexp[rows(c)] = expand(entering)
            chain[c] = expand(jnp.broadcast_to(through, (8, 128)))
            scaled = x_ref[rows(c)].astype(f32) * expand(width)
            xw[rows(c)] = scaled.astype(bf16)
            weighted = (scaled * expand(leaving)).astype(bf16)
            added = dot_tn(bc_ref[rows(c), :STATE], weighted)
            gstate[c] = added
            hst[0] = chain[c][0:1] * hst[0] + added
            return carried * through

        carried = lax.fori_loop(0, CHUNKS, begin, jnp.ones((1, 128), f32))
        wide8 = jnp.broadcast_to(carried, (8, 128))
        sub8, lane8 = iota((8, 128), 0), iota((8, 128), 1)
        even = jnp.sum(jnp.where(lane8 == 2 * sub8, wide8, 0.0), axis=1, keepdims=True)
        odd = jnp.sum(jnp.where(lane8 == 2 * sub8 + 1, wide8, 0.0), axis=1, keepdims=True)
        cs[...] = jnp.where(lane8 < HEAD, even, odd)

        def to_blocks(state, out):
            for r in range(8):
                for h in range(2):
                    out[2 * r + h] = state[16 * r : 16 * r + 16, HALF * h : HALF * (h + 1)].astype(bf16)

        to_blocks(hst[0], hs)

        @pl.when(step == 0)
        def _():
            pl.semaphore_wait(barrier, 67)

        exchange_start(hs, hr, 0)
        spread_start(cs, cr, 1)

        @pl.when(step == 0)
        def _():
            ag_start()

        def inside(c, carry):
            s = dec_s[rows(c)]
            s_t = s.T
            scores = sc[c]
            for p in range(PAIRS):
                parts = []
                for h in (2 * p, 2 * p + 1):
                    gap = jnp.minimum(s[:, h : h + 1] - s_t[h : h + 1, :], 0.0)
                    parts.append((jnp.exp(gap) * scores).astype(bf16))
                mine = xw[rows(c), 128 * p : 128 * (p + 1)]
                both = jnp.concatenate([mine * low_half, mine * high_half], axis=0)
                yin[rows(c), 128 * p : 128 * (p + 1)] = dot(jnp.concatenate(parts, axis=1), both)
            return carry

        lax.fori_loop(0, CHUNKS, inside, 0)

        half = seq % 2

        def carry_rows(i):
            return [cr[i, pl.ds(4 * half + m, 1), :] for m in range(4)]

        recv_wait(hr, 0, 15)
        recv_wait(cr, 1, 15)

        def forward(i, state):
            factors = carry_rows(i)
            out = []
            for m in range(4):
                lanes = slice(128 * m, 128 * (m + 1))
                hp[i, :, lanes] = state[m].astype(bf16)
                out.append(factors[m] * state[m] + hr[i, :, lanes].astype(f32))
            return tuple(out)

        zeros4 = tuple(jnp.zeros((16, 128), f32) for _ in range(4))
        lax.fori_loop(0, N_SEQ, forward, zeros4)
        exchange_start(hp, hi, 2)
        ag_finish()
        recv_wait(hi, 2, 15)
        for r in range(8):
            for h in range(2):
                hst[0, 16 * r : 16 * r + 16, HALF * h : HALF * (h + 1)] = hi[2 * r + h].astype(f32)

        skip_e = expand(jnp.broadcast_to(skip_t, (8, 128)))[0:1]
        gain_e = gain[...]
        scale = 2.0 / (WIDE * total_f)
        accs[...] = jnp.zeros(accs.shape, f32)

        def mix(c, loss):
            state = hst[c]
            b_c, c_c = bc_ref[rows(c), :STATE], bc_ref[rows(c), STATE:]
            y_sum = yin[rows(c)] + eexp[rows(c)] * dot(c_c, state.astype(bf16))
            x_f = x_ref[rows(c)].astype(f32)
            z_f = z_ref[rows(c)].astype(f32)
            act = z_f / (1.0 + jnp.exp(-z_f))
            gated = (y_sum + skip_e * x_f) * act
            inv = lax.rsqrt(jnp.sum(gated * gated, axis=1, keepdims=True) * (1.0 / WIDE) + norm_floor)
            normed = (gated * gain_e * inv).astype(bf16)
            normb[rows(c)] = normed
            res = dot(normed, wfull[...]) - tgt_ref[rows(c)].astype(f32)
            position = seq * TOK + c * CHUNK + iota((CHUNK, 1), 0)
            scored = jnp.where(position < own_count, 1.0, 0.0)
            loss = loss + jnp.sum(jnp.sum(res * res, axis=1, keepdims=True) * scored, axis=0, keepdims=True)
            og = (res * (scored * scale)).astype(bf16)
            ogb[rows(c)] = og
            d_norm = dot_nt(og, wfull[...])
            d_gr = d_norm * gated * inv
            accs[0] += jnp.sum(d_gr.reshape(16, 8, WIDE), axis=0)
            inner = jnp.sum(d_gr * gain_e, axis=1, keepdims=True) * (1.0 / WIDE)
            d_gated = inv * (gain_e * d_norm - gated * (inv * inner))
            g = d_gated * act
            g_b = g.astype(bf16)
            gb[rows(c)] = g_b
            accs[1] += jnp.sum((g * x_f).reshape(16, 8, WIDE), axis=0)
            ds1[rows(c)] = head_sum(g_b.astype(f32) * y_sum)
            apart[c] = dot_tn(c_c, (g * eexp[rows(c)]).astype(bf16))
            hst[c + 1] = chain[c][0:1] * state + gstate[c]
            return loss

        loss = lax.fori_loop(0, CHUNKS, mix, jnp.zeros((1, 1), f32))
        entry = apart[0] + chain[0][0:1] * (apart[1] + chain[1][0:1] * apart[2])
        to_blocks(entry, gs)
        exchange_start(gs, gr, 3)
        gain_g = jnp.sum(accs[0], axis=0, keepdims=True)
        for r in range(8):
            sa[r : r + 1, :] = gain_g[:, 128 * r : 128 * (r + 1)]
        skip_g = head_sum(jnp.broadcast_to(jnp.sum(accs[1], axis=0, keepdims=True), (8, WIDE)))
        sub = iota((8, 128), 0)
        sa[8:16, :] = jnp.where(sub == 0, skip_g, jnp.where(sub == 1, jnp.broadcast_to(loss, (8, 128)), 0.0))
        spread_start(sa, sar, 4)

        def grad_rows(d):
            lanes = pl.ds(pl.multiple_of(d * 128, 128), 128)
            return blocks_of(dot_tn(normb[:, lanes], ogb[...]))

        for k in range(N_Y):
            y_k = (yy + k) % N_Y
            d = y_k * 2 + 1 - core
            wgp[k] = grad_rows(d).astype(bf16)
            remote(wgp.at[k], pr.at[k], s_ps.at[k], s_pr.at[k], partner, seq).start()
        for k in range(N_Y):
            y_k = (yy + k) % N_Y
            d = y_k * 2 + core
            mine = grad_rows(d)
            remote(wgp.at[k], pr.at[k], s_ps.at[k], s_pr.at[k], partner, seq).wait_recv()
            sb[pl.ds(y_k * N_SEQ, N_SEQ)] = (mine + pr[k].astype(f32)).astype(bf16)

            def send(j, carry):
                s = (seq + j) % N_SEQ
                remote(sb.at[y_k * N_SEQ + s], rb.at[own_q], s_rs, s_rr, d, s).start()
                return carry

            lax.fori_loop(1 if k == 0 else 0, N_SEQ, send, 0)
        rb[own_q] = sb[own_q]

        recv_wait(gr, 3, 15)

        def backward(n, state):
            i = N_SEQ - 1 - n
            factors = carry_rows(i)
            out = []
            for m in range(4):
                lanes = slice(128 * m, 128 * (m + 1))
                gp[i, :, lanes] = state[m].astype(bf16)
                out.append(factors[m] * state[m] + gr[i, :, lanes].astype(f32))
            return tuple(out)

        lax.fori_loop(0, N_SEQ, backward, zeros4)
        exchange_start(gp, gi, 5)

        def inside_back(c, carry):
            s = dec_s[rows(c)]
            s_t = s.T
            scores = sc[c].T
            for p in range(PAIRS):
                parts = []
                for h in (2 * p, 2 * p + 1):
                    gap = jnp.minimum(s_t[h : h + 1, :] - s[:, h : h + 1], 0.0)
                    parts.append((jnp.exp(gap) * scores).astype(bf16))
                mine = gb[rows(c), 128 * p : 128 * (p + 1)]
                both = jnp.concatenate([mine * low_half, mine * high_half], axis=0)
                zin[rows(c), 128 * p : 128 * (p + 1)] = dot(jnp.concatenate(parts, axis=1), both)
            return carry

        lax.fori_loop(0, CHUNKS, inside_back, 0)

        def summed(ref, count):
            value = ref[0]
            for k in range(1, count):
                value = value + ref[k]
            return value

        recv_wait(sar, 4, 15)
        sb2[...] = summed(sar, N_SEQ)
        cross_start(sb2, sbr, 6)

        recv_wait(gi, 5, 15)
        for r in range(8):
            for h in range(2):
                apart[3, 16 * r : 16 * r + 16, HALF * h : HALF * (h + 1)] = gi[2 * r + h].astype(f32)

        def back(n, sums):
            dec_g, bias_g = sums
            c = CHUNKS - 1 - n
            after = apart[3]
            width = wid[rows(c)]
            z_t = dot(bc_ref[rows(c), :STATE], after.astype(bf16))
            z_all = zin[rows(c)] + expand(tail[rows(c)]) * z_t
            q2 = head_sum(xw[rows(c)].astype(f32) * z_all)
            ends = jnp.sum((after * hst[c + 1]).reshape(16, 8, WIDE), axis=0)
            end_h = jnp.sum(head_sum(ends), axis=0, keepdims=True)
            d_s = ds1[rows(c)] - q2
            d_a = lax.dot_general(
                tri[...], d_s, (((0,), (0,)), ((), ())), precision=highest, preferred_element_type=f32
            ) + end_h
            d_w = q2 / width - rate * d_a
            pre = rawt[rows(c)] + bias_t
            sig = 1.0 / (1.0 + jnp.exp(-pre))
            dec_g = dec_g - jnp.sum(d_a * (rate * width), axis=0, keepdims=True)
            bias_g = bias_g + jnp.sum(d_w * sig, axis=0, keepdims=True)
            apart[3] = apart[c] + chain[c][0:1] * after
            return dec_g, bias_g

        zero_row = jnp.zeros((1, 128), f32)
        dec_g, bias_g = lax.fori_loop(0, CHUNKS, back, (zero_row, zero_row))

        recv_wait(sbr, 6, 7)
        sums_a = summed(sbr, N_DP)

        got = rb.at[pl.ds(0, 63)]
        remote(got, got, s_rs, s_rr, partner, seq).wait_recv()

        def add_up(q, value):
            return value + rb[q].astype(f32)

        grad = lax.fori_loop(0, 64, add_up, jnp.zeros((16, HALF), f32))
        square = jnp.sum(jnp.sum(grad * grad, axis=1, keepdims=True), axis=0, keepdims=True)
        ta[...] = jnp.where(
            sub == 0, dec_g, jnp.where(sub == 1, bias_g, jnp.where(sub == 2, jnp.broadcast_to(square, (8, 128)), 0.0))
        )
        spread_start(ta, tar, 7)
        recv_wait(tar, 7, 15)
        tb[...] = summed(tar, N_SEQ)
        cross_start(tb, tbr, 8)
        recv_wait(tbr, 8, 7)
        sums_b = summed(tbr, N_DP)

        dec_g, bias_g, squares = sums_b[0:1], sums_b[1:2], sums_b[2:3]
        gain_rows, skip_g, loss_all = sums_a[0:8], sums_a[8:9], sums_a[9:10]
        small = jnp.sum(
            jnp.where(lane < HEADS, dec_g * dec_g + bias_g * bias_g + skip_g * skip_g, 0.0), axis=1, keepdims=True
        )
        gains = jnp.sum(jnp.sum(gain_rows * gain_rows, axis=1, keepdims=True), axis=0, keepdims=True)
        norm = jnp.sqrt(squares + (small + gains))
        move = learn_rate * (clip_limit / jnp.maximum(norm, clip_limit))
        par[0] = jnp.broadcast_to(dec_t - move * dec_g, (8, 128))
        par[1] = jnp.broadcast_to(bias_t - move * bias_g, (8, 128))
        par[2] = jnp.broadcast_to(skip_t - move * skip_g, (8, 128))
        for r in range(8):
            lanes = slice(128 * r, 128 * (r + 1))
            gain[:, lanes] = gain[:, lanes] - move * gain_rows[r : r + 1]
        move_w = jnp.broadcast_to(move[:, 0:1], (8, HALF))
        wown[:, :HALF] = wown[:, :HALF] - move_w * grad[0:8]
        wown[:, HALF:] = wown[:, HALF:] - move_w * grad[8:16]

        send_wait(hr, 0, 15)
        send_wait(cr, 1, 15)
        send_wait(hi, 2, 15)
        send_wait(gr, 3, 15)
        send_wait(sar, 4, 15)
        send_wait(gi, 5, 15)
        send_wait(sbr, 6, 7)
        send_wait(tar, 7, 15)
        send_wait(tbr, 8, 7)
        for k in range(N_Y):
            remote(wgp.at[k], pr.at[k], s_ps.at[k], s_pr.at[k], partner, seq).wait_send()
        remote(got, got, s_rs, s_rr, partner, seq).wait_send()

        @pl.when(step == 0)
        def _():
            ag_start()

        step_loss = loss_all[:, 0:1] * (1.0 / WIDE) / total_f
        return jnp.where(iota((1, STEPS), 1) == step, step_loss, losses)

    losses = lax.fori_loop(0, STEPS, one_step, jnp.zeros((1, STEPS), f32))
    loss_out[...] = losses
    w_out[...] = wown[...]
    dec_out[...] = par[0, 0:1, :HEADS]
    bias_out[...] = par[1, 0:1, :HEADS]
    skip_out[...] = par[2, 0:1, :HEADS]
    gain_out[...] = gain[...]


def per_device(x, z, bc, raw, ids, counts, target, weight, dec, bias, skip, gain):
    vmem = pl.BlockSpec(memory_space=pltpu.VMEM)
    smem = pl.BlockSpec(memory_space=pltpu.SMEM)
    dma = pltpu.SemaphoreType.DMA
    shape = jax.ShapeDtypeStruct
    v = pltpu.VMEM
    rows_f = v((TOK, 128), f32)
    wide_f = v((TOK, WIDE), f32)
    wide_b = v((TOK, WIDE), bf16)
    states = v((CHUNKS + 1, STATE, WIDE), f32)
    sixteen = v((N_SEQ, 16, HALF), bf16)
    outs = pl.pallas_call(
        kernel,
        out_shape=(
            shape((1, STEPS), f32), shape((8, WIDE), f32), shape((1, HEADS), f32), shape((1, HEADS), f32),
            shape((1, HEADS), f32), shape((1, WIDE), f32),
        ),
        in_specs=[vmem] * 5 + [smem] + [vmem] * 6,
        out_specs=(vmem,) * 6,
        scratch_shapes=[
            v((128, WIDE), bf16), v((WIDE, 128), bf16), v((CHUNK, CHUNK), f32), v((3, 8, 128), f32), v((1, WIDE), f32),
            v((8, WIDE), f32),
            rows_f, rows_f, rows_f, v((8, 128), f32), rows_f, v((CHUNKS, 8, WIDE), f32),
            v((CHUNKS, CHUNK, CHUNK), f32), v((CHUNKS, CHUNK, CHUNK), f32),
            wide_b, wide_f, wide_f, v((8, 128), f32), v((CHUNKS, STATE, WIDE), f32), states, states, wide_b, wide_b, wide_b,
            wide_f, rows_f, v((2, 8, WIDE), f32),
            sixteen, sixteen, sixteen, sixteen, sixteen, sixteen, sixteen, sixteen, v((8, 128), f32),
            v((N_SEQ, 8, 128), f32),
            v((128, 16, HALF), bf16), v((WIDE, WIDE), bf16), v((N_Y, N_SEQ, 16, HALF), bf16),
            v((N_Y, N_SEQ, 16, HALF), bf16), v((64, 16, HALF), bf16), v((64, 16, HALF), bf16),
            v((16, 128), f32), v((N_SEQ, 16, 128), f32), v((16, 128), f32), v((N_DP, 16, 128), f32),
            v((8, 128), f32), v((N_SEQ, 8, 128), f32), v((8, 128), f32), v((N_DP, 8, 128), f32),
            dma((9,)), dma((9,)), dma, dma((N_Y,)), dma((N_Y,)), dma((N_Y,)), dma((N_Y,)), dma((N_Y,)), dma, dma,
        ],
        compiler_params=pltpu.CompilerParams(
            collective_id=0, has_side_effects=True, vmem_limit_bytes=62 * 1024 * 1024
        ),
    )(
        x[0], z[0], bc[0], raw[0], ids, counts, target[0], weight,
        dec.reshape(1, HEADS), bias.reshape(1, HEADS), skip.reshape(1, HEADS), gain.reshape(1, WIDE),
    )
    losses, weight, dec, bias, skip, gain = outs
    return (
        losses.reshape(STEPS), weight, dec.reshape(HEADS), bias.reshape(HEADS), skip.reshape(HEADS), gain.reshape(WIDE)
    )


def solution(mesh):
    tokens = P(DP, SEQ, None)
    return jax.shard_map(
        per_device,
        mesh=mesh,
        in_specs=(
            tokens, tokens, tokens, tokens, P(DP, SEQ), P(), tokens, P((DP, SEQ), None), P(), P(), P(), P(),
        ),
        out_specs=(P(), P((DP, SEQ), None), P(), P(), P(), P()),
        check_vma=False,
    )
```

```python
import jax
import jax.numpy as jnp
from jax import lax
from jax.experimental import pallas as pl
from jax.experimental.pallas import tpu as pltpu
from jax.sharding import PartitionSpec as P

STEPS = 2
DP, SEQ = "dp", "seq"
N_DP, N_SEQ, N_Y = 8, 16, 4
TOK, WIDE, STATE, HEADS, HEAD = 384, 1024, 128, 16, 64
CHUNK, CHUNKS, PAIRS = 128, 3, 8
HALF = WIDE // 2

norm_floor = 1.0
clip_limit = 1.0
learn_rate = 8.0
f32, bf16 = jnp.float32, jnp.bfloat16
highest = lax.Precision.HIGHEST


def dot(a, b):
    return jnp.dot(a, b, preferred_element_type=f32)


def dot_tn(a, b):
    return lax.dot_general(a, b, (((0,), (0,)), ((), ())), preferred_element_type=f32)


def dot_nt(a, b):
    return lax.dot_general(a, b, (((1,), (1,)), ((), ())), preferred_element_type=f32)


def iota(shape, dim):
    return lax.broadcasted_iota(jnp.int32, shape, dim)


def three_parts(v):
    high = v.astype(bf16).astype(f32)
    rest = v - high
    mid = rest.astype(bf16).astype(f32)
    low = rest - mid
    group = (iota(v.shape, 1) >> 4) & 3
    zero = jnp.zeros_like(v)
    return jnp.where(
        group == 0, high, jnp.where(group == 1, mid, jnp.where(group == 2, low, zero))
    ).astype(bf16)


def blocks_of(rows):
    left = rows[:, :HALF].reshape(N_SEQ, 1, 8, HALF)
    right = rows[:, HALF:].reshape(N_SEQ, 1, 8, HALF)
    return jnp.concatenate([left, right], axis=1).reshape(N_SEQ, 16, HALF)


def rows_of(blocks):
    count = blocks.shape[0]
    split = blocks.reshape(count, 2, 8, HALF)
    return split[:, 0].reshape(count * 8, HALF), split[:, 1].reshape(count * 8, HALF)


INPUTS = (
    "x_ref", "z_ref", "bc_ref", "raw_ref", "ids_ref", "cnt_ref", "tgt_ref", "w_ref", "dec_in", "bias_in",
    "skip_in", "gain_in",
)
OUTPUTS = (
    "loss_out", "w_out", "dec_out", "bias_out", "skip_out", "gain_out",
)
PARTS = "yxz"
WIDTH = {"y": 256, "x": 128, "z": 128}
FIRST = {"y": 0, "x": 256, "z": 384}


def scratch():
    dma, v = pltpu.SemaphoreType.DMA, pltpu.VMEM
    rows_f, wide_f, wide_b = v((TOK, 128), f32), v((TOK, WIDE), f32), v((TOK, WIDE), bf16)
    states, sixteen = v((CHUNKS + 1, STATE, WIDE), f32), v((N_SEQ, 16, HALF), bf16)
    small, small16, small8 = v((16, 128), f32), v((N_SEQ, 16, 128), f32), v((N_DP, 16, 128), f32)
    named = dict(
        ex=v((128, WIDE), bf16), red=v((WIDE, 128), bf16), tri=v((CHUNK, CHUNK), f32), par=v((3, 8, 128), f32),
        gain=v((1, WIDE), f32), wown=v((8, WIDE), f32), rawt=rows_f, wid=rows_f, dec_s=rows_f, ent=rows_f,
        chain=v((CHUNKS, 8, WIDE), f32), fcol=v((CHUNKS, CHUNK, CHUNK), f32), sc=v((CHUNKS, CHUNK, CHUNK), f32),
        xw=wide_b, wtd=wide_b, yin=wide_f, eexp=wide_f, gstate=v((CHUNKS, STATE, WIDE), f32), hst=states, apart=states,
        normb=wide_b, ogb=wide_b, gb=wide_b, q2a=rows_f, ds1=rows_f, accs=v((2, 8, WIDE), f32),
        hs=sixteen, hr=sixteen, hp=sixteen, hi=sixteen, gs=sixteen, gr=sixteen, gp=sixteen, gi=sixteen,
        cs=v((8, 128), f32), cr=v((N_SEQ, 8, 128), f32), wfull=v((WIDE, WIDE), bf16),
        wgp=v((N_Y, N_SEQ, 16, HALF), bf16), pr=v((N_Y, N_SEQ, 16, HALF), bf16),
        sa=small, sar=small16, sb2=small, sbr=small8, t1=v((1, 128), f32), t1r=v((1, 128), f32), t2=v((1, 128), f32),
        t2r=v((64, 1, 128), f32),
    )
    for p in PARTS:
        w = WIDTH[p]
        named["ag" + p] = v((128, 16, w), bf16)
        named["sb" + p] = v((64, 16, w), bf16)
        named["ra" + p] = v((3, N_SEQ, 16, w), bf16)
        named["mid" + p] = v((N_SEQ, 16, w), bf16)
        named["rb" + p] = v((N_SEQ, 16, w), bf16)
    for name, count in dict(s_send=9, s_recv=9, s_ps=4, s_pr=4, g1s=3, g1r=3, g2s=3, g2r=3, g3s=3, g3r=3, r1s=3, r1r=3, r2s=3, r2r=3).items():
        named[name] = dma((count,))
    return named


def kernel(*refs):
    names = INPUTS + OUTPUTS + tuple(scratch())
    assert len(names) == len(refs)
    program(**dict(zip(names, refs)))


def program(
    x_ref, z_ref, bc_ref, raw_ref, ids_ref, cnt_ref, tgt_ref, w_ref, dec_in, bias_in, skip_in, gain_in,
    loss_out, w_out, dec_out, bias_out, skip_out, gain_out,
    ex, red, tri, par, gain, wown, rawt, wid, dec_s, ent, chain, fcol, sc,
    xw, wtd, yin, eexp, gstate, hst, apart, normb, ogb, gb, q2a, ds1, accs,
    hs, hr, hp, hi, gs, gr, gp, gi, cs, cr, wfull, wgp, pr, sa, sar, sb2, sbr, t1, t1r, t2, t2r,
    s_send, s_recv, s_ps, s_pr, g1s, g1r, g2s, g2r, g3s, g3r, r1s, r1r, r2s, r2r, **part,
):
    dp, seq = lax.axis_index(DP), lax.axis_index(SEQ)
    yy, core = dp // 2, dp % 2
    partner = dp + 1 - 2 * core
    own_q = yy * N_SEQ + seq
    xx, zz = seq // 4, seq % 4
    place = {"y": yy, "x": xx, "z": zz}
    MESH = pl.DeviceIdType.MESH

    def at(d, s):
        return {DP: d, SEQ: s}

    def remote(src, dst, ss, rs, d, s):
        return pltpu.make_async_remote_copy(
            src_ref=src, dst_ref=dst, send_sem=ss, recv_sem=rs, device_id=at(d, s), device_id_type=MESH
        )

    barrier = pltpu.get_barrier_semaphore()

    def greet_same(k, carry):
        q = (own_q + k) % 64
        pl.semaphore_signal(barrier, 1, device_id=at((q // 16) * 2 + core, q % 16), device_id_type=MESH)
        return carry

    lax.fori_loop(1, 64, greet_same, 0)

    def greet_other(k, carry):
        pl.semaphore_signal(barrier, 1, device_id=at(k * 2 + 1 - core, seq), device_id_type=MESH)
        return carry

    lax.fori_loop(0, N_Y, greet_other, 0)

    row = iota((CHUNK, WIDE), 0)
    col = iota((CHUNK, WIDE), 1)
    ex[...] = jnp.where(((row & 15) == (col >> 6)) & (row < 48), 1.0, 0.0).astype(bf16)
    rrow = iota((WIDE, 128), 0)
    rcol = iota((WIDE, 128), 1)
    red[...] = jnp.where((rrow >> 6) == (rcol & 15), 1.0, 0.0).astype(bf16)
    ti, tj = iota((CHUNK, CHUNK), 0), iota((CHUNK, CHUNK), 1)
    tri[...] = jnp.where(ti >= tj, 1.0, 0.0)
    rep = jnp.where(iota((HEADS, 128), 0) == (iota((HEADS, 128), 1) & 15), 1.0, 0.0)

    spread = jnp.where((iota((128, 128), 0) & 15) == (iota((128, 128), 1) & 15), 1.0, 0.0)

    def tiled(ref):
        return jnp.dot(jnp.broadcast_to(ref[...], (8, HEADS)), rep, precision=highest, preferred_element_type=f32)

    par[0] = tiled(dec_in)
    par[1] = tiled(bias_in)
    par[2] = tiled(skip_in)
    gain[...] = gain_in[...]
    wown[...] = w_ref[...]
    rawt[...] = jnp.dot(raw_ref[...], rep, precision=highest, preferred_element_type=f32)

    def expand(v):
        return dot(three_parts(v), ex[...])

    def head_sum(v):
        high = v.astype(bf16)
        low = (v - high.astype(f32)).astype(bf16)
        return dot(high, red[...]) + dot(low, red[...])

    lane = iota((1, 128), 1)
    low_half = jnp.where(lane < HEAD, 1.0, 0.0).astype(bf16)
    high_half = jnp.where(lane < HEAD, 0.0, 1.0).astype(bf16)

    total = cnt_ref[0]
    for k in range(1, N_DP):
        total = total + cnt_ref[k]
    total_f = total.astype(f32)
    own_count = cnt_ref[dp]

    def rows(c):
        return pl.ds(pl.multiple_of(c * CHUNK, CHUNK), CHUNK)

    def prepare(c, carry):
        flag = jnp.where(ids_ref[0:1, rows(c)] == 0, 1.0, 0.0)
        flag_col = jnp.broadcast_to(flag, (CHUNK, CHUNK)).T
        seg = dot(tri[...], flag_col)
        seg_row = seg.T
        fcol[c] = seg
        scores = dot_nt(bc_ref[rows(c), STATE:], bc_ref[rows(c), :STATE])
        sc[c] = jnp.where((seg == seg_row) & (ti >= tj), scores, 0.0)
        return carry

    lax.fori_loop(0, CHUNKS, prepare, 0)

    def index_in(p, y, x, z):
        return {"y": y * 16 + x * 4 + z, "x": x * 16 + y * 4 + z, "z": z * 16 + x * 4 + y}[p]

    def plane_peer(p, k):
        a, b = {"y": (xx, zz), "x": (yy, zz), "z": (xx, yy)}[p]
        q = (a * 4 + b + k) % 16
        if p == "y":
            return dp, q, q
        if p == "x":
            return (q // 4) * 2 + core, xx * 4 + q % 4, q
        return (q % 4) * 2 + core, (q // 4) * 4 + zz, q

    def line_peer(p, k):
        c = (place[p] + k) % 4
        if p == "y":
            return c * 2 + core, seq, c
        if p == "x":
            return dp, c * 4 + zz, c
        return dp, xx * 4 + c, c

    mine_in = {p: index_in(p, yy, xx, zz) for p in PARTS}

    def ag_start():
        for n, p in enumerate(PARTS):
            buf = part["ag" + p]
            lanes = slice(FIRST[p], FIRST[p] + WIDTH[p])
            right = slice(HALF + FIRST[p], HALF + FIRST[p] + WIDTH[p])
            own = core * 64 + mine_in[p]
            buf[own] = jnp.concatenate([wown[:, lanes], wown[:, right]], axis=0).astype(bf16)

            def send(k, carry):
                d, s, _ = plane_peer(p, k)
                remote(buf.at[own], buf.at[own], g1s.at[n], g1r.at[n], d, s).start()
                return carry

            lax.fori_loop(1, 16, send, 0)

    def ag_line():
        for n, p in enumerate(PARTS):
            buf = part["ag" + p]
            piece = buf.at[pl.ds(0, 15)]
            remote(piece, piece, g1s.at[n], g1r.at[n], partner, seq).wait_recv()
            slab = buf.at[pl.ds(core * 64 + place[p] * 16, 16)]
            for k in range(1, 4):
                d, s, _ = line_peer(p, k)
                remote(slab, slab, g2s.at[n], g2r.at[n], d, s).start()

    def ag_cross():
        for n, p in enumerate(PARTS):
            buf = part["ag" + p]
            piece = buf.at[pl.ds(0, 48)]
            remote(piece, piece, g2s.at[n], g2r.at[n], partner, seq).wait_recv()
            ours = buf.at[pl.ds(core * 64, 64)]
            remote(ours, ours, g3s.at[n], g3r.at[n], partner, seq).start()

    def ag_finish():
        for n, p in enumerate(PARTS):
            buf = part["ag" + p]
            piece = buf.at[pl.ds((1 - core) * 64, 64)]
            remote(piece, piece, g3s.at[n], g3r.at[n], partner, seq).wait_recv()

        def unpack(d, carry):
            base, y = (d % 2) * 64, d // 2
            for p in PARTS:
                buf, w = part["ag" + p], WIDTH[p]
                if p == "y":
                    blocks = [buf[pl.ds(base + y * 16, 16)].astype(f32)]
                elif p == "x":
                    blocks = [buf[pl.ds(base + x * 16 + y * 4, 4)].astype(f32) for x in range(4)]
                else:
                    blocks = [buf[pl.ds(base + z * 16 + x * 4 + y, 1)].astype(f32) for x in range(4) for z in range(4)]
                tops, lows = [], []
                for block in blocks:
                    split = block.reshape(block.shape[0], 2, 8, w)
                    tops.append(split[:, 0].reshape(-1, w))
                    lows.append(split[:, 1].reshape(-1, w))
                wfull[rows(d), FIRST[p] : FIRST[p] + w] = jnp.concatenate(tops, axis=0).astype(bf16)
                wfull[rows(d), HALF + FIRST[p] : HALF + FIRST[p] + w] = jnp.concatenate(lows, axis=0).astype(bf16)
            return carry

        lax.fori_loop(0, N_DP, unpack, 0)

    def ag_sent():
        for n, p in enumerate(PARTS):
            buf = part["ag" + p]
            for count, ss, rs in ((15, g1s, g1r), (48, g2s, g2r), (64, g3s, g3r)):
                piece = buf.at[pl.ds(0, count)]
                remote(piece, piece, ss.at[n], rs.at[n], partner, seq).wait_send()

    def exchange_start(src, dst, n):
        def send(k, carry):
            peer = (seq + k) % N_SEQ
            remote(src.at[peer], dst.at[seq], s_send.at[n], s_recv.at[n], dp, peer).start()
            return carry

        lax.fori_loop(1, N_SEQ, send, 0)
        dst[seq] = src[seq]

    def spread_start(src, dst, n):
        def send(k, carry):
            peer = (seq + k) % N_SEQ
            remote(src, dst.at[seq], s_send.at[n], s_recv.at[n], dp, peer).start()
            return carry

        lax.fori_loop(1, N_SEQ, send, 0)
        dst[seq] = src[...]

    def cross_start(src, dst, n):
        def send(k, carry):
            peer = (dp + k) % N_DP
            remote(src, dst.at[dp], s_send.at[n], s_recv.at[n], peer, seq).start()
            return carry

        lax.fori_loop(1, N_DP, send, 0)
        dst[dp] = src[...]

    def recv_wait(dst, n, count):
        piece = dst.at[pl.ds(0, count)]
        remote(piece, piece, s_send.at[n], s_recv.at[n], partner, seq).wait_recv()

    def send_wait(dst, n, count):
        piece = dst.at[pl.ds(0, count)]
        remote(piece, piece, s_send.at[n], s_recv.at[n], partner, seq).wait_send()

    def one_step(step, losses):
        dec_t, bias_t, skip_t = par[0, 0:1], par[1, 0:1], par[2, 0:1]
        rate = jnp.exp(dec_t)

        hst[0] = jnp.zeros((STATE, WIDE), f32)

        def begin(c, carried):
            seg = fcol[c]
            pre = rawt[rows(c)] + bias_t
            u = jnp.exp(-jnp.abs(pre))
            v = 1.0 + u
            log1p = jnp.where(v == 1.0, u, jnp.log(v) * u / jnp.where(v == 1.0, 1.0, v - 1.0))
            width = jnp.maximum(pre, 0.0) + log1p
            s = jnp.dot(tri[...], -rate * width, precision=highest, preferred_element_type=f32)
            last = s[CHUNK - 1 : CHUNK]
            seg_last = seg[CHUNK - 1 : CHUNK]
            entering = jnp.exp(s) * jnp.where(seg == 0.0, 1.0, 0.0)
            leaving = jnp.exp(last - s) * jnp.where(seg == seg_last, 1.0, 0.0)
            through = jnp.exp(last) * jnp.where(seg_last == 0.0, 1.0, 0.0)
            wid[rows(c)] = width
            dec_s[rows(c)] = s
            ent[rows(c)] = entering
            chain[c] = expand(jnp.broadcast_to(through, (8, 128)))
            weighted = (x_ref[rows(c)].astype(f32) * expand(width * leaving)).astype(bf16)
            wtd[rows(c)] = weighted
            added = dot_tn(bc_ref[rows(c), :STATE], weighted)
            gstate[c] = added
            hst[0] = chain[c][0:1] * hst[0] + added
            return carried * through

        carried = lax.fori_loop(0, CHUNKS, begin, jnp.ones((1, 128), f32))
        wide8 = jnp.broadcast_to(carried, (8, 128))
        sub8, lane8 = iota((8, 128), 0), iota((8, 128), 1)
        even = jnp.sum(jnp.where(lane8 == 2 * sub8, wide8, 0.0), axis=1, keepdims=True)
        odd = jnp.sum(jnp.where(lane8 == 2 * sub8 + 1, wide8, 0.0), axis=1, keepdims=True)
        cs[...] = jnp.where(lane8 < HEAD, even, odd)

        def to_blocks(state, out):
            for r in range(8):
                for h in range(2):
                    out[2 * r + h] = state[16 * r : 16 * r + 16, HALF * h : HALF * (h + 1)].astype(bf16)

        to_blocks(hst[0], hs)

        @pl.when(step == 0)
        def _():
            pl.semaphore_wait(barrier, 67)

        exchange_start(hs, hr, 0)
        spread_start(cs, cr, 1)

        @pl.when(step == 0)
        def _():
            ag_start()

        def inside(c, carry):
            s = dec_s[rows(c)]
            s_t = s.T
            scores = sc[c]
            xw[rows(c)] = (x_ref[rows(c)].astype(f32) * expand(wid[rows(c)])).astype(bf16)
            eexp[rows(c)] = expand(ent[rows(c)])
            for p in range(PAIRS):
                parts = []
                for h in (2 * p, 2 * p + 1):
                    gap = jnp.minimum(s[:, h : h + 1] - s_t[h : h + 1, :], 0.0)
                    parts.append((jnp.exp(gap) * scores).astype(bf16))
                mine = xw[rows(c), 128 * p : 128 * (p + 1)]
                both = jnp.concatenate([mine * low_half, mine * high_half], axis=0)
                yin[rows(c), 128 * p : 128 * (p + 1)] = dot(jnp.concatenate(parts, axis=1), both)
            return carry

        lax.fori_loop(0, CHUNKS, inside, 0)
        ag_line()

        half = seq % 2

        def carry_rows(i):
            return [cr[i, pl.ds(4 * half + m, 1), :] for m in range(4)]

        recv_wait(hr, 0, 15)
        recv_wait(cr, 1, 15)

        def forward(i, state):
            factors = carry_rows(i)
            out = []
            for m in range(4):
                lanes = slice(128 * m, 128 * (m + 1))
                hp[i, :, lanes] = state[m].astype(bf16)
                out.append(factors[m] * state[m] + hr[i, :, lanes].astype(f32))
            return tuple(out)

        zeros4 = tuple(jnp.zeros((16, 128), f32) for _ in range(4))
        lax.fori_loop(0, N_SEQ, forward, zeros4)
        exchange_start(hp, hi, 2)
        ag_cross()
        ag_finish()
        recv_wait(hi, 2, 15)
        for r in range(8):
            for h in range(2):
                hst[0, 16 * r : 16 * r + 16, HALF * h : HALF * (h + 1)] = hi[2 * r + h].astype(f32)

        skip_e = expand(jnp.broadcast_to(skip_t, (8, 128)))[0:1]
        gain_e = gain[...]
        scale = 2.0 / (WIDE * total_f)
        accs[...] = jnp.zeros(accs.shape, f32)

        def mix(c, loss):
            state = hst[c]
            b_c, c_c = bc_ref[rows(c), :STATE], bc_ref[rows(c), STATE:]
            y_sum = yin[rows(c)] + eexp[rows(c)] * dot(c_c, state.astype(bf16))
            x_f = x_ref[rows(c)].astype(f32)
            z_f = z_ref[rows(c)].astype(f32)
            act = z_f / (1.0 + jnp.exp(-z_f))
            gated = (y_sum + skip_e * x_f) * act
            inv = lax.rsqrt(jnp.sum(gated * gated, axis=1, keepdims=True) * (1.0 / WIDE) + norm_floor)
            normed = (gated * gain_e * inv).astype(bf16)
            normb[rows(c)] = normed
            res = dot(normed, wfull[...]) - tgt_ref[rows(c)].astype(f32)
            position = seq * TOK + c * CHUNK + iota((CHUNK, 1), 0)
            scored = jnp.where(position < own_count, 1.0, 0.0)
            loss = loss + jnp.sum(jnp.sum(res * res, axis=1, keepdims=True) * scored, axis=0, keepdims=True)
            og = (res * (scored * scale)).astype(bf16)
            ogb[rows(c)] = og
            d_norm = dot_nt(og, wfull[...])
            d_gr = d_norm * gated * inv
            accs[0] += jnp.sum(d_gr.reshape(16, 8, WIDE), axis=0)
            inner = jnp.sum(d_gr * gain_e, axis=1, keepdims=True) * (1.0 / WIDE)
            d_gated = inv * (gain_e * d_norm - gated * (inv * inner))
            g = d_gated * act
            g_b = g.astype(bf16)
            gb[rows(c)] = g_b
            accs[1] += jnp.sum((g * x_f).reshape(16, 8, WIDE), axis=0)
            yin[rows(c)] = y_sum
            apart[c] = dot_tn(c_c, (g * eexp[rows(c)]).astype(bf16))
            hst[c + 1] = chain[c][0:1] * state + gstate[c]
            return loss

        loss = lax.fori_loop(0, CHUNKS, mix, jnp.zeros((1, 1), f32))
        entry = apart[0] + chain[0][0:1] * (apart[1] + chain[1][0:1] * apart[2])
        to_blocks(entry, gs)
        exchange_start(gs, gr, 3)
        gain_g = jnp.sum(accs[0], axis=0, keepdims=True)
        for r in range(8):
            sa[r : r + 1, :] = gain_g[:, 128 * r : 128 * (r + 1)]
        skip_g = head_sum(jnp.broadcast_to(jnp.sum(accs[1], axis=0, keepdims=True), (8, WIDE)))
        sub = iota((8, 128), 0)
        sa[8:16, :] = jnp.where(sub == 0, skip_g, jnp.where(sub == 1, jnp.broadcast_to(loss, (8, 128)), 0.0))
        spread_start(sa, sar, 4)

        def grad_rows(d):
            lanes = pl.ds(pl.multiple_of(d * 128, 128), 128)
            return blocks_of(dot_tn(normb[:, lanes], ogb[...]))

        for k in range(N_Y):
            y_k = (yy + k) % N_Y
            d = y_k * 2 + 1 - core
            wgp[k] = grad_rows(d).astype(bf16)
            remote(wgp.at[k], pr.at[k], s_ps.at[k], s_pr.at[k], partner, seq).start()
        for k in range(N_Y):
            y_k = (yy + k) % N_Y
            mine = grad_rows(y_k * 2 + core)
            remote(wgp.at[k], pr.at[k], s_ps.at[k], s_pr.at[k], partner, seq).wait_recv()
            both = (mine + pr[k].astype(f32)).astype(bf16)
            part["sby"][pl.ds(y_k * 16, 16)] = both[:, :, : WIDTH["y"]]
            if k > 0:
                slab = part["sby"].at[pl.ds(y_k * 16, 16)]
                remote(slab, part["ray"].at[k - 1], r1s.at[0], r1r.at[0], y_k * 2 + core, seq).start()
            for p in "xz":
                piece = both[:, :, FIRST[p] : FIRST[p] + WIDTH[p]]
                for x in range(4):
                    if p == "x":
                        part["sbx"][pl.ds(x * 16 + y_k * 4, 4)] = piece[4 * x : 4 * x + 4]
                    else:
                        for z in range(4):
                            part["sbz"][z * 16 + x * 4 + y_k] = piece[4 * x + z]
        for n, p in ((1, "x"), (2, "z")):
            for k in range(1, 4):
                d, s, c = line_peer(p, k)
                slab = part["sb" + p].at[pl.ds(c * 16, 16)]
                remote(slab, part["ra" + p].at[k - 1], r1s.at[n], r1r.at[n], d, s).start()

        def scatter_plane():
            for n, p in enumerate(PARTS):
                got, mid, dst = part["ra" + p], part["mid" + p], part["rb" + p]
                remote(got, got, r1s.at[n], r1r.at[n], partner, seq).wait_recv()

                def add(j, carry):
                    value = part["sb" + p][place[p] * 16 + j].astype(f32)
                    for k in range(3):
                        value = value + got[k, j].astype(f32)
                    mid[j] = value.astype(bf16)
                    return carry

                lax.fori_loop(0, 16, add, 0)
                here = mine_in[p] % 16

                def send(k, carry):
                    d, s, q = plane_peer(p, k)
                    remote(mid.at[q], dst.at[here], r2s.at[n], r2r.at[n], d, s).start()
                    return carry

                lax.fori_loop(1, 16, send, 0)
                dst[here] = mid[here]

        def inside_back(c, carry):
            s = dec_s[rows(c)]
            s_t = s.T
            scores = sc[c].T
            for p in range(PAIRS):
                parts = []
                for h in (2 * p, 2 * p + 1):
                    gap = jnp.minimum(s_t[h : h + 1, :] - s[:, h : h + 1], 0.0)
                    parts.append((jnp.exp(gap) * scores).astype(bf16))
                mine = gb[rows(c), 128 * p : 128 * (p + 1)]
                both = jnp.concatenate([mine * low_half, mine * high_half], axis=0)
                lanes = slice(128 * p, 128 * (p + 1))
                eexp[rows(c), lanes] = dot(jnp.concatenate(parts, axis=1), both)
            ds1[rows(c)] = head_sum(gb[rows(c)].astype(f32) * yin[rows(c)])
            q2a[rows(c)] = head_sum(xw[rows(c)].astype(f32) * eexp[rows(c)])
            return carry

        lax.fori_loop(0, CHUNKS, inside_back, 0)

        recv_wait(gr, 3, 15)

        def backward(n, state):
            i = N_SEQ - 1 - n
            factors = carry_rows(i)
            out = []
            for m in range(4):
                lanes = slice(128 * m, 128 * (m + 1))
                gp[i, :, lanes] = state[m].astype(bf16)
                out.append(factors[m] * state[m] + gr[i, :, lanes].astype(f32))
            return tuple(out)

        lax.fori_loop(0, N_SEQ, backward, zeros4)
        exchange_start(gp, gi, 5)

        scatter_plane()

        def summed(ref, count):
            value = ref[0]
            for k in range(1, count):
                value = value + ref[k]
            return value

        recv_wait(sar, 4, 15)
        sb2[...] = summed(sar, N_SEQ)
        cross_start(sb2, sbr, 6)

        recv_wait(gi, 5, 15)
        for r in range(8):
            for h in range(2):
                apart[3, 16 * r : 16 * r + 16, HALF * h : HALF * (h + 1)] = gi[2 * r + h].astype(f32)

        apart[2] = apart[2] + chain[2][0:1] * apart[3]
        apart[1] = apart[1] + chain[1][0:1] * apart[2]

        def back(c, sums):
            dec_g, bias_g = sums
            after = apart[c + 1]
            width = wid[rows(c)]
            z_t = dot(bc_ref[rows(c), :STATE], after.astype(bf16))
            q2 = q2a[rows(c)] + head_sum(wtd[rows(c)].astype(f32) * z_t)
            ends = jnp.sum((after * hst[c + 1]).reshape(16, 8, WIDE), axis=0)
            end_h = jnp.sum(head_sum(ends), axis=0, keepdims=True)
            d_s = ds1[rows(c)] - q2
            d_a = lax.dot_general(
                tri[...], d_s, (((0,), (0,)), ((), ())), precision=highest, preferred_element_type=f32
            ) + end_h
            d_w = q2 / width - rate * d_a
            pre = rawt[rows(c)] + bias_t
            sig = 1.0 / (1.0 + jnp.exp(-pre))
            dec_g = dec_g - jnp.sum(d_a * (rate * width), axis=0, keepdims=True)
            bias_g = bias_g + jnp.sum(d_w * sig, axis=0, keepdims=True)
            return dec_g, bias_g

        zero_row = jnp.zeros((1, 128), f32)
        dec_g, bias_g = lax.fori_loop(0, CHUNKS, back, (zero_row, zero_row))

        recv_wait(sbr, 6, 7)
        sums_a = summed(sbr, N_DP)

        ag_sent()

        grad, square = {}, jnp.zeros((1, 1), f32)
        for n, p in enumerate(PARTS):
            dst = part["rb" + p]
            got = dst.at[pl.ds(0, 15)]
            remote(got, got, r2s.at[n], r2r.at[n], partner, seq).wait_recv()
            value = dst[0].astype(f32)
            for q in range(1, 16):
                value = value + dst[q].astype(f32)
            grad[p] = value
            square = square + jnp.sum(jnp.sum(value * value, axis=1, keepdims=True), axis=0, keepdims=True)
        t1[...] = jnp.where(lane < 16, dec_g, jnp.where(lane < 32, bias_g, jnp.where(lane == 32, square, 0.0)))
        pair = remote(t1, t1r, s_send.at[7], s_recv.at[7], partner, seq)
        pair.start()
        pair.wait_recv()
        t2[...] = t1[...] + t1r[...]

        def send_small(k, carry):
            q = (own_q + k) % 64
            remote(t2, t2r.at[own_q], s_send.at[8], s_recv.at[8], (q // 16) * 2 + core, q % 16).start()
            return carry

        lax.fori_loop(1, 64, send_small, 0)
        t2r[own_q] = t2[...]
        recv_wait(t2r, 8, 63)
        sums_b = jnp.sum(t2r[...], axis=0)

        def heads_at(first):
            picked = jnp.where((lane >= first) & (lane < first + 16), sums_b, 0.0)
            return jnp.dot(jnp.broadcast_to(picked, (8, 128)), spread, precision=highest, preferred_element_type=f32)[0:1]

        dec_g, bias_g = heads_at(0), heads_at(16)
        squares = jnp.sum(jnp.where(lane == 32, sums_b, 0.0), axis=1, keepdims=True)
        gain_rows, skip_g, loss_all = sums_a[0:8], sums_a[8:9], sums_a[9:10]
        small = jnp.sum(
            jnp.where(lane < HEADS, dec_g * dec_g + bias_g * bias_g + skip_g * skip_g, 0.0), axis=1, keepdims=True
        )
        gains = jnp.sum(jnp.sum(gain_rows * gain_rows, axis=1, keepdims=True), axis=0, keepdims=True)
        norm = jnp.sqrt(squares + (small + gains))
        move = learn_rate * (clip_limit / jnp.maximum(norm, clip_limit))
        par[0] = jnp.broadcast_to(dec_t - move * dec_g, (8, 128))
        par[1] = jnp.broadcast_to(bias_t - move * bias_g, (8, 128))
        par[2] = jnp.broadcast_to(skip_t - move * skip_g, (8, 128))
        for r in range(8):
            lanes = slice(128 * r, 128 * (r + 1))
            gain[:, lanes] = gain[:, lanes] - move * gain_rows[r : r + 1]
        for p in PARTS:
            for h in range(2):
                lanes = slice(HALF * h + FIRST[p], HALF * h + FIRST[p] + WIDTH[p])
                wown[:, lanes] = wown[:, lanes] - move * grad[p][8 * h : 8 * h + 8]

        send_wait(hr, 0, 15)
        send_wait(cr, 1, 15)
        send_wait(hi, 2, 15)
        send_wait(gr, 3, 15)
        send_wait(sar, 4, 15)
        send_wait(gi, 5, 15)
        send_wait(sbr, 6, 7)
        pair.wait_send()
        send_wait(t2r, 8, 63)
        for k in range(N_Y):
            remote(wgp.at[k], pr.at[k], s_ps.at[k], s_pr.at[k], partner, seq).wait_send()
        for n, p in enumerate(PARTS):
            got, dst = part["ra" + p], part["rb" + p].at[pl.ds(0, 15)]
            remote(got, got, r1s.at[n], r1r.at[n], partner, seq).wait_send()
            remote(dst, dst, r2s.at[n], r2r.at[n], partner, seq).wait_send()

        @pl.when(step == 0)
        def _():
            ag_start()

        step_loss = loss_all[:, 0:1] * (1.0 / WIDE) / total_f
        return jnp.where(iota((1, STEPS), 1) == step, step_loss, losses)

    losses = lax.fori_loop(0, STEPS, one_step, jnp.zeros((1, STEPS), f32))
    loss_out[...] = losses
    w_out[...] = wown[...]
    dec_out[...] = par[0, 0:1, :HEADS]
    bias_out[...] = par[1, 0:1, :HEADS]
    skip_out[...] = par[2, 0:1, :HEADS]
    gain_out[...] = gain[...]


def per_device(x, z, bc, raw, ids, counts, target, weight, dec, bias, skip, gain):
    vmem = pl.BlockSpec(memory_space=pltpu.VMEM)
    smem = pl.BlockSpec(memory_space=pltpu.SMEM)
    shape = jax.ShapeDtypeStruct
    outs = pl.pallas_call(
        kernel,
        out_shape=(
            shape((1, STEPS), f32), shape((8, WIDE), f32), shape((1, HEADS), f32), shape((1, HEADS), f32),
            shape((1, HEADS), f32), shape((1, WIDE), f32),
        ),
        in_specs=[vmem] * 5 + [smem] + [vmem] * 6,
        out_specs=(vmem,) * 6,
        scratch_shapes=list(scratch().values()),
        compiler_params=pltpu.CompilerParams(
            collective_id=0, has_side_effects=True, vmem_limit_bytes=62 * 1024 * 1024
        ),
    )(
        x[0], z[0], bc[0], raw[0], ids, counts, target[0], weight,
        dec.reshape(1, HEADS), bias.reshape(1, HEADS), skip.reshape(1, HEADS), gain.reshape(1, WIDE),
    )
    losses, weight, dec, bias, skip, gain = outs
    return (
        losses.reshape(STEPS), weight, dec.reshape(HEADS), bias.reshape(HEADS), skip.reshape(HEADS), gain.reshape(WIDE)
    )


def solution(mesh):
    tokens = P(DP, SEQ, None)
    return jax.shard_map(
        per_device,
        mesh=mesh,
        in_specs=(
            tokens, tokens, tokens, tokens, P(DP, SEQ), P(), tokens, P((DP, SEQ), None), P(), P(), P(), P(),
        ),
        out_specs=(P(), P((DP, SEQ), None), P(), P(), P(), P()),
        check_vma=False,
    )
```

```python
import jax
import jax.numpy as jnp
from jax import lax
from jax.experimental import pallas as pl
from jax.experimental.pallas import tpu as pltpu
from jax.sharding import PartitionSpec as P

STEPS = 2
DP, SEQ = "dp", "seq"
N_DP, N_SEQ, N_Y = 8, 16, 4
TOK, WIDE, STATE, HEADS, HEAD = 384, 1024, 128, 16, 64
CHUNK, CHUNKS, PAIRS = 128, 3, 8
HALF = WIDE // 2

norm_floor = 1.0
clip_limit = 1.0
learn_rate = 8.0
f32, bf16 = jnp.float32, jnp.bfloat16
highest = lax.Precision.HIGHEST


def dot(a, b):
    return jnp.dot(a, b, preferred_element_type=f32)


def dot_tn(a, b):
    return lax.dot_general(a, b, (((0,), (0,)), ((), ())), preferred_element_type=f32)


def dot_nt(a, b):
    return lax.dot_general(a, b, (((1,), (1,)), ((), ())), preferred_element_type=f32)


def iota(shape, dim):
    return lax.broadcasted_iota(jnp.int32, shape, dim)


def three_parts(v):
    high = v.astype(bf16).astype(f32)
    rest = v - high
    mid = rest.astype(bf16).astype(f32)
    low = rest - mid
    group = (iota(v.shape, 1) >> 4) & 3
    zero = jnp.zeros_like(v)
    return jnp.where(
        group == 0, high, jnp.where(group == 1, mid, jnp.where(group == 2, low, zero))
    ).astype(bf16)


def blocks_of(rows):
    left = rows[:, :HALF].reshape(N_SEQ, 1, 8, HALF)
    right = rows[:, HALF:].reshape(N_SEQ, 1, 8, HALF)
    return jnp.concatenate([left, right], axis=1).reshape(N_SEQ, 16, HALF)


def rows_of(blocks):
    count = blocks.shape[0]
    split = blocks.reshape(count, 2, 8, HALF)
    return split[:, 0].reshape(count * 8, HALF), split[:, 1].reshape(count * 8, HALF)


INPUTS = (
    "x_in", "z_in", "bc_in", "raw_in", "ids_ref", "cnt_ref", "tgt_in", "w_ref", "dec_in", "bias_in", "skip_in", "gain_in",
)
OUTPUTS = ("packed_out",)
PARTS = "yxz"
WIDTH = {"y": 256, "x": 128, "z": 128}
FIRST = {"y": 0, "x": 256, "z": 384}


def scratch():
    dma, v = pltpu.SemaphoreType.DMA, pltpu.VMEM
    rows_f, wide_f, wide_b = v((TOK, 128), f32), v((TOK, WIDE), f32), v((TOK, WIDE), bf16)
    states, sixteen = v((CHUNKS + 1, STATE, WIDE), f32), v((N_SEQ, 16, HALF), bf16)
    small, small16, small8 = v((16, 128), f32), v((N_SEQ, 16, 128), f32), v((N_DP, 16, 128), f32)
    named = dict(
        x_ref=wide_b, z_ref=wide_b, bc_ref=v((TOK, 2 * STATE), bf16), tgt_ref=wide_b, s_in=dma((4,)),
        act=wide_f, gat=wide_f, dnf=wide_f, invs=rows_f,
        ex=v((128, WIDE), bf16), red=v((WIDE, 128), bf16), tri=v((CHUNK, CHUNK), f32), par=v((3, 8, 128), f32),
        gain=v((1, WIDE), f32), wown=v((8, WIDE), f32), rawt=rows_f, wid=rows_f, dec_s=rows_f, ent=rows_f,
        chain=v((8, WIDE), f32), fcol=v((CHUNKS, CHUNK, CHUNK), f32), sc=v((CHUNKS, CHUNK, CHUNK), f32),
        xw=wide_b, wtd=wide_b, yin=wide_f, eexp=wide_f, gstate=v((CHUNKS, STATE, WIDE), f32), hst=states, apart=states,
        normb=wide_b, ogb=wide_b, gb=wide_b, q2a=rows_f, ds1=rows_f, accs=v((2, 8, WIDE), f32),
        hs=sixteen, hr=sixteen, hp=sixteen, hi=sixteen, gs=sixteen, gr=sixteen, gp=sixteen, gi=sixteen,
        cs=v((8, 128), f32), cr=v((N_SEQ, 8, 128), f32), wfull=v((WIDE, WIDE), bf16),
        wgp=v((N_Y, N_SEQ, 16, HALF), bf16), pr=v((N_Y, N_SEQ, 16, HALF), bf16),
        sa=small, sar=small16, sb2=small, sbr=small8, t1=v((1, 128), f32), t1r=v((1, 128), f32), t2=v((1, 128), f32),
        t2r=v((64, 1, 128), f32),
    )
    for p in PARTS:
        w = WIDTH[p]
        named["ag" + p] = v((128, 16, w), bf16)
        named["sb" + p] = v((64, 16, w), bf16)
        named["ra" + p] = v((3, N_SEQ, 16, w), bf16)
        named["mid" + p] = v((N_SEQ, 16, w), bf16)
        named["rb" + p] = v((N_SEQ, 16, w), bf16)
    for name, count in dict(s_send=9, s_recv=9, s_ps=4, s_pr=4, g1s=3, g1r=3, g2s=3, g2r=3, g3s=3, g3r=3, r1s=3, r1r=3, r2s=3, r2r=3).items():
        named[name] = dma((count,))
    return named


def kernel(*refs):
    names = INPUTS + OUTPUTS + tuple(scratch())
    assert len(names) == len(refs)
    program(**dict(zip(names, refs)))


def program(
    x_in, z_in, bc_in, raw_in, ids_ref, cnt_ref, tgt_in, w_ref, dec_in, bias_in, skip_in, gain_in,
    packed_out, x_ref, z_ref, bc_ref, tgt_ref, s_in, act, gat, dnf, invs,
    ex, red, tri, par, gain, wown, rawt, wid, dec_s, ent, chain, fcol, sc,
    xw, wtd, yin, eexp, gstate, hst, apart, normb, ogb, gb, q2a, ds1, accs,
    hs, hr, hp, hi, gs, gr, gp, gi, cs, cr, wfull, wgp, pr, sa, sar, sb2, sbr, t1, t1r, t2, t2r,
    s_send, s_recv, s_ps, s_pr, g1s, g1r, g2s, g2r, g3s, g3r, r1s, r1r, r2s, r2r, **part,
):
    dp, seq = lax.axis_index(DP), lax.axis_index(SEQ)
    yy, core = dp // 2, dp % 2
    partner = dp + 1 - 2 * core
    own_q = yy * N_SEQ + seq
    xx, zz = seq // 4, seq % 4
    place = {"y": yy, "x": xx, "z": zz}
    MESH = pl.DeviceIdType.MESH

    def at(d, s):
        return {DP: d, SEQ: s}

    def remote(src, dst, ss, rs, d, s):
        return pltpu.make_async_remote_copy(
            src_ref=src, dst_ref=dst, send_sem=ss, recv_sem=rs, device_id=at(d, s), device_id_type=MESH
        )

    barrier = pltpu.get_barrier_semaphore()

    dps = [((yy + k) % 4) * 2 + core for k in range(4)]
    seqs = {(a, b): ((xx + a) % 4) * 4 + (zz + b) % 4 for a in range(4) for b in range(4)}

    def hops(offset):
        return sum(min(k, 4 - k) for k in offset)

    chips = [(a, b, c) for a in range(4) for b in range(4) for c in range(4)]
    far_first = sorted(chips[1:], key=lambda offset: -hops(offset))
    for a, b, c in far_first:
        pl.semaphore_signal(barrier, 1, device_id=at(dps[a], seqs[b, c]), device_id_type=MESH)
    for k in range(4):
        pl.semaphore_signal(barrier, 1, device_id=at(dps[k] + 1 - 2 * core, seq), device_id_type=MESH)
    loads = [
        pltpu.make_async_copy(source, target, s_in.at[n])
        for n, (source, target) in enumerate(((bc_in, bc_ref), (x_in, x_ref), (z_in, z_ref), (tgt_in, tgt_ref)))
    ]
    for load in loads:
        load.start()

    row = iota((CHUNK, WIDE), 0)
    col = iota((CHUNK, WIDE), 1)
    ex[...] = jnp.where(((row & 15) == (col >> 6)) & (row < 48), 1.0, 0.0).astype(bf16)
    rrow = iota((WIDE, 128), 0)
    rcol = iota((WIDE, 128), 1)
    red[...] = jnp.where((rrow >> 6) == (rcol & 15), 1.0, 0.0).astype(bf16)
    ti, tj = iota((CHUNK, CHUNK), 0), iota((CHUNK, CHUNK), 1)
    tri[...] = jnp.where(ti >= tj, 1.0, 0.0)
    rep = jnp.where(iota((HEADS, 128), 0) == (iota((HEADS, 128), 1) & 15), 1.0, 0.0)

    spread = jnp.where((iota((128, 128), 0) & 15) == (iota((128, 128), 1) & 15), 1.0, 0.0)

    def tiled(ref):
        return jnp.dot(jnp.broadcast_to(ref[...], (8, HEADS)), rep, precision=highest, preferred_element_type=f32)

    par[0] = tiled(dec_in)
    par[1] = tiled(bias_in)
    par[2] = tiled(skip_in)
    gain[...] = gain_in[...]
    wown[...] = w_ref[...]
    rawt[...] = lax.dot_general(
        raw_in[...], rep, (((0,), (0,)), ((), ())), precision=highest, preferred_element_type=f32
    )
    loads[0].wait()

    def expand(v):
        return dot(three_parts(v), ex[...])

    def head_sum(v):
        high = v.astype(bf16)
        low = (v - high.astype(f32)).astype(bf16)
        return dot(high, red[...]) + dot(low, red[...])

    lane = iota((1, 128), 1)
    low_half = jnp.where(lane < HEAD, 1.0, 0.0).astype(bf16)
    high_half = jnp.where(lane < HEAD, 0.0, 1.0).astype(bf16)

    total = cnt_ref[0]
    for k in range(1, N_DP):
        total = total + cnt_ref[k]
    total_f = total.astype(f32)
    own_count = cnt_ref[dp]

    def rows(c):
        return pl.ds(pl.multiple_of(c * CHUNK, CHUNK), CHUNK)

    def prepare(c, carry):
        flag = jnp.where(ids_ref[0:1, rows(c)] == 0, 1.0, 0.0)
        flag_col = jnp.broadcast_to(flag, (CHUNK, CHUNK)).T
        seg = dot(tri[...], flag_col)
        seg_row = seg.T
        fcol[c] = seg
        scores = dot_nt(bc_ref[rows(c), STATE:], bc_ref[rows(c), :STATE])
        sc[c] = jnp.where((seg == seg_row) & (ti >= tj), scores, 0.0)
        return carry

    lax.fori_loop(0, CHUNKS, prepare, 0)
    loads[1].wait()

    def index_in(p, y, x, z):
        return {"y": y * 16 + x * 4 + z, "x": x * 16 + y * 4 + z, "z": z * 16 + x * 4 + y}[p]

    def plane_peer(p, k):
        a, b = {"y": (xx, zz), "x": (yy, zz), "z": (xx, yy)}[p]
        q = (a * 4 + b + k) % 16
        if p == "y":
            return dp, q, q
        if p == "x":
            return (q // 4) * 2 + core, xx * 4 + q % 4, q
        return (q % 4) * 2 + core, (q // 4) * 4 + zz, q

    def line_peer(p, k):
        c = (place[p] + k) % 4
        if p == "y":
            return c * 2 + core, seq, c
        if p == "x":
            return dp, c * 4 + zz, c
        return dp, xx * 4 + c, c

    mine_in = {p: index_in(p, yy, xx, zz) for p in PARTS}

    def ag_start():
        for n, p in enumerate(PARTS):
            buf = part["ag" + p]
            lanes = slice(FIRST[p], FIRST[p] + WIDTH[p])
            right = slice(HALF + FIRST[p], HALF + FIRST[p] + WIDTH[p])
            own = core * 64 + mine_in[p]
            buf[own] = jnp.concatenate([wown[:, lanes], wown[:, right]], axis=0).astype(bf16)

            def send(k, carry):
                d, s, _ = plane_peer(p, k)
                remote(buf.at[own], buf.at[own], g1s.at[n], g1r.at[n], d, s).start()
                return carry

            lax.fori_loop(1, 16, send, 0)

    def ag_line():
        for n, p in enumerate(PARTS):
            buf = part["ag" + p]
            piece = buf.at[pl.ds(0, 15)]
            remote(piece, piece, g1s.at[n], g1r.at[n], partner, seq).wait_recv()
            slab = buf.at[pl.ds(core * 64 + place[p] * 16, 16)]
            for k in range(1, 4):
                d, s, _ = line_peer(p, k)
                remote(slab, slab, g2s.at[n], g2r.at[n], d, s).start()

    def ag_cross():
        for n, p in enumerate(PARTS):
            buf = part["ag" + p]
            piece = buf.at[pl.ds(0, 48)]
            remote(piece, piece, g2s.at[n], g2r.at[n], partner, seq).wait_recv()
            ours = buf.at[pl.ds(core * 64, 64)]
            remote(ours, ours, g3s.at[n], g3r.at[n], partner, seq).start()

    def ag_finish():
        def unpack(y, its_core):
            base, d = its_core * 64, y * 2 + its_core
            for p in PARTS:
                buf, w = part["ag" + p], WIDTH[p]
                if p == "y":
                    blocks = [buf[pl.ds(base + y * 16, 16)].astype(f32)]
                elif p == "x":
                    blocks = [buf[pl.ds(base + x * 16 + y * 4, 4)].astype(f32) for x in range(4)]
                else:
                    blocks = [buf[pl.ds(base + z * 16 + x * 4 + y, 1)].astype(f32) for x in range(4) for z in range(4)]
                tops, lows = [], []
                for block in blocks:
                    split = block.reshape(block.shape[0], 2, 8, w)
                    tops.append(split[:, 0].reshape(-1, w))
                    lows.append(split[:, 1].reshape(-1, w))
                wfull[rows(d), FIRST[p] : FIRST[p] + w] = jnp.concatenate(tops, axis=0).astype(bf16)
                wfull[rows(d), HALF + FIRST[p] : HALF + FIRST[p] + w] = jnp.concatenate(lows, axis=0).astype(bf16)
            return its_core

        lax.fori_loop(0, N_Y, unpack, core)
        for n, p in enumerate(PARTS):
            buf = part["ag" + p]
            piece = buf.at[pl.ds((1 - core) * 64, 64)]
            remote(piece, piece, g3s.at[n], g3r.at[n], partner, seq).wait_recv()
        lax.fori_loop(0, N_Y, unpack, 1 - core)

    def ag_sent():
        for n, p in enumerate(PARTS):
            buf = part["ag" + p]
            for count, ss, rs in ((15, g1s, g1r), (48, g2s, g2r), (64, g3s, g3r)):
                piece = buf.at[pl.ds(0, count)]
                remote(piece, piece, ss.at[n], rs.at[n], partner, seq).wait_send()

    def exchange_start(src, dst, n):
        def send(k, carry):
            peer = (seq + k) % N_SEQ
            remote(src.at[peer], dst.at[seq], s_send.at[n], s_recv.at[n], dp, peer).start()
            return carry

        lax.fori_loop(1, N_SEQ, send, 0)
        dst[seq] = src[seq]

    def spread_start(src, dst, n):
        def send(k, carry):
            peer = (seq + k) % N_SEQ
            remote(src, dst.at[seq], s_send.at[n], s_recv.at[n], dp, peer).start()
            return carry

        lax.fori_loop(1, N_SEQ, send, 0)
        dst[seq] = src[...]

    def cross_start(src, dst, n):
        def send(k, carry):
            peer = (dp + k) % N_DP
            remote(src, dst.at[dp], s_send.at[n], s_recv.at[n], peer, seq).start()
            return carry

        lax.fori_loop(1, N_DP, send, 0)
        dst[dp] = src[...]

    def recv_wait(dst, n, count):
        piece = dst.at[pl.ds(0, count)]
        remote(piece, piece, s_send.at[n], s_recv.at[n], partner, seq).wait_recv()

    def send_wait(dst, n, count):
        piece = dst.at[pl.ds(0, count)]
        remote(piece, piece, s_send.at[n], s_recv.at[n], partner, seq).wait_send()

    def one_step(step, losses):
        dec_t, bias_t, skip_t = par[0, 0:1], par[1, 0:1], par[2, 0:1]
        rate = jnp.exp(dec_t)

        pre = rawt[...] + bias_t
        u = jnp.exp(-jnp.abs(pre))
        v = 1.0 + u
        log1p = jnp.where(v == 1.0, u, jnp.log(v) * u / jnp.where(v == 1.0, 1.0, v - 1.0))
        widths = jnp.maximum(pre, 0.0) + log1p
        wid[...] = widths
        sub8, lane8 = iota((8, 128), 0), iota((8, 128), 1)
        through = jnp.zeros((8, 128), f32)
        carried = jnp.ones((1, 128), f32)
        for c in range(CHUNKS):
            span = slice(c * CHUNK, (c + 1) * CHUNK)
            seg = fcol[c]
            width = widths[span]
            s = jnp.dot(tri[...], -rate * width, precision=highest, preferred_element_type=f32)
            last = s[CHUNK - 1 : CHUNK]
            seg_last = seg[CHUNK - 1 : CHUNK]
            leaving = jnp.exp(last - s) * jnp.where(seg == seg_last, 1.0, 0.0)
            passing = jnp.exp(last) * jnp.where(seg_last == 0.0, 1.0, 0.0)
            dec_s[span] = s
            ent[span] = jnp.exp(s) * jnp.where(seg == 0.0, 1.0, 0.0)
            weighted = (x_ref[span].astype(f32) * expand(width * leaving)).astype(bf16)
            wtd[span] = weighted
            gstate[c] = dot_tn(bc_ref[span, :STATE], weighted)
            through = jnp.where(sub8 == c, passing, through)
            carried = carried * passing
        chain[...] = expand(through)
        wide8 = jnp.broadcast_to(carried, (8, 128))
        even = jnp.sum(jnp.where(lane8 == 2 * sub8, wide8, 0.0), axis=1, keepdims=True)
        odd = jnp.sum(jnp.where(lane8 == 2 * sub8 + 1, wide8, 0.0), axis=1, keepdims=True)
        cs[...] = jnp.where(lane8 < HEAD, even, odd)
        hst[0] = gstate[2] + chain[2:3] * (gstate[1] + chain[1:2] * gstate[0])

        def to_blocks(state, out):
            for r in range(8):
                for h in range(2):
                    out[2 * r + h] = state[16 * r : 16 * r + 16, HALF * h : HALF * (h + 1)].astype(bf16)

        to_blocks(hst[0], hs)

        @pl.when(step == 0)
        def _():
            loads[2].wait()

            def activate(c, carry):
                z_f = z_ref[rows(c)].astype(f32)
                act[rows(c)] = z_f / (1.0 + jnp.exp(-z_f))
                return carry

            lax.fori_loop(0, CHUNKS, activate, 0)
            loads[3].wait()
            pl.semaphore_wait(barrier, 67)
            ag_start()

        exchange_start(hs, hr, 0)
        spread_start(cs, cr, 1)

        def inside(c, carry):
            s = dec_s[rows(c)]
            s_t = s.T
            scores = sc[c]
            xw[rows(c)] = (x_ref[rows(c)].astype(f32) * expand(wid[rows(c)])).astype(bf16)
            eexp[rows(c)] = expand(ent[rows(c)])
            for p in range(PAIRS):
                parts = []
                for h in (2 * p, 2 * p + 1):
                    gap = jnp.minimum(s[:, h : h + 1] - s_t[h : h + 1, :], 0.0)
                    parts.append((jnp.exp(gap) * scores).astype(bf16))
                mine = xw[rows(c), 128 * p : 128 * (p + 1)]
                both = jnp.concatenate([mine * low_half, mine * high_half], axis=0)
                yin[rows(c), 128 * p : 128 * (p + 1)] = dot(jnp.concatenate(parts, axis=1), both)
            return carry

        lax.fori_loop(0, CHUNKS, inside, 0)
        ag_line()

        half = seq % 2

        def carry_rows(i):
            return [cr[i, pl.ds(4 * half + m, 1), :] for m in range(4)]

        recv_wait(hr, 0, 15)
        recv_wait(cr, 1, 15)

        def forward(i, state):
            factors = carry_rows(i)
            out = []
            for m in range(4):
                lanes = slice(128 * m, 128 * (m + 1))
                hp[i, :, lanes] = state[m].astype(bf16)
                out.append(factors[m] * state[m] + hr[i, :, lanes].astype(f32))
            return tuple(out)

        zeros4 = tuple(jnp.zeros((16, 128), f32) for _ in range(4))
        lax.fori_loop(0, N_SEQ, forward, zeros4)
        exchange_start(hp, hi, 2)
        ag_cross()
        ag_finish()
        recv_wait(hi, 2, 15)
        for r in range(8):
            for h in range(2):
                hst[0, 16 * r : 16 * r + 16, HALF * h : HALF * (h + 1)] = hi[2 * r + h].astype(f32)

        skip_e = expand(jnp.broadcast_to(skip_t, (8, 128)))[0:1]
        gain_e = gain[...]
        scale = 2.0 / (WIDE * total_f)
        accs[1] = jnp.zeros((8, WIDE), f32)

        for c in range(CHUNKS):
            span = slice(c * CHUNK, (c + 1) * CHUNK)
            state = hst[c]
            y_sum = yin[span] + eexp[span] * dot(bc_ref[span, STATE:], state.astype(bf16))
            yin[span] = y_sum
            gated = (y_sum + skip_e * x_ref[span].astype(f32)) * act[span]
            gat[span] = gated
            inv = lax.rsqrt(jnp.sum(gated * gated, axis=1, keepdims=True) * (1.0 / WIDE) + norm_floor)
            invs[span] = jnp.broadcast_to(inv, (CHUNK, 128))
            normb[span] = (gated * gain_e * inv).astype(bf16)
            hst[c + 1] = chain[c : c + 1] * state + gstate[c]
        position = seq * TOK + iota((TOK, 256), 0)
        scored = jnp.where(position < own_count, 1.0, 0.0)
        losses_8 = jnp.zeros((8, 256), f32)
        for n in range(4):
            lanes = slice(256 * n, 256 * (n + 1))
            res = (dot(normb[...], wfull[:, lanes]) - tgt_ref[:, lanes].astype(f32)) * scored
            losses_8 = losses_8 + jnp.sum((res * res).reshape(TOK // 8, 8, 256), axis=0)
            ogb[:, lanes] = (res * scale).astype(bf16)
        loss = jnp.sum(jnp.sum(losses_8, axis=1, keepdims=True), axis=0, keepdims=True)
        inner_l = jnp.zeros((TOK, 128), f32)
        for n in range(4):
            lanes = slice(256 * n, 256 * (n + 1))
            d_norm = dot_nt(ogb[...], wfull[lanes, :])
            dnf[:, lanes] = d_norm
            inv_2 = jnp.concatenate([invs[...], invs[...]], axis=1)
            d_gr = d_norm * gat[:, lanes] * inv_2
            accs[0, :, lanes] = jnp.sum(d_gr.reshape(TOK // 8, 8, 256), axis=0)
            term = d_gr * gain_e[:, lanes]
            inner_l = inner_l + (term[:, :128] + term[:, 128:])
        inner = jnp.sum(inner_l, axis=1, keepdims=True) * (1.0 / WIDE)
        for c in range(CHUNKS):
            span = slice(c * CHUNK, (c + 1) * CHUNK)
            inv = invs[span, 0:1]
            g = inv * (gain_e * dnf[span] - gat[span] * (inv * inner[span])) * act[span]
            gb[span] = g.astype(bf16)
            accs[1] += jnp.sum((g * x_ref[span].astype(f32)).reshape(16, 8, WIDE), axis=0)
            apart[c] = dot_tn(bc_ref[span, STATE:], (g * eexp[span]).astype(bf16))
        entry = apart[0] + chain[0:1] * (apart[1] + chain[1:2] * apart[2])
        to_blocks(entry, gs)
        exchange_start(gs, gr, 3)
        def grad_rows(d):
            lanes = pl.ds(pl.multiple_of(d * 128, 128), 128)
            return blocks_of(dot_tn(normb[:, lanes], ogb[...]))

        for k in (1, 2, 3, 0):
            y_k = (yy + k) % N_Y
            d = y_k * 2 + 1 - core
            wgp[k] = grad_rows(d).astype(bf16)
            remote(wgp.at[k], pr.at[k], s_ps.at[k], s_pr.at[k], partner, seq).start()
        gain_g = jnp.sum(accs[0], axis=0, keepdims=True)
        for r in range(8):
            sa[r : r + 1, :] = gain_g[:, 128 * r : 128 * (r + 1)]
        skip_g = head_sum(jnp.broadcast_to(jnp.sum(accs[1], axis=0, keepdims=True), (8, WIDE)))
        sub = iota((8, 128), 0)
        sa[8:16, :] = jnp.where(sub == 0, skip_g, jnp.where(sub == 1, jnp.broadcast_to(loss, (8, 128)), 0.0))
        spread_start(sa, sar, 4)

        for k in (1, 2, 3, 0):
            y_k = (yy + k) % N_Y
            mine = grad_rows(y_k * 2 + core)
            remote(wgp.at[k], pr.at[k], s_ps.at[k], s_pr.at[k], partner, seq).wait_recv()
            both = (mine + pr[k].astype(f32)).astype(bf16)
            part["sby"][pl.ds(y_k * 16, 16)] = both[:, :, : WIDTH["y"]]
            if k > 0:
                slab = part["sby"].at[pl.ds(y_k * 16, 16)]
                remote(slab, part["ray"].at[k - 1], r1s.at[0], r1r.at[0], y_k * 2 + core, seq).start()
            for p in "xz":
                piece = both[:, :, FIRST[p] : FIRST[p] + WIDTH[p]]
                for x in range(4):
                    if p == "x":
                        part["sbx"][pl.ds(x * 16 + y_k * 4, 4)] = piece[4 * x : 4 * x + 4]
                    else:
                        for z in range(4):
                            part["sbz"][z * 16 + x * 4 + y_k] = piece[4 * x + z]
        for n, p in ((1, "x"), (2, "z")):
            for k in range(1, 4):
                d, s, c = line_peer(p, k)
                slab = part["sb" + p].at[pl.ds(c * 16, 16)]
                remote(slab, part["ra" + p].at[k - 1], r1s.at[n], r1r.at[n], d, s).start()

        def scatter_plane():
            for n, p in enumerate(PARTS):
                got, mid, dst = part["ra" + p], part["mid" + p], part["rb" + p]
                remote(got, got, r1s.at[n], r1r.at[n], partner, seq).wait_recv()

                def add(j, carry):
                    value = part["sb" + p][place[p] * 16 + j].astype(f32)
                    for k in range(3):
                        value = value + got[k, j].astype(f32)
                    mid[j] = value.astype(bf16)
                    return carry

                lax.fori_loop(0, 16, add, 0)
                here = mine_in[p] % 16

                def send(k, carry):
                    d, s, q = plane_peer(p, k)
                    remote(mid.at[q], dst.at[here], r2s.at[n], r2r.at[n], d, s).start()
                    return carry

                lax.fori_loop(1, 16, send, 0)
                dst[here] = mid[here]

        def inside_back(c, carry):
            s = dec_s[rows(c)]
            s_t = s.T
            scores = sc[c].T
            for p in range(PAIRS):
                parts = []
                for h in (2 * p, 2 * p + 1):
                    gap = jnp.minimum(s_t[h : h + 1, :] - s[:, h : h + 1], 0.0)
                    parts.append((jnp.exp(gap) * scores).astype(bf16))
                mine = gb[rows(c), 128 * p : 128 * (p + 1)]
                both = jnp.concatenate([mine * low_half, mine * high_half], axis=0)
                lanes = slice(128 * p, 128 * (p + 1))
                eexp[rows(c), lanes] = dot(jnp.concatenate(parts, axis=1), both)
            ds1[rows(c)] = head_sum(gb[rows(c)].astype(f32) * yin[rows(c)])
            q2a[rows(c)] = head_sum(xw[rows(c)].astype(f32) * eexp[rows(c)])
            return carry

        lax.fori_loop(0, CHUNKS, inside_back, 0)

        recv_wait(gr, 3, 15)

        def backward(n, state):
            i = N_SEQ - 1 - n
            factors = carry_rows(i)
            out = []
            for m in range(4):
                lanes = slice(128 * m, 128 * (m + 1))
                gp[i, :, lanes] = state[m].astype(bf16)
                out.append(factors[m] * state[m] + gr[i, :, lanes].astype(f32))
            return tuple(out)

        lax.fori_loop(0, N_SEQ, backward, zeros4)
        exchange_start(gp, gi, 5)

        scatter_plane()

        def summed(ref, count):
            value = ref[0]
            for k in range(1, count):
                value = value + ref[k]
            return value

        recv_wait(sar, 4, 15)
        sb2[...] = summed(sar, N_SEQ)
        cross_start(sb2, sbr, 6)

        recv_wait(gi, 5, 15)
        for r in range(8):
            for h in range(2):
                apart[3, 16 * r : 16 * r + 16, HALF * h : HALF * (h + 1)] = gi[2 * r + h].astype(f32)

        apart[2] = apart[2] + chain[2:3] * apart[3]
        apart[1] = apart[1] + chain[1:2] * apart[2]

        def back(c, sums):
            dec_g, bias_g = sums
            after = apart[c + 1]
            width = wid[rows(c)]
            z_t = dot(bc_ref[rows(c), :STATE], after.astype(bf16))
            q2 = q2a[rows(c)] + head_sum(wtd[rows(c)].astype(f32) * z_t)
            ends = jnp.sum((after * hst[c + 1]).reshape(16, 8, WIDE), axis=0)
            end_h = jnp.sum(head_sum(ends), axis=0, keepdims=True)
            d_s = ds1[rows(c)] - q2
            d_a = lax.dot_general(
                tri[...], d_s, (((0,), (0,)), ((), ())), precision=highest, preferred_element_type=f32
            ) + end_h
            d_w = q2 / width - rate * d_a
            pre = rawt[rows(c)] + bias_t
            sig = 1.0 / (1.0 + jnp.exp(-pre))
            dec_g = dec_g - jnp.sum(d_a * (rate * width), axis=0, keepdims=True)
            bias_g = bias_g + jnp.sum(d_w * sig, axis=0, keepdims=True)
            return dec_g, bias_g

        zero_row = jnp.zeros((1, 128), f32)
        dec_g, bias_g = lax.fori_loop(0, CHUNKS, back, (zero_row, zero_row))

        recv_wait(sbr, 6, 7)
        sums_a = summed(sbr, N_DP)

        ag_sent()

        grad, square = {}, jnp.zeros((1, 1), f32)
        for n, p in enumerate(PARTS):
            dst = part["rb" + p]
            got = dst.at[pl.ds(0, 15)]
            remote(got, got, r2s.at[n], r2r.at[n], partner, seq).wait_recv()
            value = dst[0].astype(f32)
            for q in range(1, 16):
                value = value + dst[q].astype(f32)
            grad[p] = value
            square = square + jnp.sum(jnp.sum(value * value, axis=1, keepdims=True), axis=0, keepdims=True)
        t1[...] = jnp.where(lane < 16, dec_g, jnp.where(lane < 32, bias_g, jnp.where(lane == 32, square, 0.0)))
        pair = remote(t1, t1r, s_send.at[7], s_recv.at[7], partner, seq)
        pair.start()
        pair.wait_recv()
        t2[...] = t1[...] + t1r[...]

        for a, b, c in far_first:
            remote(t2, t2r.at[own_q], s_send.at[8], s_recv.at[8], dps[a], seqs[b, c]).start()
        t2r[own_q] = t2[...]
        recv_wait(t2r, 8, 63)
        sums_b = jnp.sum(t2r[...], axis=0)

        def heads_at(first):
            picked = jnp.where((lane >= first) & (lane < first + 16), sums_b, 0.0)
            return jnp.dot(jnp.broadcast_to(picked, (8, 128)), spread, precision=highest, preferred_element_type=f32)[0:1]

        dec_g, bias_g = heads_at(0), heads_at(16)
        squares = jnp.sum(jnp.where(lane == 32, sums_b, 0.0), axis=1, keepdims=True)
        gain_rows, skip_g, loss_all = sums_a[0:8], sums_a[8:9], sums_a[9:10]
        small = jnp.sum(
            jnp.where(lane < HEADS, dec_g * dec_g + bias_g * bias_g + skip_g * skip_g, 0.0), axis=1, keepdims=True
        )
        gains = jnp.sum(jnp.sum(gain_rows * gain_rows, axis=1, keepdims=True), axis=0, keepdims=True)
        norm = jnp.sqrt(squares + (small + gains))
        move = learn_rate * (clip_limit / jnp.maximum(norm, clip_limit))
        par[0] = jnp.broadcast_to(dec_t - move * dec_g, (8, 128))
        par[1] = jnp.broadcast_to(bias_t - move * bias_g, (8, 128))
        par[2] = jnp.broadcast_to(skip_t - move * skip_g, (8, 128))
        for r in range(8):
            lanes = slice(128 * r, 128 * (r + 1))
            gain[:, lanes] = gain[:, lanes] - move * gain_rows[r : r + 1]
        for p in PARTS:
            for h in range(2):
                lanes = slice(HALF * h + FIRST[p], HALF * h + FIRST[p] + WIDTH[p])
                wown[:, lanes] = wown[:, lanes] - move * grad[p][8 * h : 8 * h + 8]

        send_wait(hr, 0, 15)
        send_wait(cr, 1, 15)
        send_wait(hi, 2, 15)
        send_wait(gr, 3, 15)
        send_wait(sar, 4, 15)
        send_wait(gi, 5, 15)
        send_wait(sbr, 6, 7)
        pair.wait_send()
        send_wait(t2r, 8, 63)
        for k in range(N_Y):
            remote(wgp.at[k], pr.at[k], s_ps.at[k], s_pr.at[k], partner, seq).wait_send()
        for n, p in enumerate(PARTS):
            got, dst = part["ra" + p], part["rb" + p].at[pl.ds(0, 15)]
            remote(got, got, r1s.at[n], r1r.at[n], partner, seq).wait_send()
            remote(dst, dst, r2s.at[n], r2r.at[n], partner, seq).wait_send()

        @pl.when(step == 0)
        def _():
            ag_start()

        step_loss = loss_all[:, 0:1] * (1.0 / WIDE) / total_f
        return jnp.where(iota((1, STEPS), 1) == step, step_loss, losses)

    losses = lax.fori_loop(0, STEPS, one_step, jnp.zeros((1, STEPS), f32))
    packed_out[0:8] = wown[...]
    packed_out[8:9] = gain[...]
    packed_out[9:10, :] = jnp.zeros((1, WIDE), f32)
    for n in range(3):
        packed_out[9:10, 128 * n : 128 * (n + 1)] = par[n, 0:1]
    packed_out[9:10, 384 : 384 + STEPS] = losses


def split_kernel(packed, loss_out, w_out, dec_out, bias_out, skip_out, gain_out):
    w_out[...] = packed[0:8]
    gain_out[...] = packed[8:9]
    dec_out[...] = packed[9:10, 0:HEADS]
    bias_out[...] = packed[9:10, 128 : 128 + HEADS]
    skip_out[...] = packed[9:10, 256 : 256 + HEADS]
    loss_out[...] = packed[9:10, 384 : 384 + STEPS]


def per_device(x, z, bc, raw, ids, counts, target, weight, dec, bias, skip, gain):
    vmem = pl.BlockSpec(memory_space=pltpu.VMEM)
    smem = pl.BlockSpec(memory_space=pltpu.SMEM)
    anywhere = pl.BlockSpec(memory_space=pl.ANY)
    shape = jax.ShapeDtypeStruct
    packed = pl.pallas_call(
        kernel,
        out_shape=shape((16, WIDE), f32),
        in_specs=[anywhere] * 3 + [vmem] * 2 + [smem] + [anywhere] + [vmem] * 5,
        out_specs=vmem,
        scratch_shapes=list(scratch().values()),
        compiler_params=pltpu.CompilerParams(
            collective_id=0, has_side_effects=True, vmem_limit_bytes=62 * 1024 * 1024
        ),
    )(
        x[0], z[0], bc[0], raw[0].T, ids, counts, target[0], weight,
        dec.reshape(1, HEADS), bias.reshape(1, HEADS), skip.reshape(1, HEADS), gain.reshape(1, WIDE),
    )
    losses, weight, dec, bias, skip, gain = pl.pallas_call(
        split_kernel,
        out_shape=(
            shape((1, STEPS), f32), shape((8, WIDE), f32), shape((1, HEADS), f32), shape((1, HEADS), f32),
            shape((1, HEADS), f32), shape((1, WIDE), f32),
        ),
        in_specs=[vmem],
        out_specs=(vmem,) * 6,
    )(packed)
    return (
        losses.reshape(STEPS), weight, dec.reshape(HEADS), bias.reshape(HEADS), skip.reshape(HEADS), gain.reshape(WIDE)
    )


def solution(mesh):
    tokens = P(DP, SEQ, None)
    return jax.shard_map(
        per_device,
        mesh=mesh,
        in_specs=(
            tokens, tokens, tokens, tokens, P(DP, SEQ), P(), tokens, P((DP, SEQ), None), P(), P(), P(), P(),
        ),
        out_specs=(P(), P((DP, SEQ), None), P(), P(), P(), P()),
        check_vma=False,
    )
```

```python
import jax
import jax.numpy as jnp
from jax import lax
from jax.experimental import pallas as pl
from jax.experimental.pallas import tpu as pltpu
from jax.sharding import PartitionSpec as P

STEPS = 2
DP, SEQ = "dp", "seq"
N_DP, N_SEQ, N_Y = 8, 16, 4
TOK, WIDE, STATE, HEADS, HEAD = 384, 1024, 128, 16, 64
CHUNK, CHUNKS, PAIRS = 128, 3, 8
HALF = WIDE // 2

norm_floor = 1.0
clip_limit = 1.0
learn_rate = 8.0
f32, bf16 = jnp.float32, jnp.bfloat16
highest = lax.Precision.HIGHEST


def dot(a, b):
    return jnp.dot(a, b, preferred_element_type=f32)


def dot_tn(a, b):
    return lax.dot_general(a, b, (((0,), (0,)), ((), ())), preferred_element_type=f32)


def dot_nt(a, b):
    return lax.dot_general(a, b, (((1,), (1,)), ((), ())), preferred_element_type=f32)


def iota(shape, dim):
    return lax.broadcasted_iota(jnp.int32, shape, dim)


def three_parts(v):
    high = v.astype(bf16).astype(f32)
    rest = v - high
    mid = rest.astype(bf16).astype(f32)
    low = rest - mid
    group = (iota(v.shape, 1) >> 4) & 3
    zero = jnp.zeros_like(v)
    return jnp.where(
        group == 0, high, jnp.where(group == 1, mid, jnp.where(group == 2, low, zero))
    ).astype(bf16)


def blocks_of(rows):
    left = rows[:, :HALF].reshape(N_SEQ, 1, 8, HALF)
    right = rows[:, HALF:].reshape(N_SEQ, 1, 8, HALF)
    return jnp.concatenate([left, right], axis=1).reshape(N_SEQ, 16, HALF)


def rows_of(blocks):
    count = blocks.shape[0]
    split = blocks.reshape(count, 2, 8, HALF)
    return split[:, 0].reshape(count * 8, HALF), split[:, 1].reshape(count * 8, HALF)


INPUTS = (
    "x_in", "z_in", "bc_in", "raw_in", "ids_ref", "cnt_ref", "tgt_in", "w_ref", "dec_in", "bias_in", "skip_in", "gain_in",
)
OUTPUTS = ("packed_out",)
PARTS = "yxz"
WIDTH = {"y": 256, "x": 128, "z": 128}
FIRST = {"y": 0, "x": 256, "z": 384}


def scratch():
    dma, v = pltpu.SemaphoreType.DMA, pltpu.VMEM
    rows_f, wide_f, wide_b = v((TOK, 128), f32), v((TOK, WIDE), f32), v((TOK, WIDE), bf16)
    states, sixteen = v((CHUNKS + 1, STATE, WIDE), f32), v((2, N_SEQ, 16, HALF // 2), bf16)
    small, small16, small8 = v((16, 128), f32), v((N_SEQ, 16, 128), f32), v((N_DP, 16, 128), f32)
    named = dict(
        x_ref=wide_b, z_ref=wide_b, bc_ref=v((TOK, 2 * STATE), bf16), tgt_ref=wide_b, s_in=dma((4,)),
        act=wide_f, gat=wide_f, dnf=wide_f, invs=rows_f,
        ex=v((128, WIDE), bf16), red=v((WIDE, 128), bf16), tri=v((CHUNK, CHUNK), f32), par=v((3, 8, 128), f32),
        gain=v((1, WIDE), f32), wown=v((8, WIDE), f32), rawt=rows_f, wid=rows_f, dec_s=rows_f, ent=rows_f,
        chain=v((8, WIDE), f32), fcol=v((CHUNKS, CHUNK, CHUNK), f32), sc=v((CHUNKS, CHUNK, CHUNK), f32),
        xw=wide_b, wtd=wide_b, yin=wide_f, eexp=wide_f, gstate=v((CHUNKS, STATE, WIDE), f32), hst=states, apart=states,
        normb=wide_b, ogb=wide_b, gb=wide_b, q2a=rows_f, ds1=rows_f, accs=v((2, 8, WIDE), f32),
        hs=sixteen, hr=sixteen, hp=sixteen, hi=sixteen, gs=sixteen, gr=sixteen, gp=sixteen, gi=sixteen,
        cs=v((8, 128), f32), cr=v((N_SEQ, 8, 128), f32), wfull=v((WIDE, WIDE), bf16),
        wgp=v((N_Y, N_SEQ, 16, HALF), bf16), pr=v((N_Y, N_SEQ, 16, HALF), bf16),
        sa=small, sar=small16, sb2=small, sbr=small8, t1=v((1, 128), f32), t1r=v((1, 128), f32), t2=v((1, 128), f32),
        t2r=v((64, 1, 128), f32),
    )
    for p in PARTS:
        w = WIDTH[p]
        named["ag" + p] = v((128, 16, w), bf16)
        named["sb" + p] = v((64, 16, w), bf16)
        named["ra" + p] = v((3, N_SEQ, 16, w), bf16)
        named["mid" + p] = v((N_SEQ, 16, w), bf16)
        named["rb" + p] = v((N_SEQ, 16, w), bf16)
    for name, count in dict(s_ps=4, s_pr=4, g1s=3, g1r=3, g2s=3, g2r=3, g3s=3, g3r=3, r1s=3, r1r=3, r2s=3, r2r=3).items():
        named[name] = dma((count,))
    named["s_send"] = dma((9, 2))
    named["s_recv"] = dma((9, 2))
    return named


def kernel(*refs):
    names = INPUTS + OUTPUTS + tuple(scratch())
    assert len(names) == len(refs)
    program(**dict(zip(names, refs)))


def program(
    x_in, z_in, bc_in, raw_in, ids_ref, cnt_ref, tgt_in, w_ref, dec_in, bias_in, skip_in, gain_in,
    packed_out, x_ref, z_ref, bc_ref, tgt_ref, s_in, act, gat, dnf, invs,
    ex, red, tri, par, gain, wown, rawt, wid, dec_s, ent, chain, fcol, sc,
    xw, wtd, yin, eexp, gstate, hst, apart, normb, ogb, gb, q2a, ds1, accs,
    hs, hr, hp, hi, gs, gr, gp, gi, cs, cr, wfull, wgp, pr, sa, sar, sb2, sbr, t1, t1r, t2, t2r,
    s_send, s_recv, s_ps, s_pr, g1s, g1r, g2s, g2r, g3s, g3r, r1s, r1r, r2s, r2r, **part,
):
    dp, seq = lax.axis_index(DP), lax.axis_index(SEQ)
    yy, core = dp // 2, dp % 2
    partner = dp + 1 - 2 * core
    own_q = yy * N_SEQ + seq
    xx, zz = seq // 4, seq % 4
    place = {"y": yy, "x": xx, "z": zz}
    MESH = pl.DeviceIdType.MESH

    def at(d, s):
        return {DP: d, SEQ: s}

    def remote(src, dst, ss, rs, d, s):
        return pltpu.make_async_remote_copy(
            src_ref=src, dst_ref=dst, send_sem=ss, recv_sem=rs, device_id=at(d, s), device_id_type=MESH
        )

    barrier = pltpu.get_barrier_semaphore()

    dps = [((yy + k) % 4) * 2 + core for k in range(4)]
    seqs = {(a, b): ((xx + a) % 4) * 4 + (zz + b) % 4 for a in range(4) for b in range(4)}

    def hops(offset):
        return sum(min(k, 4 - k) for k in offset)

    chips = [(a, b, c) for a in range(4) for b in range(4) for c in range(4)]
    far_first = sorted(chips[1:], key=lambda offset: -hops(offset))
    for a, b, c in far_first:
        pl.semaphore_signal(barrier, 1, device_id=at(dps[a], seqs[b, c]), device_id_type=MESH)
    for k in range(4):
        pl.semaphore_signal(barrier, 1, device_id=at(dps[k] + 1 - 2 * core, seq), device_id_type=MESH)
    loads = [
        pltpu.make_async_copy(source, target, s_in.at[n])
        for n, (source, target) in enumerate(((bc_in, bc_ref), (x_in, x_ref), (z_in, z_ref), (tgt_in, tgt_ref)))
    ]
    for load in loads:
        load.start()

    row = iota((CHUNK, WIDE), 0)
    col = iota((CHUNK, WIDE), 1)
    ex[...] = jnp.where(((row & 15) == (col >> 6)) & (row < 48), 1.0, 0.0).astype(bf16)
    rrow = iota((WIDE, 128), 0)
    rcol = iota((WIDE, 128), 1)
    red[...] = jnp.where((rrow >> 6) == (rcol & 15), 1.0, 0.0).astype(bf16)
    ti, tj = iota((CHUNK, CHUNK), 0), iota((CHUNK, CHUNK), 1)
    tri[...] = jnp.where(ti >= tj, 1.0, 0.0)
    rep = jnp.where(iota((HEADS, 128), 0) == (iota((HEADS, 128), 1) & 15), 1.0, 0.0)

    spread = jnp.where((iota((128, 128), 0) & 15) == (iota((128, 128), 1) & 15), 1.0, 0.0)

    def tiled(ref):
        return jnp.dot(jnp.broadcast_to(ref[...], (8, HEADS)), rep, precision=highest, preferred_element_type=f32)

    par[0] = tiled(dec_in)
    par[1] = tiled(bias_in)
    par[2] = tiled(skip_in)
    gain[...] = gain_in[...]
    wown[...] = w_ref[...]
    rawt[...] = lax.dot_general(
        raw_in[...], rep, (((0,), (0,)), ((), ())), precision=highest, preferred_element_type=f32
    )
    loads[0].wait()

    def expand(v):
        return dot(three_parts(v), ex[...])

    def head_sum(v):
        high = v.astype(bf16)
        low = (v - high.astype(f32)).astype(bf16)
        return dot(high, red[...]) + dot(low, red[...])

    lane = iota((1, 128), 1)
    low_half = jnp.where(lane < HEAD, 1.0, 0.0).astype(bf16)
    high_half = jnp.where(lane < HEAD, 0.0, 1.0).astype(bf16)

    total = cnt_ref[0]
    for k in range(1, N_DP):
        total = total + cnt_ref[k]
    total_f = total.astype(f32)
    own_count = cnt_ref[dp]

    def rows(c):
        return pl.ds(pl.multiple_of(c * CHUNK, CHUNK), CHUNK)

    def prepare(c, carry):
        flag = jnp.where(ids_ref[0:1, rows(c)] == 0, 1.0, 0.0)
        flag_col = jnp.broadcast_to(flag, (CHUNK, CHUNK)).T
        seg = dot(tri[...], flag_col)
        seg_row = seg.T
        fcol[c] = seg
        scores = dot_nt(bc_ref[rows(c), STATE:], bc_ref[rows(c), :STATE])
        sc[c] = jnp.where((seg == seg_row) & (ti >= tj), scores, 0.0)
        return carry

    lax.fori_loop(0, CHUNKS, prepare, 0)
    loads[1].wait()

    def index_in(p, y, x, z):
        return {"y": y * 16 + x * 4 + z, "x": x * 16 + y * 4 + z, "z": z * 16 + x * 4 + y}[p]

    plane_far = sorted([(a, b) for a in range(4) for b in range(4)][1:], key=lambda offset: -hops(offset))

    def plane_peer(p, a, b):
        if p == "y":
            return dp, seqs[a, b], seqs[a, b]
        if p == "x":
            return dps[a], seqs[0, b], ((yy + a) % 4) * 4 + (zz + b) % 4
        return dps[b], seqs[a, 0], ((xx + a) % 4) * 4 + (yy + b) % 4

    def line_peer(p, k):
        c = (place[p] + k) % 4
        if p == "y":
            return c * 2 + core, seq, c
        if p == "x":
            return dp, c * 4 + zz, c
        return dp, xx * 4 + c, c

    mine_in = {p: index_in(p, yy, xx, zz) for p in PARTS}

    def ag_start():
        for n, p in enumerate(PARTS):
            buf = part["ag" + p]
            lanes = slice(FIRST[p], FIRST[p] + WIDTH[p])
            right = slice(HALF + FIRST[p], HALF + FIRST[p] + WIDTH[p])
            own = core * 64 + mine_in[p]
            buf[own] = jnp.concatenate([wown[:, lanes], wown[:, right]], axis=0).astype(bf16)

            for a, b in plane_far:
                d, s, _ = plane_peer(p, a, b)
                remote(buf.at[own], buf.at[own], g1s.at[n], g1r.at[n], d, s).start()

    def ag_line():
        for n, p in enumerate(PARTS):
            buf = part["ag" + p]
            piece = buf.at[pl.ds(0, 15)]
            remote(piece, piece, g1s.at[n], g1r.at[n], partner, seq).wait_recv()
            slab = buf.at[pl.ds(core * 64 + place[p] * 16, 16)]
            for k in range(1, 4):
                d, s, _ = line_peer(p, k)
                remote(slab, slab, g2s.at[n], g2r.at[n], d, s).start()

    def ag_cross():
        for n, p in enumerate(PARTS):
            buf = part["ag" + p]
            piece = buf.at[pl.ds(0, 48)]
            remote(piece, piece, g2s.at[n], g2r.at[n], partner, seq).wait_recv()
            ours = buf.at[pl.ds(core * 64, 64)]
            remote(ours, ours, g3s.at[n], g3r.at[n], partner, seq).start()

    def ag_finish():
        def unpack(y, its_core):
            base, d = its_core * 64, y * 2 + its_core
            for p in PARTS:
                buf, w = part["ag" + p], WIDTH[p]
                if p == "y":
                    blocks = [buf[pl.ds(base + y * 16, 16)].astype(f32)]
                elif p == "x":
                    blocks = [buf[pl.ds(base + x * 16 + y * 4, 4)].astype(f32) for x in range(4)]
                else:
                    blocks = [buf[pl.ds(base + z * 16 + x * 4 + y, 1)].astype(f32) for x in range(4) for z in range(4)]
                tops, lows = [], []
                for block in blocks:
                    split = block.reshape(block.shape[0], 2, 8, w)
                    tops.append(split[:, 0].reshape(-1, w))
                    lows.append(split[:, 1].reshape(-1, w))
                wfull[rows(d), FIRST[p] : FIRST[p] + w] = jnp.concatenate(tops, axis=0).astype(bf16)
                wfull[rows(d), HALF + FIRST[p] : HALF + FIRST[p] + w] = jnp.concatenate(lows, axis=0).astype(bf16)
            return its_core

        lax.fori_loop(0, N_Y, unpack, core)
        for n, p in enumerate(PARTS):
            buf = part["ag" + p]
            piece = buf.at[pl.ds((1 - core) * 64, 64)]
            remote(piece, piece, g3s.at[n], g3r.at[n], partner, seq).wait_recv()
        lax.fori_loop(0, N_Y, unpack, 1 - core)

    def ag_sent():
        for n, p in enumerate(PARTS):
            buf = part["ag" + p]
            for count, ss, rs in ((15, g1s, g1r), (48, g2s, g2r), (64, g3s, g3r)):
                piece = buf.at[pl.ds(0, count)]
                remote(piece, piece, ss.at[n], rs.at[n], partner, seq).wait_send()

    def exchange_start(src, dst, n, h):
        for a, b in plane_far:
            peer = seqs[a, b]
            remote(src.at[h, peer], dst.at[h, seq], s_send.at[n, h], s_recv.at[n, h], dp, peer).start()
        dst[h, seq] = src[h, seq]

    def spread_start(src, dst, n):
        for a, b in plane_far:
            remote(src, dst.at[seq], s_send.at[n, 0], s_recv.at[n, 0], dp, seqs[a, b]).start()
        dst[seq] = src[...]

    def cross_start(src, dst, n):
        for k in range(1, N_DP):
            remote(src, dst.at[dp], s_send.at[n, 0], s_recv.at[n, 0], (dp + k) % N_DP, seq).start()
        dst[dp] = src[...]

    def recv_wait(dst, n, count, h=0):
        piece = dst.at[pl.ds(0, count)]
        remote(piece, piece, s_send.at[n, h], s_recv.at[n, h], partner, seq).wait_recv()

    def send_wait(dst, n, count, h=0):
        piece = dst.at[pl.ds(0, count)]
        remote(piece, piece, s_send.at[n, h], s_recv.at[n, h], partner, seq).wait_send()

    def one_step(step, losses):
        dec_t, bias_t, skip_t = par[0, 0:1], par[1, 0:1], par[2, 0:1]
        rate = jnp.exp(dec_t)

        pre = rawt[...] + bias_t
        u = jnp.exp(-jnp.abs(pre))
        v = 1.0 + u
        log1p = jnp.where(v == 1.0, u, jnp.log(v) * u / jnp.where(v == 1.0, 1.0, v - 1.0))
        widths = jnp.maximum(pre, 0.0) + log1p
        wid[...] = widths
        sub8, lane8 = iota((8, 128), 0), iota((8, 128), 1)
        through = jnp.zeros((8, 128), f32)
        carried = jnp.ones((1, 128), f32)
        for c in range(CHUNKS):
            span = slice(c * CHUNK, (c + 1) * CHUNK)
            seg = fcol[c]
            width = widths[span]
            s = jnp.dot(tri[...], -rate * width, precision=highest, preferred_element_type=f32)
            last = s[CHUNK - 1 : CHUNK]
            seg_last = seg[CHUNK - 1 : CHUNK]
            leaving = jnp.exp(last - s) * jnp.where(seg == seg_last, 1.0, 0.0)
            passing = jnp.exp(last) * jnp.where(seg_last == 0.0, 1.0, 0.0)
            dec_s[span] = s
            ent[span] = jnp.exp(s) * jnp.where(seg == 0.0, 1.0, 0.0)
            weighted = (x_ref[span].astype(f32) * expand(width * leaving)).astype(bf16)
            wtd[span] = weighted
            gstate[c] = dot_tn(bc_ref[span, :STATE], weighted)
            through = jnp.where(sub8 == c, passing, through)
            carried = carried * passing
        chain[...] = expand(through)
        wide8 = jnp.broadcast_to(carried, (8, 128))
        even = jnp.sum(jnp.where(lane8 == 2 * sub8, wide8, 0.0), axis=1, keepdims=True)
        odd = jnp.sum(jnp.where(lane8 == 2 * sub8 + 1, wide8, 0.0), axis=1, keepdims=True)
        cs[...] = jnp.where(lane8 < HEAD, even, odd)
        hst[0] = gstate[2] + chain[2:3] * (gstate[1] + chain[1:2] * gstate[0])

        def to_blocks(state, out):
            for r in range(8):
                for h in range(2):
                    for q in range(2):
                        first = HALF * h + 256 * q
                        out[q, 2 * r + h] = state[16 * r : 16 * r + 16, first : first + 256].astype(bf16)

        def from_blocks(source, put):
            for q in range(2):
                for r in range(8):
                    for h in range(2):
                        first = HALF * h + 256 * q
                        put(slice(16 * r, 16 * r + 16), slice(first, first + 256), source[q, 2 * r + h].astype(f32))

        to_blocks(hst[0], hs)

        @pl.when(step == 0)
        def _():
            loads[2].wait()

            def activate(c, carry):
                z_f = z_ref[rows(c)].astype(f32)
                act[rows(c)] = z_f / (1.0 + jnp.exp(-z_f))
                return carry

            lax.fori_loop(0, CHUNKS, activate, 0)
            loads[3].wait()
            pl.semaphore_wait(barrier, 67)
            ag_start()

        exchange_start(hs, hr, 0, 0)
        spread_start(cs, cr, 1)
        exchange_start(hs, hr, 0, 1)

        def inside(c, carry):
            s = dec_s[rows(c)]
            s_t = s.T
            scores = sc[c]
            xw[rows(c)] = (x_ref[rows(c)].astype(f32) * expand(wid[rows(c)])).astype(bf16)
            eexp[rows(c)] = expand(ent[rows(c)])
            for p in range(PAIRS):
                parts = []
                for h in (2 * p, 2 * p + 1):
                    gap = jnp.minimum(s[:, h : h + 1] - s_t[h : h + 1, :], 0.0)
                    parts.append((jnp.exp(gap) * scores).astype(bf16))
                mine = xw[rows(c), 128 * p : 128 * (p + 1)]
                both = jnp.concatenate([mine * low_half, mine * high_half], axis=0)
                yin[rows(c), 128 * p : 128 * (p + 1)] = dot(jnp.concatenate(parts, axis=1), both)
            return carry

        lax.fori_loop(0, CHUNKS, inside, 0)
        ag_line()

        half = seq % 2

        def scan(source, out, h, order):
            state = [jnp.zeros((16, 128), f32) for _ in range(2)]
            for i in order:
                for m in range(2):
                    lanes = slice(128 * m, 128 * (m + 1))
                    out[h, i, :, lanes] = state[m].astype(bf16)
                    factor = cr[i, pl.ds(4 * half + 2 * h + m, 1), :]
                    state[m] = factor * state[m] + source[h, i, :, lanes].astype(f32)

        recv_wait(cr, 1, 15)
        for h in range(2):
            recv_wait(hr.at[h], 0, 15, h)
            scan(hr, hp, h, range(N_SEQ))
            exchange_start(hp, hi, 2, h)
        ag_cross()
        ag_finish()
        for h in range(2):
            recv_wait(hi.at[h], 2, 15, h)

        def put_state(at_rows, lanes, value):
            hst[0, at_rows, lanes] = value

        from_blocks(hi, put_state)

        skip_e = expand(jnp.broadcast_to(skip_t, (8, 128)))[0:1]
        gain_e = gain[...]
        scale = 2.0 / (WIDE * total_f)
        accs[1] = jnp.zeros((8, WIDE), f32)

        for c in range(CHUNKS):
            span = slice(c * CHUNK, (c + 1) * CHUNK)
            state = hst[c]
            y_sum = yin[span] + eexp[span] * dot(bc_ref[span, STATE:], state.astype(bf16))
            yin[span] = y_sum
            gated = (y_sum + skip_e * x_ref[span].astype(f32)) * act[span]
            gat[span] = gated
            inv = lax.rsqrt(jnp.sum(gated * gated, axis=1, keepdims=True) * (1.0 / WIDE) + norm_floor)
            invs[span] = jnp.broadcast_to(inv, (CHUNK, 128))
            normb[span] = (gated * gain_e * inv).astype(bf16)
            hst[c + 1] = chain[c : c + 1] * state + gstate[c]
        position = seq * TOK + iota((TOK, 256), 0)
        scored = jnp.where(position < own_count, 1.0, 0.0)
        losses_8 = jnp.zeros((8, 256), f32)
        for n in range(4):
            lanes = slice(256 * n, 256 * (n + 1))
            res = (dot(normb[...], wfull[:, lanes]) - tgt_ref[:, lanes].astype(f32)) * scored
            losses_8 = losses_8 + jnp.sum((res * res).reshape(TOK // 8, 8, 256), axis=0)
            ogb[:, lanes] = (res * scale).astype(bf16)
        loss = jnp.sum(jnp.sum(losses_8, axis=1, keepdims=True), axis=0, keepdims=True)
        inner_l = jnp.zeros((TOK, 128), f32)
        for n in range(4):
            lanes = slice(256 * n, 256 * (n + 1))
            d_norm = dot_nt(ogb[...], wfull[lanes, :])
            dnf[:, lanes] = d_norm
            inv_2 = jnp.concatenate([invs[...], invs[...]], axis=1)
            d_gr = d_norm * gat[:, lanes] * inv_2
            accs[0, :, lanes] = jnp.sum(d_gr.reshape(TOK // 8, 8, 256), axis=0)
            term = d_gr * gain_e[:, lanes]
            inner_l = inner_l + (term[:, :128] + term[:, 128:])
        inner = jnp.sum(inner_l, axis=1, keepdims=True) * (1.0 / WIDE)
        for c in range(CHUNKS):
            span = slice(c * CHUNK, (c + 1) * CHUNK)
            inv = invs[span, 0:1]
            g = inv * (gain_e * dnf[span] - gat[span] * (inv * inner[span])) * act[span]
            gb[span] = g.astype(bf16)
            accs[1] += jnp.sum((g * x_ref[span].astype(f32)).reshape(16, 8, WIDE), axis=0)
            apart[c] = dot_tn(bc_ref[span, STATE:], (g * eexp[span]).astype(bf16))
        entry = apart[0] + chain[0:1] * (apart[1] + chain[1:2] * apart[2])
        to_blocks(entry, gs)
        for h in range(2):
            exchange_start(gs, gr, 3, h)
        def grad_rows(first, second):
            lanes = [normb[:, pl.ds(pl.multiple_of(d * 128, 128), 128)] for d in (first, second)]
            both = dot_tn(jnp.concatenate(lanes, axis=1), ogb[...])
            return blocks_of(both[:128]), blocks_of(both[128:])

        def group(k, c):
            return ((yy + k) % N_Y) * 2 + c

        for pair in ((1, 2), (3, 0)):
            pieces = grad_rows(*[group(k, 1 - core) for k in pair])
            for k, piece in zip(pair, pieces):
                wgp[k] = piece.astype(bf16)
                remote(wgp.at[k], pr.at[k], s_ps.at[k], s_pr.at[k], partner, seq).start()
        gain_g = jnp.sum(accs[0], axis=0, keepdims=True)
        for r in range(8):
            sa[r : r + 1, :] = gain_g[:, 128 * r : 128 * (r + 1)]
        skip_g = head_sum(jnp.broadcast_to(jnp.sum(accs[1], axis=0, keepdims=True), (8, WIDE)))
        sub = iota((8, 128), 0)
        sa[8:16, :] = jnp.where(sub == 0, skip_g, jnp.where(sub == 1, jnp.broadcast_to(loss, (8, 128)), 0.0))
        spread_start(sa, sar, 4)

        for pair in ((1, 2), (3, 0)):
            pieces = grad_rows(*[group(k, core) for k in pair])
            for k, mine in zip(pair, pieces):
                y_k = (yy + k) % N_Y
                remote(wgp.at[k], pr.at[k], s_ps.at[k], s_pr.at[k], partner, seq).wait_recv()
                both = (mine + pr[k].astype(f32)).astype(bf16)
                part["sby"][pl.ds(y_k * 16, 16)] = both[:, :, : WIDTH["y"]]
                if k > 0:
                    slab = part["sby"].at[pl.ds(y_k * 16, 16)]
                    remote(slab, part["ray"].at[k - 1], r1s.at[0], r1r.at[0], y_k * 2 + core, seq).start()
                for p in "xz":
                    piece = both[:, :, FIRST[p] : FIRST[p] + WIDTH[p]]
                    for x in range(4):
                        if p == "x":
                            part["sbx"][pl.ds(x * 16 + y_k * 4, 4)] = piece[4 * x : 4 * x + 4]
                        else:
                            for z in range(4):
                                part["sbz"][z * 16 + x * 4 + y_k] = piece[4 * x + z]
        for n, p in ((1, "x"), (2, "z")):
            for k in range(1, 4):
                d, s, c = line_peer(p, k)
                slab = part["sb" + p].at[pl.ds(c * 16, 16)]
                remote(slab, part["ra" + p].at[k - 1], r1s.at[n], r1r.at[n], d, s).start()

        def scatter_plane():
            for p in "xzy":
                n = PARTS.index(p)
                got, mid, dst = part["ra" + p], part["mid" + p], part["rb" + p]
                remote(got, got, r1s.at[n], r1r.at[n], partner, seq).wait_recv()
                value = part["sb" + p][pl.ds(place[p] * 16, 16)].astype(f32)
                for k in range(3):
                    value = value + got[k].astype(f32)
                mid[...] = value.astype(bf16)
                here = mine_in[p] % 16
                for a, b in plane_far:
                    d, s, q = plane_peer(p, a, b)
                    remote(mid.at[q], dst.at[here], r2s.at[n], r2r.at[n], d, s).start()
                dst[here] = mid[here]

        def inside_back(c, carry):
            s = dec_s[rows(c)]
            s_t = s.T
            scores = sc[c].T
            for p in range(PAIRS):
                parts = []
                for h in (2 * p, 2 * p + 1):
                    gap = jnp.minimum(s_t[h : h + 1, :] - s[:, h : h + 1], 0.0)
                    parts.append((jnp.exp(gap) * scores).astype(bf16))
                mine = gb[rows(c), 128 * p : 128 * (p + 1)]
                both = jnp.concatenate([mine * low_half, mine * high_half], axis=0)
                lanes = slice(128 * p, 128 * (p + 1))
                eexp[rows(c), lanes] = dot(jnp.concatenate(parts, axis=1), both)
            ds1[rows(c)] = head_sum(gb[rows(c)].astype(f32) * yin[rows(c)])
            q2a[rows(c)] = head_sum(xw[rows(c)].astype(f32) * eexp[rows(c)])
            return carry

        lax.fori_loop(0, CHUNKS, inside_back, 0)

        for h in range(2):
            recv_wait(gr.at[h], 3, 15, h)
            scan(gr, gp, h, range(N_SEQ - 1, -1, -1))
            exchange_start(gp, gi, 5, h)

        scatter_plane()

        def summed(ref, count):
            value = ref[0]
            for k in range(1, count):
                value = value + ref[k]
            return value

        recv_wait(sar, 4, 15)
        sb2[...] = summed(sar, N_SEQ)
        cross_start(sb2, sbr, 6)

        for h in range(2):
            recv_wait(gi.at[h], 5, 15, h)

        def put_after(at_rows, lanes, value):
            apart[3, at_rows, lanes] = value

        from_blocks(gi, put_after)
        apart[2] = apart[2] + chain[2:3] * apart[3]
        apart[1] = apart[1] + chain[1:2] * apart[2]

        def back(c, sums):
            dec_g, bias_g = sums
            after = apart[c + 1]
            width = wid[rows(c)]
            z_t = dot(bc_ref[rows(c), :STATE], after.astype(bf16))
            q2 = q2a[rows(c)] + head_sum(wtd[rows(c)].astype(f32) * z_t)
            ends = jnp.sum((after * hst[c + 1]).reshape(16, 8, WIDE), axis=0)
            end_h = jnp.sum(head_sum(ends), axis=0, keepdims=True)
            d_s = ds1[rows(c)] - q2
            d_a = lax.dot_general(
                tri[...], d_s, (((0,), (0,)), ((), ())), precision=highest, preferred_element_type=f32
            ) + end_h
            d_w = q2 / width - rate * d_a
            pre = rawt[rows(c)] + bias_t
            sig = 1.0 / (1.0 + jnp.exp(-pre))
            dec_g = dec_g - jnp.sum(d_a * (rate * width), axis=0, keepdims=True)
            bias_g = bias_g + jnp.sum(d_w * sig, axis=0, keepdims=True)
            return dec_g, bias_g

        zero_row = jnp.zeros((1, 128), f32)
        dec_g, bias_g = lax.fori_loop(0, CHUNKS, back, (zero_row, zero_row))

        recv_wait(sbr, 6, 7)
        sums_a = summed(sbr, N_DP)

        ag_sent()

        grad, square = {}, jnp.zeros((1, 1), f32)
        for n, p in enumerate(PARTS):
            dst = part["rb" + p]
            got = dst.at[pl.ds(0, 15)]
            remote(got, got, r2s.at[n], r2r.at[n], partner, seq).wait_recv()
            value = dst[0].astype(f32)
            for q in range(1, 16):
                value = value + dst[q].astype(f32)
            grad[p] = value
            square = square + jnp.sum(jnp.sum(value * value, axis=1, keepdims=True), axis=0, keepdims=True)
        t1[...] = jnp.where(lane < 16, dec_g, jnp.where(lane < 32, bias_g, jnp.where(lane == 32, square, 0.0)))
        pair = remote(t1, t1r, s_send.at[7, 0], s_recv.at[7, 0], partner, seq)
        pair.start()
        pair.wait_recv()
        t2[...] = t1[...] + t1r[...]

        for a, b, c in far_first:
            remote(t2, t2r.at[own_q], s_send.at[8, 0], s_recv.at[8, 0], dps[a], seqs[b, c]).start()
        t2r[own_q] = t2[...]
        recv_wait(t2r, 8, 63)
        sums_b = jnp.sum(t2r[...], axis=0)

        def heads_at(first):
            picked = jnp.where((lane >= first) & (lane < first + 16), sums_b, 0.0)
            return jnp.dot(jnp.broadcast_to(picked, (8, 128)), spread, precision=highest, preferred_element_type=f32)[0:1]

        dec_g, bias_g = heads_at(0), heads_at(16)
        squares = jnp.sum(jnp.where(lane == 32, sums_b, 0.0), axis=1, keepdims=True)
        gain_rows, skip_g, loss_all = sums_a[0:8], sums_a[8:9], sums_a[9:10]
        small = jnp.sum(
            jnp.where(lane < HEADS, dec_g * dec_g + bias_g * bias_g + skip_g * skip_g, 0.0), axis=1, keepdims=True
        )
        gains = jnp.sum(jnp.sum(gain_rows * gain_rows, axis=1, keepdims=True), axis=0, keepdims=True)
        norm = jnp.sqrt(squares + (small + gains))
        move = learn_rate * (clip_limit / jnp.maximum(norm, clip_limit))
        par[0] = jnp.broadcast_to(dec_t - move * dec_g, (8, 128))
        par[1] = jnp.broadcast_to(bias_t - move * bias_g, (8, 128))
        par[2] = jnp.broadcast_to(skip_t - move * skip_g, (8, 128))
        for r in range(8):
            lanes = slice(128 * r, 128 * (r + 1))
            gain[:, lanes] = gain[:, lanes] - move * gain_rows[r : r + 1]
        for p in PARTS:
            for h in range(2):
                lanes = slice(HALF * h + FIRST[p], HALF * h + FIRST[p] + WIDTH[p])
                wown[:, lanes] = wown[:, lanes] - move * grad[p][8 * h : 8 * h + 8]

        for h in range(2):
            send_wait(hr.at[h], 0, 15, h)
        send_wait(cr, 1, 15)
        for h in range(2):
            send_wait(hi.at[h], 2, 15, h)
        for h in range(2):
            send_wait(gr.at[h], 3, 15, h)
        send_wait(sar, 4, 15)
        for h in range(2):
            send_wait(gi.at[h], 5, 15, h)
        send_wait(sbr, 6, 7)
        pair.wait_send()
        send_wait(t2r, 8, 63)
        for k in range(N_Y):
            remote(wgp.at[k], pr.at[k], s_ps.at[k], s_pr.at[k], partner, seq).wait_send()
        for n, p in enumerate(PARTS):
            got, dst = part["ra" + p], part["rb" + p].at[pl.ds(0, 15)]
            remote(got, got, r1s.at[n], r1r.at[n], partner, seq).wait_send()
            remote(dst, dst, r2s.at[n], r2r.at[n], partner, seq).wait_send()

        @pl.when(step == 0)
        def _():
            ag_start()

        step_loss = loss_all[:, 0:1] * (1.0 / WIDE) / total_f
        return jnp.where(iota((1, STEPS), 1) == step, step_loss, losses)

    losses = lax.fori_loop(0, STEPS, one_step, jnp.zeros((1, STEPS), f32))
    packed_out[0:8] = wown[...]
    packed_out[8:9] = gain[...]
    packed_out[9:10, :] = jnp.zeros((1, WIDE), f32)
    for n in range(3):
        packed_out[9:10, 128 * n : 128 * (n + 1)] = par[n, 0:1]
    packed_out[9:10, 384 : 384 + STEPS] = losses


def split_kernel(packed, loss_out, w_out, dec_out, bias_out, skip_out, gain_out):
    w_out[...] = packed[0:8]
    gain_out[...] = packed[8:9]
    dec_out[...] = packed[9:10, 0:HEADS]
    bias_out[...] = packed[9:10, 128 : 128 + HEADS]
    skip_out[...] = packed[9:10, 256 : 256 + HEADS]
    loss_out[...] = packed[9:10, 384 : 384 + STEPS]


def per_device(x, z, bc, raw, ids, counts, target, weight, dec, bias, skip, gain):
    vmem = pl.BlockSpec(memory_space=pltpu.VMEM)
    smem = pl.BlockSpec(memory_space=pltpu.SMEM)
    anywhere = pl.BlockSpec(memory_space=pl.ANY)
    shape = jax.ShapeDtypeStruct
    packed = pl.pallas_call(
        kernel,
        out_shape=shape((16, WIDE), f32),
        in_specs=[anywhere] * 3 + [vmem] * 2 + [smem] + [anywhere] + [vmem] * 5,
        out_specs=vmem,
        scratch_shapes=list(scratch().values()),
        compiler_params=pltpu.CompilerParams(
            collective_id=0, has_side_effects=True, vmem_limit_bytes=62 * 1024 * 1024
        ),
    )(
        x[0], z[0], bc[0], raw[0].T, ids, counts, target[0], weight,
        dec.reshape(1, HEADS), bias.reshape(1, HEADS), skip.reshape(1, HEADS), gain.reshape(1, WIDE),
    )
    losses, weight, dec, bias, skip, gain = pl.pallas_call(
        split_kernel,
        out_shape=(
            shape((1, STEPS), f32), shape((8, WIDE), f32), shape((1, HEADS), f32), shape((1, HEADS), f32),
            shape((1, HEADS), f32), shape((1, WIDE), f32),
        ),
        in_specs=[vmem],
        out_specs=(vmem,) * 6,
    )(packed)
    return (
        losses.reshape(STEPS), weight, dec.reshape(HEADS), bias.reshape(HEADS), skip.reshape(HEADS), gain.reshape(WIDE)
    )


def solution(mesh):
    tokens = P(DP, SEQ, None)
    return jax.shard_map(
        per_device,
        mesh=mesh,
        in_specs=(
            tokens, tokens, tokens, tokens, P(DP, SEQ), P(), tokens, P((DP, SEQ), None), P(), P(), P(), P(),
        ),
        out_specs=(P(), P((DP, SEQ), None), P(), P(), P(), P()),
        check_vma=False,
    )
```

```python
import jax
import jax.numpy as jnp
from jax import lax
from jax.experimental import pallas as pl
from jax.experimental.pallas import tpu as pltpu
from jax.sharding import PartitionSpec as P

STEPS = 2
DP, SEQ = "dp", "seq"
N_DP, N_SEQ, N_Y = 8, 16, 4
TOK, WIDE, STATE, HEADS, HEAD = 384, 1024, 128, 16, 64
CHUNK, CHUNKS, PAIRS = 128, 3, 8
HALF = WIDE // 2

norm_floor = 1.0
clip_limit = 1.0
learn_rate = 8.0
f32, bf16 = jnp.float32, jnp.bfloat16
highest = lax.Precision.HIGHEST


def dot(a, b):
    return jnp.dot(a, b, preferred_element_type=f32)


def dot_tn(a, b):
    return lax.dot_general(a, b, (((0,), (0,)), ((), ())), preferred_element_type=f32)


def dot_nt(a, b):
    return lax.dot_general(a, b, (((1,), (1,)), ((), ())), preferred_element_type=f32)


def iota(shape, dim):
    return lax.broadcasted_iota(jnp.int32, shape, dim)


def three_parts(v):
    high = v.astype(bf16).astype(f32)
    rest = v - high
    mid = rest.astype(bf16).astype(f32)
    low = rest - mid
    group = (iota(v.shape, 1) >> 4) & 3
    zero = jnp.zeros_like(v)
    return jnp.where(
        group == 0, high, jnp.where(group == 1, mid, jnp.where(group == 2, low, zero))
    ).astype(bf16)


def blocks_of(rows):
    left = rows[:, :HALF].reshape(N_SEQ, 1, 8, HALF)
    right = rows[:, HALF:].reshape(N_SEQ, 1, 8, HALF)
    return jnp.concatenate([left, right], axis=1).reshape(N_SEQ, 16, HALF)


def rows_of(blocks):
    count = blocks.shape[0]
    split = blocks.reshape(count, 2, 8, HALF)
    return split[:, 0].reshape(count * 8, HALF), split[:, 1].reshape(count * 8, HALF)


INPUTS = (
    "x_in", "z_in", "bc_in", "raw_in", "ids_ref", "cnt_ref", "tgt_in", "w_ref", "dec_in", "bias_in", "skip_in", "gain_in",
)
OUTPUTS = ("packed_out",)
PARTS = "yxz"
WIDTH = {"y": 256, "x": 128, "z": 128}
FIRST = {"y": 0, "x": 256, "z": 384}


def scratch():
    dma, v = pltpu.SemaphoreType.DMA, pltpu.VMEM
    rows_f, wide_f, wide_b = v((TOK, 128), f32), v((TOK, WIDE), f32), v((TOK, WIDE), bf16)
    states, sixteen = v((CHUNKS + 1, STATE, WIDE), f32), v((2, N_SEQ, 16, HALF // 2), bf16)
    small, small16, small8 = v((16, 128), f32), v((N_SEQ, 16, 128), f32), v((N_DP, 16, 128), f32)
    named = dict(
        x_ref=wide_b, z_ref=wide_b, bc_ref=v((TOK, 2 * STATE), bf16), tgt_ref=wide_b, s_in=dma((4,)),
        act=wide_f, gat=wide_f, dnf=wide_f, gdn=wide_f, invs=rows_f,
        ex=v((128, WIDE), bf16), red=v((WIDE, 128), bf16), tri=v((CHUNK, CHUNK), f32), par=v((3, 8, 128), f32),
        gain=v((1, WIDE), f32), wown=v((8, WIDE), f32), rawt=rows_f, wid=rows_f, dec_s=rows_f, ent=rows_f,
        chain=v((8, WIDE), f32), fcol=v((CHUNKS, CHUNK, CHUNK), f32), sc=v((CHUNKS, CHUNK, CHUNK), f32),
        xw=wide_b, wtd=wide_b, yin=wide_f, eexp=wide_f, gstate=v((CHUNKS, STATE, WIDE), f32), hst=states, apart=states,
        normb=wide_b, ogb=wide_b, gb=wide_b, q2a=rows_f, ds1=rows_f, accs=v((2, 8, WIDE), f32),
        hs=sixteen, hr=sixteen, hp=sixteen, hi=sixteen, gs=sixteen, gr=sixteen, gp=sixteen, gi=sixteen,
        cs=v((8, 128), f32), cr=v((N_SEQ, 8, 128), f32), wfull=v((WIDE, WIDE), bf16),
        wgp=v((N_Y, N_SEQ, 16, HALF), bf16), pr=v((N_Y, N_SEQ, 16, HALF), bf16),
        sa=small, sar=small16, sb2=small, sbr=small8, t1=v((1, 128), f32),
        t2r=v((128, 1, 128), f32),
    )
    for p in PARTS:
        w = WIDTH[p]
        named["ag" + p] = v((128, 16, w), bf16)
        named["sb" + p] = v((64, 16, w), bf16)
        named["ra" + p] = v((3, N_SEQ, 16, w), bf16)
        named["mid" + p] = v((N_SEQ, 16, w), bf16)
        named["rb" + p] = v((N_SEQ, 16, w), bf16)
    for name, count in dict(s_ps=4, s_pr=4, g1s=3, g1r=3, g2s=3, g2r=3, g3s=3, g3r=3, r1s=3, r1r=3, r2s=3, r2r=3).items():
        named[name] = dma((count,))
    named["s_send"] = dma((9, 2))
    named["s_recv"] = dma((9, 2))
    return named


def kernel(*refs):
    names = INPUTS + OUTPUTS + tuple(scratch())
    assert len(names) == len(refs)
    program(**dict(zip(names, refs)))


def program(
    x_in, z_in, bc_in, raw_in, ids_ref, cnt_ref, tgt_in, w_ref, dec_in, bias_in, skip_in, gain_in,
    packed_out, x_ref, z_ref, bc_ref, tgt_ref, s_in, act, gat, dnf, gdn, invs,
    ex, red, tri, par, gain, wown, rawt, wid, dec_s, ent, chain, fcol, sc,
    xw, wtd, yin, eexp, gstate, hst, apart, normb, ogb, gb, q2a, ds1, accs,
    hs, hr, hp, hi, gs, gr, gp, gi, cs, cr, wfull, wgp, pr, sa, sar, sb2, sbr, t1, t2r,
    s_send, s_recv, s_ps, s_pr, g1s, g1r, g2s, g2r, g3s, g3r, r1s, r1r, r2s, r2r, **part,
):
    dp, seq = lax.axis_index(DP), lax.axis_index(SEQ)
    yy, core = dp // 2, dp % 2
    partner = dp + 1 - 2 * core
    own_b = dp * N_SEQ + seq
    xx, zz = seq // 4, seq % 4
    place = {"y": yy, "x": xx, "z": zz}
    MESH = pl.DeviceIdType.MESH

    def at(d, s):
        return {DP: d, SEQ: s}

    def remote(src, dst, ss, rs, d, s):
        return pltpu.make_async_remote_copy(
            src_ref=src, dst_ref=dst, send_sem=ss, recv_sem=rs, device_id=at(d, s), device_id_type=MESH
        )

    barrier = pltpu.get_barrier_semaphore()

    dps = [((yy + k) % 4) * 2 + core for k in range(4)]
    seqs = {(a, b): ((xx + a) % 4) * 4 + (zz + b) % 4 for a in range(4) for b in range(4)}

    def hops(offset):
        return sum(min(k, 4 - k) for k in offset)

    chips = [(a, b, c) for a in range(4) for b in range(4) for c in range(4)]
    far_first = sorted(chips[1:], key=lambda offset: -hops(offset))
    everyone = []
    for a, b, c in far_first + chips[:1]:
        for flip in (0, 1):
            if (a, b, c, flip) != (0, 0, 0, 0):
                everyone.append((dps[a] + flip * (1 - 2 * core), seqs[b, c]))
    for d, s in everyone:
        pl.semaphore_signal(barrier, 1, device_id=at(d, s), device_id_type=MESH)
    loads = [
        pltpu.make_async_copy(source, target, s_in.at[n])
        for n, (source, target) in enumerate(((bc_in, bc_ref), (x_in, x_ref), (z_in, z_ref), (tgt_in, tgt_ref)))
    ]
    for load in loads:
        load.start()

    row = iota((CHUNK, WIDE), 0)
    col = iota((CHUNK, WIDE), 1)
    ex[...] = jnp.where(((row & 15) == (col >> 6)) & (row < 48), 1.0, 0.0).astype(bf16)
    rrow = iota((WIDE, 128), 0)
    rcol = iota((WIDE, 128), 1)
    red[...] = jnp.where((rrow >> 6) == (rcol & 15), 1.0, 0.0).astype(bf16)
    ti, tj = iota((CHUNK, CHUNK), 0), iota((CHUNK, CHUNK), 1)
    tri[...] = jnp.where(ti >= tj, 1.0, 0.0)
    rep = jnp.where(iota((HEADS, 128), 0) == (iota((HEADS, 128), 1) & 15), 1.0, 0.0)

    spread = jnp.where((iota((128, 128), 0) & 15) == (iota((128, 128), 1) & 15), 1.0, 0.0)

    def tiled(ref):
        return jnp.dot(jnp.broadcast_to(ref[...], (8, HEADS)), rep, precision=highest, preferred_element_type=f32)

    par[0] = tiled(dec_in)
    par[1] = tiled(bias_in)
    par[2] = tiled(skip_in)
    gain[...] = gain_in[...]
    wown[...] = w_ref[...]
    rawt[...] = lax.dot_general(
        raw_in[...], rep, (((0,), (0,)), ((), ())), precision=highest, preferred_element_type=f32
    )
    loads[0].wait()

    def expand(v):
        return dot(three_parts(v), ex[...])

    def head_sum(v):
        high = v.astype(bf16)
        low = (v - high.astype(f32)).astype(bf16)
        return dot(high, red[...]) + dot(low, red[...])

    lane = iota((1, 128), 1)
    low_half = jnp.where(lane < HEAD, 1.0, 0.0).astype(bf16)
    high_half = jnp.where(lane < HEAD, 0.0, 1.0).astype(bf16)

    total = cnt_ref[0]
    for k in range(1, N_DP):
        total = total + cnt_ref[k]
    total_f = total.astype(f32)
    own_count = cnt_ref[dp]

    def rows(c):
        return pl.ds(pl.multiple_of(c * CHUNK, CHUNK), CHUNK)

    def prepare(c, carry):
        flag = jnp.where(ids_ref[0:1, rows(c)] == 0, 1.0, 0.0)
        flag_col = jnp.broadcast_to(flag, (CHUNK, CHUNK)).T
        seg = dot(tri[...], flag_col)
        fcol[c] = seg
        return carry

    lax.fori_loop(0, CHUNKS, prepare, 0)
    loads[1].wait()

    def index_in(p, y, x, z):
        return {"y": y * 16 + x * 4 + z, "x": x * 16 + y * 4 + z, "z": z * 16 + x * 4 + y}[p]

    plane_far = sorted([(a, b) for a in range(4) for b in range(4)][1:], key=lambda offset: -hops(offset))

    def plane_peer(p, a, b):
        if p == "y":
            return dp, seqs[a, b], seqs[a, b]
        if p == "x":
            return dps[a], seqs[0, b], ((yy + a) % 4) * 4 + (zz + b) % 4
        return dps[b], seqs[a, 0], ((xx + a) % 4) * 4 + (yy + b) % 4

    def line_peer(p, k):
        c = (place[p] + k) % 4
        if p == "y":
            return c * 2 + core, seq, c
        if p == "x":
            return dp, c * 4 + zz, c
        return dp, xx * 4 + c, c

    mine_in = {p: index_in(p, yy, xx, zz) for p in PARTS}

    def ag_start():
        for n, p in enumerate(PARTS):
            buf = part["ag" + p]
            lanes = slice(FIRST[p], FIRST[p] + WIDTH[p])
            right = slice(HALF + FIRST[p], HALF + FIRST[p] + WIDTH[p])
            own = core * 64 + mine_in[p]
            buf[own] = jnp.concatenate([wown[:, lanes], wown[:, right]], axis=0).astype(bf16)

            for a, b in plane_far:
                d, s, _ = plane_peer(p, a, b)
                remote(buf.at[own], buf.at[own], g1s.at[n], g1r.at[n], d, s).start()

    def ag_line():
        for n, p in enumerate(PARTS):
            buf = part["ag" + p]
            piece = buf.at[pl.ds(0, 15)]
            remote(piece, piece, g1s.at[n], g1r.at[n], partner, seq).wait_recv()
            slab = buf.at[pl.ds(core * 64 + place[p] * 16, 16)]
            for k in range(1, 4):
                d, s, _ = line_peer(p, k)
                remote(slab, slab, g2s.at[n], g2r.at[n], d, s).start()

    def unpack(p, its_core):
        buf, w, base = part["ag" + p], WIDTH[p], its_core * 64

        def one(y, carry):
            d = y * 2 + its_core
            if p == "y":
                blocks = [buf[pl.ds(base + y * 16, 16)].astype(f32)]
            elif p == "x":
                blocks = [buf[pl.ds(base + x * 16 + y * 4, 4)].astype(f32) for x in range(4)]
            else:
                blocks = [buf[pl.ds(base + z * 16 + x * 4 + y, 1)].astype(f32) for x in range(4) for z in range(4)]
            tops, lows = [], []
            for block in blocks:
                split = block.reshape(block.shape[0], 2, 8, w)
                tops.append(split[:, 0].reshape(-1, w))
                lows.append(split[:, 1].reshape(-1, w))
            wfull[rows(d), FIRST[p] : FIRST[p] + w] = jnp.concatenate(tops, axis=0).astype(bf16)
            wfull[rows(d), HALF + FIRST[p] : HALF + FIRST[p] + w] = jnp.concatenate(lows, axis=0).astype(bf16)
            return carry

        lax.fori_loop(0, N_Y, one, 0)

    def ag_finish():
        for p in "xzy":
            n, buf = PARTS.index(p), part["ag" + p]
            piece = buf.at[pl.ds(0, 48)]
            remote(piece, piece, g2s.at[n], g2r.at[n], partner, seq).wait_recv()
            ours = buf.at[pl.ds(core * 64, 64)]
            remote(ours, ours, g3s.at[n], g3r.at[n], partner, seq).start()
            unpack(p, core)
        for p in "xzy":
            n, buf = PARTS.index(p), part["ag" + p]
            piece = buf.at[pl.ds((1 - core) * 64, 64)]
            remote(piece, piece, g3s.at[n], g3r.at[n], partner, seq).wait_recv()
            unpack(p, 1 - core)

    def ag_sent():
        for n, p in enumerate(PARTS):
            buf = part["ag" + p]
            for count, ss, rs in ((15, g1s, g1r), (48, g2s, g2r), (64, g3s, g3r)):
                piece = buf.at[pl.ds(0, count)]
                remote(piece, piece, ss.at[n], rs.at[n], partner, seq).wait_send()

    def exchange_start(src, dst, n, h):
        for a, b in plane_far:
            peer = seqs[a, b]
            remote(src.at[h, peer], dst.at[h, seq], s_send.at[n, h], s_recv.at[n, h], dp, peer).start()
        dst[h, seq] = src[h, seq]

    def spread_start(src, dst, n):
        for a, b in plane_far:
            remote(src, dst.at[seq], s_send.at[n, 0], s_recv.at[n, 0], dp, seqs[a, b]).start()
        dst[seq] = src[...]

    def cross_start(src, dst, n):
        for k in range(1, N_DP):
            remote(src, dst.at[dp], s_send.at[n, 0], s_recv.at[n, 0], (dp + k) % N_DP, seq).start()
        dst[dp] = src[...]

    def recv_wait(dst, n, count, h=0):
        piece = dst.at[pl.ds(0, count)]
        remote(piece, piece, s_send.at[n, h], s_recv.at[n, h], partner, seq).wait_recv()

    def send_wait(dst, n, count, h=0):
        piece = dst.at[pl.ds(0, count)]
        remote(piece, piece, s_send.at[n, h], s_recv.at[n, h], partner, seq).wait_send()

    def one_step(step, losses):
        dec_t, bias_t, skip_t = par[0, 0:1], par[1, 0:1], par[2, 0:1]
        rate = jnp.exp(dec_t)

        pre = rawt[...] + bias_t
        u = jnp.exp(-jnp.abs(pre))
        v = 1.0 + u
        log1p = jnp.where(v == 1.0, u, jnp.log(v) * u / jnp.where(v == 1.0, 1.0, v - 1.0))
        widths = jnp.maximum(pre, 0.0) + log1p
        wid[...] = widths
        sub8, lane8 = iota((8, 128), 0), iota((8, 128), 1)
        through = jnp.zeros((8, 128), f32)
        carried = jnp.ones((1, 128), f32)
        for c in range(CHUNKS):
            span = slice(c * CHUNK, (c + 1) * CHUNK)
            seg = fcol[c]
            width = widths[span]
            s = jnp.dot(tri[...], -rate * width, precision=highest, preferred_element_type=f32)
            last = s[CHUNK - 1 : CHUNK]
            seg_last = seg[CHUNK - 1 : CHUNK]
            leaving = jnp.exp(last - s) * jnp.where(seg == seg_last, 1.0, 0.0)
            passing = jnp.exp(last) * jnp.where(seg_last == 0.0, 1.0, 0.0)
            dec_s[span] = s
            ent[span] = jnp.exp(s) * jnp.where(seg == 0.0, 1.0, 0.0)
            weighted = (x_ref[span].astype(f32) * expand(width * leaving)).astype(bf16)
            wtd[span] = weighted
            gstate[c] = dot_tn(bc_ref[span, :STATE], weighted)
            through = jnp.where(sub8 == c, passing, through)
            carried = carried * passing
        chain[...] = expand(through)
        wide8 = jnp.broadcast_to(carried, (8, 128))
        even = jnp.sum(jnp.where(lane8 == 2 * sub8, wide8, 0.0), axis=1, keepdims=True)
        odd = jnp.sum(jnp.where(lane8 == 2 * sub8 + 1, wide8, 0.0), axis=1, keepdims=True)
        cs[...] = jnp.where(lane8 < HEAD, even, odd)
        hst[0] = gstate[2] + chain[2:3] * (gstate[1] + chain[1:2] * gstate[0])

        def to_blocks(state, out):
            for r in range(8):
                for h in range(2):
                    for q in range(2):
                        first = HALF * h + 256 * q
                        out[q, 2 * r + h] = state[16 * r : 16 * r + 16, first : first + 256].astype(bf16)

        def from_blocks(source, put):
            for q in range(2):
                for r in range(8):
                    for h in range(2):
                        first = HALF * h + 256 * q
                        put(slice(16 * r, 16 * r + 16), slice(first, first + 256), source[q, 2 * r + h].astype(f32))

        to_blocks(hst[0], hs)

        @pl.when(step == 0)
        def _():
            pl.semaphore_wait(barrier, 127)
            ag_start()

        exchange_start(hs, hr, 0, 0)
        spread_start(cs, cr, 1)
        exchange_start(hs, hr, 0, 1)

        @pl.when(step == 0)
        def _():
            loads[2].wait()

            def once(c, carry):
                z_f = z_ref[rows(c)].astype(f32)
                act[rows(c)] = z_f / (1.0 + jnp.exp(-z_f))
                scores = dot_nt(bc_ref[rows(c), STATE:], bc_ref[rows(c), :STATE])
                sc[c] = jnp.where((fcol[c] == fcol[c].T) & (ti >= tj), scores, 0.0)
                return carry

            lax.fori_loop(0, CHUNKS, once, 0)
            loads[3].wait()

        skip_e = expand(jnp.broadcast_to(skip_t, (8, 128)))[0:1]
        gain_e = gain[...]

        def inside(c, carry):
            s = dec_s[rows(c)]
            s_t = s.T
            scores = sc[c]
            xw[rows(c)] = (x_ref[rows(c)].astype(f32) * expand(wid[rows(c)])).astype(bf16)
            eexp[rows(c)] = expand(ent[rows(c)])
            for p in range(PAIRS):
                parts = []
                for h in (2 * p, 2 * p + 1):
                    gap = jnp.minimum(s[:, h : h + 1] - s_t[h : h + 1, :], 0.0)
                    parts.append((jnp.exp(gap) * scores).astype(bf16))
                mine = xw[rows(c), 128 * p : 128 * (p + 1)]
                both = jnp.concatenate([mine * low_half, mine * high_half], axis=0)
                lanes = slice(128 * p, 128 * (p + 1))
                direct = skip_e[:, lanes] * x_ref[rows(c), lanes].astype(f32)
                yin[rows(c), lanes] = dot(jnp.concatenate(parts, axis=1), both) + direct
            return carry

        lax.fori_loop(0, CHUNKS, inside, 0)
        ag_line()

        half = seq % 2

        def scan(source, out, h, order):
            state = [jnp.zeros((16, 128), f32) for _ in range(2)]
            for i in order:
                for m in range(2):
                    lanes = slice(128 * m, 128 * (m + 1))
                    out[h, i, :, lanes] = state[m].astype(bf16)
                    factor = cr[i, pl.ds(4 * half + 2 * h + m, 1), :]
                    state[m] = factor * state[m] + source[h, i, :, lanes].astype(f32)

        recv_wait(cr, 1, 15)
        for h in range(2):
            recv_wait(hr.at[h], 0, 15, h)
            scan(hr, hp, h, range(N_SEQ))
            exchange_start(hp, hi, 2, h)
        ag_finish()
        for h in range(2):
            recv_wait(hi.at[h], 2, 15, h)

        def put_state(at_rows, lanes, value):
            hst[0, at_rows, lanes] = value

        from_blocks(hi, put_state)

        scale = 2.0 / (WIDE * total_f)
        accs[...] = jnp.zeros(accs.shape, f32)

        for c in range(CHUNKS):
            span = slice(c * CHUNK, (c + 1) * CHUNK)
            state = hst[c]
            y = yin[span] + eexp[span] * dot(bc_ref[span, STATE:], state.astype(bf16))
            yin[span] = y
            gated = y * act[span]
            gat[span] = gated
            inv = lax.rsqrt(jnp.sum(gated * gated, axis=1, keepdims=True) * (1.0 / WIDE) + norm_floor)
            invs[span] = jnp.broadcast_to(inv, (CHUNK, 128))
            normb[span] = (gated * gain_e * inv).astype(bf16)
            hst[c + 1] = chain[c : c + 1] * state + gstate[c]
        block = 512
        position = seq * TOK + iota((TOK, block), 0)
        scored = jnp.where(position < own_count, 1.0, 0.0)
        losses_8 = jnp.zeros((8, block), f32)
        for first in range(0, WIDE, block):
            lanes = slice(first, first + block)
            res = (dot(normb[...], wfull[:, lanes]) - tgt_ref[:, lanes].astype(f32)) * scored
            losses_8 = losses_8 + jnp.sum((res * res).reshape(TOK // 8, 8, block), axis=0)
            ogb[:, lanes] = (res * scale).astype(bf16)
        loss = jnp.sum(jnp.sum(losses_8, axis=1, keepdims=True), axis=0, keepdims=True)
        inner_l = jnp.zeros((TOK, 128), f32)
        for first in range(0, WIDE, block):
            lanes = slice(first, first + block)
            d_norm = dot_nt(ogb[...], wfull[lanes, :])
            dnf[:, lanes] = d_norm
            d_gain = d_norm * gain_e[:, lanes]
            gdn[:, lanes] = d_gain
            term = d_gain * gat[:, lanes]
            for k in range(0, block, 128):
                inner_l = inner_l + term[:, k : k + 128]
        inner = jnp.sum(inner_l, axis=1, keepdims=True) * (1.0 / WIDE)
        for c in range(CHUNKS):
            span = slice(c * CHUNK, (c + 1) * CHUNK)
            inv = invs[span, 0:1]
            g = (gdn[span] - gat[span] * (inv * inv * inner[span])) * inv * act[span]
            gb[span] = g.astype(bf16)
            apart[c] = dot_tn(bc_ref[span, STATE:], (g * eexp[span]).astype(bf16))
        entry = apart[0] + chain[0:1] * (apart[1] + chain[1:2] * apart[2])
        to_blocks(entry, gs)
        for h in range(2):
            exchange_start(gs, gr, 3, h)
        def grad_rows(first, second):
            lanes = [normb[:, pl.ds(pl.multiple_of(d * 128, 128), 128)] for d in (first, second)]
            both = dot_tn(jnp.concatenate(lanes, axis=1), ogb[...])
            return blocks_of(both[:128]), blocks_of(both[128:])

        def group(k, c):
            return ((yy + k) % N_Y) * 2 + c

        for pair in ((1, 2), (3, 0)):
            pieces = grad_rows(*[group(k, 1 - core) for k in pair])
            for k, piece in zip(pair, pieces):
                wgp[k] = piece.astype(bf16)
                remote(wgp.at[k], pr.at[k], s_ps.at[k], s_pr.at[k], partner, seq).start()
        def small_sums(c, carry):
            x_f, inv = x_ref[rows(c)].astype(f32), invs[rows(c), 0:1]
            accs[0] += jnp.sum((dnf[rows(c)] * gat[rows(c)] * inv).reshape(16, 8, WIDE), axis=0)
            accs[1] += jnp.sum((gb[rows(c)].astype(f32) * x_f).reshape(16, 8, WIDE), axis=0)
            return carry

        lax.fori_loop(0, CHUNKS, small_sums, 0)
        gain_g = jnp.sum(accs[0], axis=0, keepdims=True)
        for r in range(8):
            sa[r : r + 1, :] = gain_g[:, 128 * r : 128 * (r + 1)]
        skip_g = head_sum(jnp.broadcast_to(jnp.sum(accs[1], axis=0, keepdims=True), (8, WIDE)))
        sub = iota((8, 128), 0)
        sa[8:16, :] = jnp.where(sub == 0, skip_g, jnp.where(sub == 1, jnp.broadcast_to(loss, (8, 128)), 0.0))
        spread_start(sa, sar, 4)
        for pair in ((1, 2), (3, 0)):
            pieces = grad_rows(*[group(k, core) for k in pair])
            for k, mine in zip(pair, pieces):
                y_k = (yy + k) % N_Y
                remote(wgp.at[k], pr.at[k], s_ps.at[k], s_pr.at[k], partner, seq).wait_recv()
                both = (mine + pr[k].astype(f32)).astype(bf16)
                part["sby"][pl.ds(y_k * 16, 16)] = both[:, :, : WIDTH["y"]]
                if k > 0:
                    slab = part["sby"].at[pl.ds(y_k * 16, 16)]
                    remote(slab, part["ray"].at[k - 1], r1s.at[0], r1r.at[0], y_k * 2 + core, seq).start()
                for p in "xz":
                    piece = both[:, :, FIRST[p] : FIRST[p] + WIDTH[p]]
                    for x in range(4):
                        if p == "x":
                            part["sbx"][pl.ds(x * 16 + y_k * 4, 4)] = piece[4 * x : 4 * x + 4]
                        else:
                            for z in range(4):
                                part["sbz"][z * 16 + x * 4 + y_k] = piece[4 * x + z]
        for n, p in ((1, "x"), (2, "z")):
            for k in range(1, 4):
                d, s, c = line_peer(p, k)
                slab = part["sb" + p].at[pl.ds(c * 16, 16)]
                remote(slab, part["ra" + p].at[k - 1], r1s.at[n], r1r.at[n], d, s).start()

        def scatter_plane():
            for p in "xzy":
                n = PARTS.index(p)
                got, mid, dst = part["ra" + p], part["mid" + p], part["rb" + p]
                remote(got, got, r1s.at[n], r1r.at[n], partner, seq).wait_recv()
                value = part["sb" + p][pl.ds(place[p] * 16, 16)].astype(f32)
                for k in range(3):
                    value = value + got[k].astype(f32)
                mid[...] = value.astype(bf16)
                here = mine_in[p] % 16
                for a, b in plane_far:
                    d, s, q = plane_peer(p, a, b)
                    remote(mid.at[q], dst.at[here], r2s.at[n], r2r.at[n], d, s).start()
                dst[here] = mid[here]

        def inside_back(c, carry):
            s = dec_s[rows(c)]
            s_t = s.T
            scores = sc[c].T
            for p in range(PAIRS):
                parts = []
                for h in (2 * p, 2 * p + 1):
                    gap = jnp.minimum(s_t[h : h + 1, :] - s[:, h : h + 1], 0.0)
                    parts.append((jnp.exp(gap) * scores).astype(bf16))
                mine = gb[rows(c), 128 * p : 128 * (p + 1)]
                both = jnp.concatenate([mine * low_half, mine * high_half], axis=0)
                lanes = slice(128 * p, 128 * (p + 1))
                eexp[rows(c), lanes] = dot(jnp.concatenate(parts, axis=1), both)
            g_f, x_f = gb[rows(c)].astype(f32), x_ref[rows(c)].astype(f32)
            ds1[rows(c)] = head_sum(g_f * (yin[rows(c)] - skip_e * x_f))
            q2a[rows(c)] = head_sum(xw[rows(c)].astype(f32) * eexp[rows(c)])
            return carry

        lax.fori_loop(0, CHUNKS - 1, inside_back, 0)

        for h in range(2):
            recv_wait(gr.at[h], 3, 15, h)
            scan(gr, gp, h, range(N_SEQ - 1, -1, -1))
            exchange_start(gp, gi, 5, h)
        lax.fori_loop(CHUNKS - 1, CHUNKS, inside_back, 0)

        scatter_plane()

        def summed(ref, count):
            value = ref[0]
            for k in range(1, count):
                value = value + ref[k]
            return value

        recv_wait(sar, 4, 15)
        sb2[...] = summed(sar, N_SEQ)
        cross_start(sb2, sbr, 6)

        for h in range(2):
            recv_wait(gi.at[h], 5, 15, h)

        def put_after(at_rows, lanes, value):
            apart[3, at_rows, lanes] = value

        from_blocks(gi, put_after)
        apart[2] = apart[2] + chain[2:3] * apart[3]
        apart[1] = apart[1] + chain[1:2] * apart[2]

        dec_g = bias_g = jnp.zeros((1, 128), f32)
        sig = 1.0 / (1.0 + jnp.exp(-(rawt[...] + bias_t)))
        for c in range(CHUNKS):
            span = slice(c * CHUNK, (c + 1) * CHUNK)
            after = apart[c + 1]
            width = wid[span]
            z_t = dot(bc_ref[span, :STATE], after.astype(bf16))
            q2 = q2a[span] + head_sum(wtd[span].astype(f32) * z_t)
            ends = jnp.sum((after * hst[c + 1]).reshape(16, 8, WIDE), axis=0)
            end_h = jnp.sum(head_sum(ends), axis=0, keepdims=True)
            d_a = lax.dot_general(
                tri[...], ds1[span] - q2, (((0,), (0,)), ((), ())), precision=highest, preferred_element_type=f32
            ) + end_h
            d_w = q2 / width - rate * d_a
            dec_g = dec_g - jnp.sum(d_a * (rate * width), axis=0, keepdims=True)
            bias_g = bias_g + jnp.sum(d_w * sig[span], axis=0, keepdims=True)

        recv_wait(sbr, 6, 7)
        sums_a = summed(sbr, N_DP)

        ag_sent()

        grad, square = {}, jnp.zeros((1, 1), f32)
        for n, p in enumerate(PARTS):
            dst = part["rb" + p]
            got = dst.at[pl.ds(0, 15)]
            remote(got, got, r2s.at[n], r2r.at[n], partner, seq).wait_recv()
            value = dst[0].astype(f32)
            for q in range(1, 16):
                value = value + dst[q].astype(f32)
            grad[p] = value
            square = square + jnp.sum(jnp.sum(value * value, axis=1, keepdims=True), axis=0, keepdims=True)
        t1[...] = jnp.where(lane < 16, dec_g, jnp.where(lane < 32, bias_g, jnp.where(lane == 32, square, 0.0)))
        for d, q in everyone:
            remote(t1, t2r.at[own_b], s_send.at[8, 0], s_recv.at[8, 0], d, q).start()
        t2r[own_b] = t1[...]
        recv_wait(t2r, 8, 127)
        sums_b = jnp.sum(t2r[...], axis=0)

        def heads_at(first):
            picked = jnp.where((lane >= first) & (lane < first + 16), sums_b, 0.0)
            return jnp.dot(jnp.broadcast_to(picked, (8, 128)), spread, precision=highest, preferred_element_type=f32)[0:1]

        dec_g, bias_g = heads_at(0), heads_at(16)
        squares = jnp.sum(jnp.where(lane == 32, sums_b, 0.0), axis=1, keepdims=True)
        gain_rows, skip_g, loss_all = sums_a[0:8], sums_a[8:9], sums_a[9:10]
        small = jnp.sum(
            jnp.where(lane < HEADS, dec_g * dec_g + bias_g * bias_g + skip_g * skip_g, 0.0), axis=1, keepdims=True
        )
        gains = jnp.sum(jnp.sum(gain_rows * gain_rows, axis=1, keepdims=True), axis=0, keepdims=True)
        norm = jnp.sqrt(squares + (small + gains))
        move = learn_rate * (clip_limit / jnp.maximum(norm, clip_limit))
        par[0] = jnp.broadcast_to(dec_t - move * dec_g, (8, 128))
        par[1] = jnp.broadcast_to(bias_t - move * bias_g, (8, 128))
        par[2] = jnp.broadcast_to(skip_t - move * skip_g, (8, 128))
        for r in range(8):
            lanes = slice(128 * r, 128 * (r + 1))
            gain[:, lanes] = gain[:, lanes] - move * gain_rows[r : r + 1]
        for p in PARTS:
            for h in range(2):
                lanes = slice(HALF * h + FIRST[p], HALF * h + FIRST[p] + WIDTH[p])
                wown[:, lanes] = wown[:, lanes] - move * grad[p][8 * h : 8 * h + 8]

        for h in range(2):
            send_wait(hr.at[h], 0, 15, h)
        send_wait(cr, 1, 15)
        for h in range(2):
            send_wait(hi.at[h], 2, 15, h)
        for h in range(2):
            send_wait(gr.at[h], 3, 15, h)
        send_wait(sar, 4, 15)
        for h in range(2):
            send_wait(gi.at[h], 5, 15, h)
        send_wait(sbr, 6, 7)
        send_wait(t2r, 8, 127)
        for k in range(N_Y):
            remote(wgp.at[k], pr.at[k], s_ps.at[k], s_pr.at[k], partner, seq).wait_send()
        for n, p in enumerate(PARTS):
            got, dst = part["ra" + p], part["rb" + p].at[pl.ds(0, 15)]
            remote(got, got, r1s.at[n], r1r.at[n], partner, seq).wait_send()
            remote(dst, dst, r2s.at[n], r2r.at[n], partner, seq).wait_send()

        @pl.when(step == 0)
        def _():
            ag_start()

        step_loss = loss_all[:, 0:1] * (1.0 / WIDE) / total_f
        return jnp.where(iota((1, STEPS), 1) == step, step_loss, losses)

    losses = lax.fori_loop(0, STEPS, one_step, jnp.zeros((1, STEPS), f32))
    packed_out[0:8] = wown[...]
    packed_out[8:9] = gain[...]
    packed_out[9:10, :] = jnp.zeros((1, WIDE), f32)
    for n in range(3):
        packed_out[9:10, 128 * n : 128 * (n + 1)] = par[n, 0:1]
    packed_out[9:10, 384 : 384 + STEPS] = losses


def split_kernel(packed, loss_out, w_out, dec_out, bias_out, skip_out, gain_out):
    w_out[...] = packed[0:8]
    gain_out[...] = packed[8:9]
    dec_out[...] = packed[9:10, 0:HEADS]
    bias_out[...] = packed[9:10, 128 : 128 + HEADS]
    skip_out[...] = packed[9:10, 256 : 256 + HEADS]
    loss_out[...] = packed[9:10, 384 : 384 + STEPS]


def per_device(x, z, bc, raw, ids, counts, target, weight, dec, bias, skip, gain):
    vmem = pl.BlockSpec(memory_space=pltpu.VMEM)
    smem = pl.BlockSpec(memory_space=pltpu.SMEM)
    anywhere = pl.BlockSpec(memory_space=pl.ANY)
    shape = jax.ShapeDtypeStruct
    packed = pl.pallas_call(
        kernel,
        out_shape=shape((16, WIDE), f32),
        in_specs=[anywhere] * 3 + [vmem] * 2 + [smem] + [anywhere] + [vmem] * 5,
        out_specs=vmem,
        scratch_shapes=list(scratch().values()),
        compiler_params=pltpu.CompilerParams(
            collective_id=0, has_side_effects=True, vmem_limit_bytes=62 * 1024 * 1024
        ),
    )(
        x[0], z[0], bc[0], raw[0].T, ids, counts, target[0], weight,
        dec.reshape(1, HEADS), bias.reshape(1, HEADS), skip.reshape(1, HEADS), gain.reshape(1, WIDE),
    )
    losses, weight, dec, bias, skip, gain = pl.pallas_call(
        split_kernel,
        out_shape=(
            shape((1, STEPS), f32), shape((8, WIDE), f32), shape((1, HEADS), f32), shape((1, HEADS), f32),
            shape((1, HEADS), f32), shape((1, WIDE), f32),
        ),
        in_specs=[vmem],
        out_specs=(vmem,) * 6,
    )(packed)
    return (
        losses.reshape(STEPS), weight, dec.reshape(HEADS), bias.reshape(HEADS), skip.reshape(HEADS), gain.reshape(WIDE)
    )


def solution(mesh):
    tokens = P(DP, SEQ, None)
    return jax.shard_map(
        per_device,
        mesh=mesh,
        in_specs=(
            tokens, tokens, tokens, tokens, P(DP, SEQ), P(), tokens, P((DP, SEQ), None), P(), P(), P(), P(),
        ),
        out_specs=(P(), P((DP, SEQ), None), P(), P(), P(), P()),
        check_vma=False,
    )
```

```python
import jax
import jax.numpy as jnp
from jax import lax
from jax.experimental import pallas as pl
from jax.experimental.pallas import tpu as pltpu
from jax.sharding import PartitionSpec as P

STEPS = 2
DP, SEQ = "dp", "seq"
N_DP, N_SEQ, N_Y = 8, 16, 4
TOK, WIDE, STATE, HEADS, HEAD = 384, 1024, 128, 16, 64
CHUNK, CHUNKS, PAIRS = 128, 3, 8
HALF = WIDE // 2

norm_floor = 1.0
clip_limit = 1.0
learn_rate = 8.0
f32, bf16 = jnp.float32, jnp.bfloat16
highest = lax.Precision.HIGHEST


def dot(a, b):
    return jnp.dot(a, b, preferred_element_type=f32)


def dot_tn(a, b):
    return lax.dot_general(a, b, (((0,), (0,)), ((), ())), preferred_element_type=f32)


def dot_nt(a, b):
    return lax.dot_general(a, b, (((1,), (1,)), ((), ())), preferred_element_type=f32)


def iota(shape, dim):
    return lax.broadcasted_iota(jnp.int32, shape, dim)


def three_parts(v):
    high = v.astype(bf16).astype(f32)
    rest = v - high
    mid = rest.astype(bf16).astype(f32)
    low = rest - mid
    group = (iota(v.shape, 1) >> 4) & 3
    zero = jnp.zeros_like(v)
    return jnp.where(
        group == 0, high, jnp.where(group == 1, mid, jnp.where(group == 2, low, zero))
    ).astype(bf16)


def blocks_of(rows):
    left = rows[:, :HALF].reshape(N_SEQ, 1, 8, HALF)
    right = rows[:, HALF:].reshape(N_SEQ, 1, 8, HALF)
    return jnp.concatenate([left, right], axis=1).reshape(N_SEQ, 16, HALF)


def rows_of(blocks):
    count = blocks.shape[0]
    split = blocks.reshape(count, 2, 8, HALF)
    return split[:, 0].reshape(count * 8, HALF), split[:, 1].reshape(count * 8, HALF)


INPUTS = (
    "x_in", "z_in", "bc_in", "raw_hbm", "ids_hbm", "cnt_hbm", "tgt_in", "w_hbm", "dec_hbm", "bias_hbm", "skip_hbm", "gain_hbm",
)
OUTPUTS = ("packed_out",)
PARTS = "yxz"
WIDTH = {"y": 256, "x": 128, "z": 128}
FIRST = {"y": 0, "x": 256, "z": 384}


def scratch():
    dma, v = pltpu.SemaphoreType.DMA, pltpu.VMEM
    rows_f, wide_f, wide_b = v((TOK, 128), f32), v((TOK, WIDE), f32), v((TOK, WIDE), bf16)
    states, sixteen = v((CHUNKS + 1, STATE, WIDE), f32), v((2, N_SEQ, 16, HALF // 2), bf16)
    small, small16, small8 = v((16, 128), f32), v((N_SEQ, 16, 128), f32), v((N_DP, 16, 128), f32)
    named = dict(
        raw_in=v((HEADS, TOK), f32), ids_ref=v((1, TOK), jnp.int32), cnt_ref=pltpu.SMEM((N_DP,), jnp.int32),
        dec_in=v((1, HEADS), f32), bias_in=v((1, HEADS), f32), skip_in=v((1, HEADS), f32),
        x_ref=wide_b, z_ref=wide_b, bc_ref=v((TOK, 2 * STATE), bf16), tgt_ref=wide_b, s_in=dma((12,)),
        act=wide_f, gat=wide_f, dnf=wide_f, gdn=wide_f, invs=rows_f,
        ex=v((128, WIDE), bf16), red=v((WIDE, 128), bf16), tri=v((CHUNK, CHUNK), f32), par=v((3, 8, 128), f32),
        gain=v((1, WIDE), f32), wown=v((8, WIDE), f32), rawt=rows_f, wid=rows_f, dec_s=rows_f, ent=rows_f,
        chain=v((8, WIDE), f32), fcol=v((CHUNKS, CHUNK, CHUNK), f32), sc=v((CHUNKS, CHUNK, CHUNK), f32),
        xw=wide_b, wtd=wide_b, yin=wide_f, eexp=wide_f, gstate=v((CHUNKS, STATE, WIDE), f32), hst=states, apart=states,
        normb=wide_b, ogb=wide_b, gb=wide_b, q2a=rows_f, ds1=rows_f, accs=v((2, 8, WIDE), f32),
        hs=sixteen, hr=sixteen, hp=sixteen, hi=sixteen, gs=sixteen, gr=sixteen, gp=sixteen, gi=sixteen,
        cs=v((8, 128), f32), cr=v((N_SEQ, 8, 128), f32), wfull=v((WIDE, WIDE), bf16),
        wgp=v((N_Y, N_SEQ, 16, HALF), bf16), pr=v((N_Y, N_SEQ, 16, HALF), bf16),
        sa=small, sar=small16, sb2=small, sbr=small8, t1=v((1, 128), f32),
        t2r=v((128, 1, 128), f32),
    )
    for p in PARTS:
        w = WIDTH[p]
        named["ag" + p] = v((128, 16, w), bf16)
        named["sb" + p] = v((64, 16, w), bf16)
        named["ra" + p] = v((3, N_SEQ, 16, w), bf16)
        named["mid" + p] = v((N_SEQ, 16, w), bf16)
        named["rb" + p] = v((N_SEQ, 16, w), bf16)
    for name, count in dict(s_ps=4, s_pr=4, g1s=3, g1r=3, g2s=3, g2r=3, g3s=3, g3r=3, r1s=3, r1r=3, r2s=3, r2r=3).items():
        named[name] = dma((count,))
    named["s_send"] = dma((9, 2))
    named["s_recv"] = dma((9, 2))
    return named


def kernel(*refs):
    names = INPUTS + OUTPUTS + tuple(scratch())
    assert len(names) == len(refs)
    program(**dict(zip(names, refs)))


def program(
    x_in, z_in, bc_in, raw_hbm, ids_hbm, cnt_hbm, tgt_in, w_hbm, dec_hbm, bias_hbm, skip_hbm, gain_hbm,
    packed_out, raw_in, ids_ref, cnt_ref, dec_in, bias_in, skip_in, x_ref, z_ref, bc_ref, tgt_ref, s_in, act, gat, dnf, gdn, invs,
    ex, red, tri, par, gain, wown, rawt, wid, dec_s, ent, chain, fcol, sc,
    xw, wtd, yin, eexp, gstate, hst, apart, normb, ogb, gb, q2a, ds1, accs,
    hs, hr, hp, hi, gs, gr, gp, gi, cs, cr, wfull, wgp, pr, sa, sar, sb2, sbr, t1, t2r,
    s_send, s_recv, s_ps, s_pr, g1s, g1r, g2s, g2r, g3s, g3r, r1s, r1r, r2s, r2r, **part,
):
    dp, seq = lax.axis_index(DP), lax.axis_index(SEQ)
    yy, core = dp // 2, dp % 2
    partner = dp + 1 - 2 * core
    own_b = dp * N_SEQ + seq
    xx, zz = seq // 4, seq % 4
    place = {"y": yy, "x": xx, "z": zz}
    MESH = pl.DeviceIdType.MESH

    def at(d, s):
        return {DP: d, SEQ: s}

    def remote(src, dst, ss, rs, d, s):
        return pltpu.make_async_remote_copy(
            src_ref=src, dst_ref=dst, send_sem=ss, recv_sem=rs, device_id=at(d, s), device_id_type=MESH
        )

    incoming = (
        (dec_hbm, dec_in), (bias_hbm, bias_in), (skip_hbm, skip_in), (raw_hbm, raw_in), (ids_hbm, ids_ref), (bc_in, bc_ref),
        (x_in, x_ref), (w_hbm, wown), (gain_hbm, gain), (z_in, z_ref), (tgt_in, tgt_ref), (cnt_hbm, cnt_ref),
    )
    loads = [pltpu.make_async_copy(source, target, s_in.at[n]) for n, (source, target) in enumerate(incoming)]
    for load in loads:
        load.start()

    barrier = pltpu.get_barrier_semaphore()

    dps = [((yy + k) % 4) * 2 + core for k in range(4)]
    seqs = {(a, b): ((xx + a) % 4) * 4 + (zz + b) % 4 for a in range(4) for b in range(4)}

    def hops(offset):
        return sum(min(k, 4 - k) for k in offset)

    chips = [(a, b, c) for a in range(4) for b in range(4) for c in range(4)]
    far_first = sorted(chips[1:], key=lambda offset: -hops(offset))
    everyone = []
    for a, b, c in far_first + chips[:1]:
        for flip in (0, 1):
            if (a, b, c, flip) != (0, 0, 0, 0):
                everyone.append((dps[a] + flip * (1 - 2 * core), seqs[b, c]))
    for d, s in everyone:
        pl.semaphore_signal(barrier, 1, device_id=at(d, s), device_id_type=MESH)

    row = iota((CHUNK, WIDE), 0)
    col = iota((CHUNK, WIDE), 1)
    ex[...] = jnp.where(((row & 15) == (col >> 6)) & (row < 48), 1.0, 0.0).astype(bf16)
    rrow = iota((WIDE, 128), 0)
    rcol = iota((WIDE, 128), 1)
    ti, tj = iota((CHUNK, CHUNK), 0), iota((CHUNK, CHUNK), 1)
    tri[...] = jnp.where(ti >= tj, 1.0, 0.0)
    rep = jnp.where(iota((HEADS, 128), 0) == (iota((HEADS, 128), 1) & 15), 1.0, 0.0)

    spread = jnp.where((iota((128, 128), 0) & 15) == (iota((128, 128), 1) & 15), 1.0, 0.0)

    def tiled(ref):
        return jnp.dot(jnp.broadcast_to(ref[...], (8, HEADS)), rep, precision=highest, preferred_element_type=f32)

    for load in loads[:5]:
        load.wait()
    par[0] = tiled(dec_in)
    par[1] = tiled(bias_in)
    par[2] = tiled(skip_in)
    rawt[...] = lax.dot_general(
        raw_in[...], rep, (((0,), (0,)), ((), ())), precision=highest, preferred_element_type=f32
    )
    loads[5].wait()
    loads[11].wait()

    def expand(v):
        return dot(three_parts(v), ex[...])

    def head_sum(v):
        high = v.astype(bf16)
        low = (v - high.astype(f32)).astype(bf16)
        return dot(high, red[...]) + dot(low, red[...])

    lane = iota((1, 128), 1)
    low_half = jnp.where(lane < HEAD, 1.0, 0.0).astype(bf16)
    high_half = jnp.where(lane < HEAD, 0.0, 1.0).astype(bf16)

    total = cnt_ref[0]
    for k in range(1, N_DP):
        total = total + cnt_ref[k]
    total_f = total.astype(f32)
    own_count = cnt_ref[dp]

    def rows(c):
        return pl.ds(pl.multiple_of(c * CHUNK, CHUNK), CHUNK)

    def prepare(c, carry):
        flag = jnp.where(ids_ref[0:1, rows(c)] == 0, 1.0, 0.0)
        flag_col = jnp.broadcast_to(flag, (CHUNK, CHUNK)).T
        seg = dot(tri[...], flag_col)
        fcol[c] = seg
        return carry

    lax.fori_loop(0, CHUNKS, prepare, 0)
    loads[6].wait()
    loads[7].wait()
    loads[8].wait()

    def index_in(p, y, x, z):
        return {"y": y * 16 + x * 4 + z, "x": x * 16 + y * 4 + z, "z": z * 16 + x * 4 + y}[p]

    plane_far = sorted([(a, b) for a in range(4) for b in range(4)][1:], key=lambda offset: -hops(offset))

    def plane_peer(p, a, b):
        if p == "y":
            return dp, seqs[a, b], seqs[a, b]
        if p == "x":
            return dps[a], seqs[0, b], ((yy + a) % 4) * 4 + (zz + b) % 4
        return dps[b], seqs[a, 0], ((xx + a) % 4) * 4 + (yy + b) % 4

    def line_peer(p, k):
        c = (place[p] + k) % 4
        if p == "y":
            return c * 2 + core, seq, c
        if p == "x":
            return dp, c * 4 + zz, c
        return dp, xx * 4 + c, c

    mine_in = {p: index_in(p, yy, xx, zz) for p in PARTS}

    def ag_start():
        for n, p in enumerate(PARTS):
            buf = part["ag" + p]
            lanes = slice(FIRST[p], FIRST[p] + WIDTH[p])
            right = slice(HALF + FIRST[p], HALF + FIRST[p] + WIDTH[p])
            own = core * 64 + mine_in[p]
            buf[own] = jnp.concatenate([wown[:, lanes], wown[:, right]], axis=0).astype(bf16)

            for a, b in plane_far:
                d, s, _ = plane_peer(p, a, b)
                remote(buf.at[own], buf.at[own], g1s.at[n], g1r.at[n], d, s).start()

    def ag_line():
        for n, p in enumerate(PARTS):
            buf = part["ag" + p]
            piece = buf.at[pl.ds(0, 15)]
            remote(piece, piece, g1s.at[n], g1r.at[n], partner, seq).wait_recv()
            slab = buf.at[pl.ds(core * 64 + place[p] * 16, 16)]
            for k in range(1, 4):
                d, s, _ = line_peer(p, k)
                remote(slab, slab, g2s.at[n], g2r.at[n], d, s).start()

    def unpack(p, its_core):
        buf, w, base = part["ag" + p], WIDTH[p], its_core * 64

        def one(y, carry):
            d = y * 2 + its_core
            if p == "y":
                blocks = [buf[pl.ds(base + y * 16, 16)].astype(f32)]
            elif p == "x":
                blocks = [buf[pl.ds(base + x * 16 + y * 4, 4)].astype(f32) for x in range(4)]
            else:
                blocks = [buf[pl.ds(base + z * 16 + x * 4 + y, 1)].astype(f32) for x in range(4) for z in range(4)]
            tops, lows = [], []
            for block in blocks:
                split = block.reshape(block.shape[0], 2, 8, w)
                tops.append(split[:, 0].reshape(-1, w))
                lows.append(split[:, 1].reshape(-1, w))
            wfull[rows(d), FIRST[p] : FIRST[p] + w] = jnp.concatenate(tops, axis=0).astype(bf16)
            wfull[rows(d), HALF + FIRST[p] : HALF + FIRST[p] + w] = jnp.concatenate(lows, axis=0).astype(bf16)
            return carry

        lax.fori_loop(0, N_Y, one, 0)

    def ag_finish():
        for p in "xzy":
            n, buf = PARTS.index(p), part["ag" + p]
            piece = buf.at[pl.ds(0, 48)]
            remote(piece, piece, g2s.at[n], g2r.at[n], partner, seq).wait_recv()
            ours = buf.at[pl.ds(core * 64, 64)]
            remote(ours, ours, g3s.at[n], g3r.at[n], partner, seq).start()
            unpack(p, core)
        for p in "xzy":
            n, buf = PARTS.index(p), part["ag" + p]
            piece = buf.at[pl.ds((1 - core) * 64, 64)]
            remote(piece, piece, g3s.at[n], g3r.at[n], partner, seq).wait_recv()
            unpack(p, 1 - core)

    def ag_sent():
        for n, p in enumerate(PARTS):
            buf = part["ag" + p]
            for count, ss, rs in ((15, g1s, g1r), (48, g2s, g2r), (64, g3s, g3r)):
                piece = buf.at[pl.ds(0, count)]
                remote(piece, piece, ss.at[n], rs.at[n], partner, seq).wait_send()

    def exchange_start(src, dst, n, h):
        for a, b in plane_far:
            peer = seqs[a, b]
            remote(src.at[h, peer], dst.at[h, seq], s_send.at[n, h], s_recv.at[n, h], dp, peer).start()
        dst[h, seq] = src[h, seq]

    def spread_start(src, dst, n):
        for a, b in plane_far:
            remote(src, dst.at[seq], s_send.at[n, 0], s_recv.at[n, 0], dp, seqs[a, b]).start()
        dst[seq] = src[...]

    def cross_start(src, dst, n):
        for k in range(1, N_DP):
            remote(src, dst.at[dp], s_send.at[n, 0], s_recv.at[n, 0], (dp + k) % N_DP, seq).start()
        dst[dp] = src[...]

    def recv_wait(dst, n, count, h=0):
        piece = dst.at[pl.ds(0, count)]
        remote(piece, piece, s_send.at[n, h], s_recv.at[n, h], partner, seq).wait_recv()

    def send_wait(dst, n, count, h=0):
        piece = dst.at[pl.ds(0, count)]
        remote(piece, piece, s_send.at[n, h], s_recv.at[n, h], partner, seq).wait_send()

    def one_step(step, losses):
        dec_t, bias_t, skip_t = par[0, 0:1], par[1, 0:1], par[2, 0:1]
        rate = jnp.exp(dec_t)

        pre = rawt[...] + bias_t
        u = jnp.exp(-jnp.abs(pre))
        v = 1.0 + u
        log1p = jnp.where(v == 1.0, u, jnp.log(v) * u / jnp.where(v == 1.0, 1.0, v - 1.0))
        widths = jnp.maximum(pre, 0.0) + log1p
        wid[...] = widths
        sub8, lane8 = iota((8, 128), 0), iota((8, 128), 1)
        through = jnp.zeros((8, 128), f32)
        carried = jnp.ones((1, 128), f32)
        for c in range(CHUNKS):
            span = slice(c * CHUNK, (c + 1) * CHUNK)
            seg = fcol[c]
            width = widths[span]
            s = jnp.dot(tri[...], -rate * width, precision=highest, preferred_element_type=f32)
            last = s[CHUNK - 1 : CHUNK]
            seg_last = seg[CHUNK - 1 : CHUNK]
            leaving = jnp.exp(last - s) * jnp.where(seg == seg_last, 1.0, 0.0)
            passing = jnp.exp(last) * jnp.where(seg_last == 0.0, 1.0, 0.0)
            dec_s[span] = s
            ent[span] = jnp.exp(s) * jnp.where(seg == 0.0, 1.0, 0.0)
            weighted = (x_ref[span].astype(f32) * expand(width * leaving)).astype(bf16)
            wtd[span] = weighted
            gstate[c] = dot_tn(bc_ref[span, :STATE], weighted)
            through = jnp.where(sub8 == c, passing, through)
            carried = carried * passing
        chain[...] = expand(through)
        wide8 = jnp.broadcast_to(carried, (8, 128))
        even = jnp.sum(jnp.where(lane8 == 2 * sub8, wide8, 0.0), axis=1, keepdims=True)
        odd = jnp.sum(jnp.where(lane8 == 2 * sub8 + 1, wide8, 0.0), axis=1, keepdims=True)
        cs[...] = jnp.where(lane8 < HEAD, even, odd)
        hst[0] = gstate[2] + chain[2:3] * (gstate[1] + chain[1:2] * gstate[0])

        def to_blocks(state, out):
            for r in range(8):
                for h in range(2):
                    for q in range(2):
                        first = HALF * h + 256 * q
                        out[q, 2 * r + h] = state[16 * r : 16 * r + 16, first : first + 256].astype(bf16)

        def from_blocks(source, put):
            for q in range(2):
                for r in range(8):
                    for h in range(2):
                        first = HALF * h + 256 * q
                        put(slice(16 * r, 16 * r + 16), slice(first, first + 256), source[q, 2 * r + h].astype(f32))

        to_blocks(hst[0], hs)

        @pl.when(step == 0)
        def _():
            pl.semaphore_wait(barrier, 127)
            ag_start()

        exchange_start(hs, hr, 0, 0)
        spread_start(cs, cr, 1)
        exchange_start(hs, hr, 0, 1)

        @pl.when(step == 0)
        def _():
            loads[9].wait()
            red[...] = jnp.where((rrow >> 6) == (rcol & 15), 1.0, 0.0).astype(bf16)

            def once(c, carry):
                z_f = z_ref[rows(c)].astype(f32)
                act[rows(c)] = z_f / (1.0 + jnp.exp(-z_f))
                scores = dot_nt(bc_ref[rows(c), STATE:], bc_ref[rows(c), :STATE])
                sc[c] = jnp.where((fcol[c] == fcol[c].T) & (ti >= tj), scores, 0.0)
                return carry

            lax.fori_loop(0, CHUNKS, once, 0)
            loads[10].wait()

        skip_e = expand(jnp.broadcast_to(skip_t, (8, 128)))[0:1]
        gain_e = gain[...]

        def inside(c, carry):
            s = dec_s[rows(c)]
            s_t = s.T
            scores = sc[c]
            xw[rows(c)] = (x_ref[rows(c)].astype(f32) * expand(wid[rows(c)])).astype(bf16)
            eexp[rows(c)] = expand(ent[rows(c)])
            for p in range(PAIRS):
                parts = []
                for h in (2 * p, 2 * p + 1):
                    gap = jnp.minimum(s[:, h : h + 1] - s_t[h : h + 1, :], 0.0)
                    parts.append((jnp.exp(gap) * scores).astype(bf16))
                mine = xw[rows(c), 128 * p : 128 * (p + 1)]
                both = jnp.concatenate([mine * low_half, mine * high_half], axis=0)
                lanes = slice(128 * p, 128 * (p + 1))
                direct = skip_e[:, lanes] * x_ref[rows(c), lanes].astype(f32)
                yin[rows(c), lanes] = dot(jnp.concatenate(parts, axis=1), both) + direct
            return carry

        lax.fori_loop(0, CHUNKS, inside, 0)
        ag_line()

        half = seq % 2

        def scan(source, out, h, order):
            state = [jnp.zeros((16, 128), f32) for _ in range(2)]
            for i in order:
                for m in range(2):
                    lanes = slice(128 * m, 128 * (m + 1))
                    out[h, i, :, lanes] = state[m].astype(bf16)
                    factor = cr[i, pl.ds(4 * half + 2 * h + m, 1), :]
                    state[m] = factor * state[m] + source[h, i, :, lanes].astype(f32)

        recv_wait(cr, 1, 15)
        for h in range(2):
            recv_wait(hr.at[h], 0, 15, h)
            scan(hr, hp, h, range(N_SEQ))
            exchange_start(hp, hi, 2, h)
        ag_finish()
        for h in range(2):
            recv_wait(hi.at[h], 2, 15, h)

        def put_state(at_rows, lanes, value):
            hst[0, at_rows, lanes] = value

        from_blocks(hi, put_state)

        scale = 2.0 / (WIDE * total_f)
        accs[...] = jnp.zeros(accs.shape, f32)

        for c in range(CHUNKS):
            span = slice(c * CHUNK, (c + 1) * CHUNK)
            state = hst[c]
            y = yin[span] + eexp[span] * dot(bc_ref[span, STATE:], state.astype(bf16))
            yin[span] = y
            gated = y * act[span]
            gat[span] = gated
            inv = lax.rsqrt(jnp.sum(gated * gated, axis=1, keepdims=True) * (1.0 / WIDE) + norm_floor)
            invs[span] = jnp.broadcast_to(inv, (CHUNK, 128))
            normb[span] = (gated * gain_e * inv).astype(bf16)
            hst[c + 1] = chain[c : c + 1] * state + gstate[c]
        block = 512
        position = seq * TOK + iota((TOK, block), 0)
        scored = jnp.where(position < own_count, 1.0, 0.0)
        losses_8 = jnp.zeros((8, block), f32)
        for first in range(0, WIDE, block):
            lanes = slice(first, first + block)
            res = (dot(normb[...], wfull[:, lanes]) - tgt_ref[:, lanes].astype(f32)) * scored
            losses_8 = losses_8 + jnp.sum((res * res).reshape(TOK // 8, 8, block), axis=0)
            ogb[:, lanes] = (res * scale).astype(bf16)
        loss = jnp.sum(jnp.sum(losses_8, axis=1, keepdims=True), axis=0, keepdims=True)
        inner_l = jnp.zeros((TOK, 128), f32)
        for first in range(0, WIDE, block):
            lanes = slice(first, first + block)
            d_norm = dot_nt(ogb[...], wfull[lanes, :])
            dnf[:, lanes] = d_norm
            d_gain = d_norm * gain_e[:, lanes]
            gdn[:, lanes] = d_gain
            term = d_gain * gat[:, lanes]
            for k in range(0, block, 128):
                inner_l = inner_l + term[:, k : k + 128]
        inner = jnp.sum(inner_l, axis=1, keepdims=True) * (1.0 / WIDE)
        for c in range(CHUNKS):
            span = slice(c * CHUNK, (c + 1) * CHUNK)
            inv = invs[span, 0:1]
            g = (gdn[span] - gat[span] * (inv * inv * inner[span])) * inv * act[span]
            gb[span] = g.astype(bf16)
            apart[c] = dot_tn(bc_ref[span, STATE:], (g * eexp[span]).astype(bf16))
        entry = apart[0] + chain[0:1] * (apart[1] + chain[1:2] * apart[2])
        to_blocks(entry, gs)
        for h in range(2):
            exchange_start(gs, gr, 3, h)
        def grad_rows(first, second):
            lanes = [normb[:, pl.ds(pl.multiple_of(d * 128, 128), 128)] for d in (first, second)]
            both = dot_tn(jnp.concatenate(lanes, axis=1), ogb[...])
            return blocks_of(both[:128]), blocks_of(both[128:])

        def group(k, c):
            return ((yy + k) % N_Y) * 2 + c

        for pair in ((1, 2), (3, 0)):
            pieces = grad_rows(*[group(k, 1 - core) for k in pair])
            for k, piece in zip(pair, pieces):
                wgp[k] = piece.astype(bf16)
                remote(wgp.at[k], pr.at[k], s_ps.at[k], s_pr.at[k], partner, seq).start()
        def small_sums(c, carry):
            x_f, inv = x_ref[rows(c)].astype(f32), invs[rows(c), 0:1]
            accs[0] += jnp.sum((dnf[rows(c)] * gat[rows(c)] * inv).reshape(16, 8, WIDE), axis=0)
            accs[1] += jnp.sum((gb[rows(c)].astype(f32) * x_f).reshape(16, 8, WIDE), axis=0)
            return carry

        lax.fori_loop(0, CHUNKS, small_sums, 0)
        gain_g = jnp.sum(accs[0], axis=0, keepdims=True)
        for r in range(8):
            sa[r : r + 1, :] = gain_g[:, 128 * r : 128 * (r + 1)]
        skip_g = head_sum(jnp.broadcast_to(jnp.sum(accs[1], axis=0, keepdims=True), (8, WIDE)))
        sub = iota((8, 128), 0)
        sa[8:16, :] = jnp.where(sub == 0, skip_g, jnp.where(sub == 1, jnp.broadcast_to(loss, (8, 128)), 0.0))
        spread_start(sa, sar, 4)
        for pair in ((1, 2), (3, 0)):
            pieces = grad_rows(*[group(k, core) for k in pair])
            for k, mine in zip(pair, pieces):
                y_k = (yy + k) % N_Y
                remote(wgp.at[k], pr.at[k], s_ps.at[k], s_pr.at[k], partner, seq).wait_recv()
                both = (mine + pr[k].astype(f32)).astype(bf16)
                part["sby"][pl.ds(y_k * 16, 16)] = both[:, :, : WIDTH["y"]]
                if k > 0:
                    slab = part["sby"].at[pl.ds(y_k * 16, 16)]
                    remote(slab, part["ray"].at[k - 1], r1s.at[0], r1r.at[0], y_k * 2 + core, seq).start()
                for p in "xz":
                    piece = both[:, :, FIRST[p] : FIRST[p] + WIDTH[p]]
                    for x in range(4):
                        if p == "x":
                            part["sbx"][pl.ds(x * 16 + y_k * 4, 4)] = piece[4 * x : 4 * x + 4]
                        else:
                            for z in range(4):
                                part["sbz"][z * 16 + x * 4 + y_k] = piece[4 * x + z]
        for n, p in ((1, "x"), (2, "z")):
            for k in range(1, 4):
                d, s, c = line_peer(p, k)
                slab = part["sb" + p].at[pl.ds(c * 16, 16)]
                remote(slab, part["ra" + p].at[k - 1], r1s.at[n], r1r.at[n], d, s).start()

        def scatter_plane():
            for p in "xzy":
                n = PARTS.index(p)
                got, mid, dst = part["ra" + p], part["mid" + p], part["rb" + p]
                remote(got, got, r1s.at[n], r1r.at[n], partner, seq).wait_recv()
                value = part["sb" + p][pl.ds(place[p] * 16, 16)].astype(f32)
                for k in range(3):
                    value = value + got[k].astype(f32)
                mid[...] = value.astype(bf16)
                here = mine_in[p] % 16
                for a, b in plane_far:
                    d, s, q = plane_peer(p, a, b)
                    remote(mid.at[q], dst.at[here], r2s.at[n], r2r.at[n], d, s).start()
                dst[here] = mid[here]

        def inside_back(c, carry):
            s = dec_s[rows(c)]
            s_t = s.T
            scores = sc[c].T
            for p in range(PAIRS):
                parts = []
                for h in (2 * p, 2 * p + 1):
                    gap = jnp.minimum(s_t[h : h + 1, :] - s[:, h : h + 1], 0.0)
                    parts.append((jnp.exp(gap) * scores).astype(bf16))
                mine = gb[rows(c), 128 * p : 128 * (p + 1)]
                both = jnp.concatenate([mine * low_half, mine * high_half], axis=0)
                lanes = slice(128 * p, 128 * (p + 1))
                eexp[rows(c), lanes] = dot(jnp.concatenate(parts, axis=1), both)
            g_f, x_f = gb[rows(c)].astype(f32), x_ref[rows(c)].astype(f32)
            ds1[rows(c)] = head_sum(g_f * (yin[rows(c)] - skip_e * x_f))
            q2a[rows(c)] = head_sum(xw[rows(c)].astype(f32) * eexp[rows(c)])
            return carry

        lax.fori_loop(0, CHUNKS - 1, inside_back, 0)

        for h in range(2):
            recv_wait(gr.at[h], 3, 15, h)
            scan(gr, gp, h, range(N_SEQ - 1, -1, -1))
            exchange_start(gp, gi, 5, h)
        lax.fori_loop(CHUNKS - 1, CHUNKS, inside_back, 0)

        scatter_plane()

        def summed(ref, count):
            value = ref[0]
            for k in range(1, count):
                value = value + ref[k]
            return value

        recv_wait(sar, 4, 15)
        sb2[...] = summed(sar, N_SEQ)
        cross_start(sb2, sbr, 6)

        for h in range(2):
            recv_wait(gi.at[h], 5, 15, h)

        def put_after(at_rows, lanes, value):
            apart[3, at_rows, lanes] = value

        from_blocks(gi, put_after)
        apart[2] = apart[2] + chain[2:3] * apart[3]
        apart[1] = apart[1] + chain[1:2] * apart[2]

        dec_g = bias_g = jnp.zeros((1, 128), f32)
        sig = 1.0 / (1.0 + jnp.exp(-(rawt[...] + bias_t)))
        for c in range(CHUNKS):
            span = slice(c * CHUNK, (c + 1) * CHUNK)
            after = apart[c + 1]
            width = wid[span]
            z_t = dot(bc_ref[span, :STATE], after.astype(bf16))
            q2 = q2a[span] + head_sum(wtd[span].astype(f32) * z_t)
            ends = jnp.sum((after * hst[c + 1]).reshape(16, 8, WIDE), axis=0)
            end_h = jnp.sum(head_sum(ends), axis=0, keepdims=True)
            d_a = lax.dot_general(
                tri[...], ds1[span] - q2, (((0,), (0,)), ((), ())), precision=highest, preferred_element_type=f32
            ) + end_h
            d_w = q2 / width - rate * d_a
            dec_g = dec_g - jnp.sum(d_a * (rate * width), axis=0, keepdims=True)
            bias_g = bias_g + jnp.sum(d_w * sig[span], axis=0, keepdims=True)

        recv_wait(sbr, 6, 7)
        sums_a = summed(sbr, N_DP)

        ag_sent()

        grad, square = {}, jnp.zeros((1, 1), f32)
        for n, p in enumerate(PARTS):
            dst = part["rb" + p]
            got = dst.at[pl.ds(0, 15)]
            remote(got, got, r2s.at[n], r2r.at[n], partner, seq).wait_recv()
            value = dst[0].astype(f32)
            for q in range(1, 16):
                value = value + dst[q].astype(f32)
            grad[p] = value
            square = square + jnp.sum(jnp.sum(value * value, axis=1, keepdims=True), axis=0, keepdims=True)
        t1[...] = jnp.where(lane < 16, dec_g, jnp.where(lane < 32, bias_g, jnp.where(lane == 32, square, 0.0)))
        for d, q in everyone:
            remote(t1, t2r.at[own_b], s_send.at[8, 0], s_recv.at[8, 0], d, q).start()
        t2r[own_b] = t1[...]
        recv_wait(t2r, 8, 127)
        sums_b = jnp.sum(t2r[...], axis=0)

        def heads_at(first):
            picked = jnp.where((lane >= first) & (lane < first + 16), sums_b, 0.0)
            return jnp.dot(jnp.broadcast_to(picked, (8, 128)), spread, precision=highest, preferred_element_type=f32)[0:1]

        dec_g, bias_g = heads_at(0), heads_at(16)
        squares = jnp.sum(jnp.where(lane == 32, sums_b, 0.0), axis=1, keepdims=True)
        gain_rows, skip_g, loss_all = sums_a[0:8], sums_a[8:9], sums_a[9:10]
        small = jnp.sum(
            jnp.where(lane < HEADS, dec_g * dec_g + bias_g * bias_g + skip_g * skip_g, 0.0), axis=1, keepdims=True
        )
        gains = jnp.sum(jnp.sum(gain_rows * gain_rows, axis=1, keepdims=True), axis=0, keepdims=True)
        norm = jnp.sqrt(squares + (small + gains))
        move = learn_rate * (clip_limit / jnp.maximum(norm, clip_limit))
        par[0] = jnp.broadcast_to(dec_t - move * dec_g, (8, 128))
        par[1] = jnp.broadcast_to(bias_t - move * bias_g, (8, 128))
        par[2] = jnp.broadcast_to(skip_t - move * skip_g, (8, 128))
        for r in range(8):
            lanes = slice(128 * r, 128 * (r + 1))
            gain[:, lanes] = gain[:, lanes] - move * gain_rows[r : r + 1]
        for p in PARTS:
            for h in range(2):
                lanes = slice(HALF * h + FIRST[p], HALF * h + FIRST[p] + WIDTH[p])
                wown[:, lanes] = wown[:, lanes] - move * grad[p][8 * h : 8 * h + 8]

        for h in range(2):
            send_wait(hr.at[h], 0, 15, h)
        send_wait(cr, 1, 15)
        for h in range(2):
            send_wait(hi.at[h], 2, 15, h)
        for h in range(2):
            send_wait(gr.at[h], 3, 15, h)
        send_wait(sar, 4, 15)
        for h in range(2):
            send_wait(gi.at[h], 5, 15, h)
        send_wait(sbr, 6, 7)
        send_wait(t2r, 8, 127)
        for k in range(N_Y):
            remote(wgp.at[k], pr.at[k], s_ps.at[k], s_pr.at[k], partner, seq).wait_send()
        for n, p in enumerate(PARTS):
            got, dst = part["ra" + p], part["rb" + p].at[pl.ds(0, 15)]
            remote(got, got, r1s.at[n], r1r.at[n], partner, seq).wait_send()
            remote(dst, dst, r2s.at[n], r2r.at[n], partner, seq).wait_send()

        @pl.when(step == 0)
        def _():
            ag_start()

        step_loss = loss_all[:, 0:1] * (1.0 / WIDE) / total_f
        return jnp.where(iota((1, STEPS), 1) == step, step_loss, losses)

    losses = lax.fori_loop(0, STEPS, one_step, jnp.zeros((1, STEPS), f32))
    packed_out[0:8] = wown[...]
    packed_out[8:9] = gain[...]
    packed_out[9:10, :] = jnp.zeros((1, WIDE), f32)
    for n in range(3):
        packed_out[9:10, 128 * n : 128 * (n + 1)] = par[n, 0:1]
    packed_out[9:10, 384 : 384 + STEPS] = losses


def split_kernel(packed, loss_out, w_out, dec_out, bias_out, skip_out, gain_out):
    w_out[...] = packed[0:8]
    gain_out[...] = packed[8:9]
    dec_out[...] = packed[9:10, 0:HEADS]
    bias_out[...] = packed[9:10, 128 : 128 + HEADS]
    skip_out[...] = packed[9:10, 256 : 256 + HEADS]
    loss_out[...] = packed[9:10, 384 : 384 + STEPS]


def per_device(x, z, bc, raw, ids, counts, target, weight, dec, bias, skip, gain):
    vmem = pl.BlockSpec(memory_space=pltpu.VMEM)
    in_hbm = pl.BlockSpec(memory_space=pltpu.HBM)
    shape = jax.ShapeDtypeStruct
    packed = pl.pallas_call(
        kernel,
        out_shape=shape((16, WIDE), f32),
        in_specs=[in_hbm] * 12,
        out_specs=vmem,
        scratch_shapes=list(scratch().values()),
        compiler_params=pltpu.CompilerParams(
            collective_id=0, has_side_effects=True, vmem_limit_bytes=62 * 1024 * 1024
        ),
    )(
        x[0], z[0], bc[0], raw[0].T, ids, counts, target[0], weight,
        dec.reshape(1, HEADS), bias.reshape(1, HEADS), skip.reshape(1, HEADS), gain.reshape(1, WIDE),
    )
    losses, weight, dec, bias, skip, gain = pl.pallas_call(
        split_kernel,
        out_shape=(
            shape((1, STEPS), f32), shape((8, WIDE), f32), shape((1, HEADS), f32), shape((1, HEADS), f32),
            shape((1, HEADS), f32), shape((1, WIDE), f32),
        ),
        in_specs=[vmem],
        out_specs=(vmem,) * 6,
    )(packed)
    return (
        losses.reshape(STEPS), weight, dec.reshape(HEADS), bias.reshape(HEADS), skip.reshape(HEADS), gain.reshape(WIDE)
    )


def solution(mesh):
    tokens = P(DP, SEQ, None)
    return jax.shard_map(
        per_device,
        mesh=mesh,
        in_specs=(
            tokens, tokens, tokens, tokens, P(DP, SEQ), P(), tokens, P((DP, SEQ), None), P(), P(), P(), P(),
        ),
        out_specs=(P(), P((DP, SEQ), None), P(), P(), P(), P()),
        check_vma=False,
    )
```

```python
import jax
import jax.numpy as jnp
from jax import lax
from jax.experimental import pallas as pl
from jax.experimental.pallas import tpu as pltpu
from jax.sharding import PartitionSpec as P

STEPS = 2
DP, SEQ = "dp", "seq"
N_DP, N_SEQ, N_Y = 8, 16, 4
TOK, WIDE, STATE, HEADS, HEAD = 384, 1024, 128, 16, 64
CHUNK, CHUNKS, PAIRS = 128, 3, 8
HALF = WIDE // 2

norm_floor = 1.0
clip_limit = 1.0
learn_rate = 8.0
f32, bf16 = jnp.float32, jnp.bfloat16
highest = lax.Precision.HIGHEST


def dot(a, b):
    return jnp.dot(a, b, preferred_element_type=f32)


def dot_tn(a, b):
    return lax.dot_general(a, b, (((0,), (0,)), ((), ())), preferred_element_type=f32)


def dot_nt(a, b):
    return lax.dot_general(a, b, (((1,), (1,)), ((), ())), preferred_element_type=f32)


def iota(shape, dim):
    return lax.broadcasted_iota(jnp.int32, shape, dim)


def three_parts(v):
    high = v.astype(bf16).astype(f32)
    rest = v - high
    mid = rest.astype(bf16).astype(f32)
    low = rest - mid
    group = (iota(v.shape, 1) >> 4) & 3
    zero = jnp.zeros_like(v)
    return jnp.where(
        group == 0, high, jnp.where(group == 1, mid, jnp.where(group == 2, low, zero))
    ).astype(bf16)


def blocks_of(rows):
    left = rows[:, :HALF].reshape(N_SEQ, 1, 8, HALF)
    right = rows[:, HALF:].reshape(N_SEQ, 1, 8, HALF)
    return jnp.concatenate([left, right], axis=1).reshape(N_SEQ, 16, HALF)


def rows_of(blocks):
    count = blocks.shape[0]
    split = blocks.reshape(count, 2, 8, HALF)
    return split[:, 0].reshape(count * 8, HALF), split[:, 1].reshape(count * 8, HALF)


INPUTS = (
    "x_in", "z_in", "bc_in", "raw_hbm", "ids_hbm", "cnt_hbm", "tgt_in", "w_hbm", "dec_hbm", "bias_hbm", "skip_hbm", "gain_hbm",
)
OUTPUTS = ("packed_out",)
PARTS = "yxz"
WIDTH = {"y": 256, "x": 128, "z": 128}
FIRST = {"y": 0, "x": 256, "z": 384}


def scratch():
    dma, v = pltpu.SemaphoreType.DMA, pltpu.VMEM
    rows_f, wide_f, wide_b = v((TOK, 128), f32), v((TOK, WIDE), f32), v((TOK, WIDE), bf16)
    states, sixteen = v((CHUNKS + 1, STATE, WIDE), f32), v((2, N_SEQ, 16, HALF // 2), bf16)
    small, small16, small8 = v((16, 128), f32), v((N_SEQ, 16, 128), f32), v((N_DP, 16, 128), f32)
    named = dict(
        raw_in=v((HEADS, TOK), f32), ids_ref=v((1, TOK), jnp.int32), cnt_ref=pltpu.SMEM((N_DP,), jnp.int32),
        dec_in=v((1, HEADS), f32), bias_in=v((1, HEADS), f32), skip_in=v((1, HEADS), f32),
        x_ref=wide_b, z_ref=wide_b, bc_ref=v((TOK, 2 * STATE), bf16), tgt_ref=wide_b, s_in=dma((12,)),
        act=wide_f, gat=wide_f, dnf=wide_f, gdn=wide_f, invs=rows_f,
        ex=v((128, WIDE), bf16), red=v((WIDE, 128), bf16), tri=v((CHUNK, CHUNK), f32), par=v((3, 8, 128), f32),
        gain=v((1, WIDE), f32), wown=v((8, WIDE), f32), rawt=rows_f, wid=rows_f, dec_s=rows_f, ent=rows_f,
        chain=v((8, WIDE), f32), fcol=v((CHUNKS, CHUNK, CHUNK), f32), sc=v((CHUNKS, CHUNK, CHUNK), f32),
        xw=wide_b, wtd=wide_b, yin=wide_f, eexp=wide_f, gstate=v((CHUNKS, STATE, WIDE), f32), hst=states, apart=states,
        normb=wide_b, ogb=wide_b, gb=wide_b, q2a=rows_f, ds1=rows_f, accs=v((2, 8, WIDE), f32),
        hs=sixteen, hr=sixteen, hp=sixteen, hi=sixteen, gs=sixteen, gr=sixteen, gp=sixteen, gi=sixteen,
        cs=v((8, 128), f32), cr=v((N_SEQ, 8, 128), f32), wfull=v((WIDE, WIDE), bf16),
        wgp=v((N_Y, N_SEQ, 16, HALF), bf16), pr=v((N_Y, N_SEQ, 16, HALF), bf16),
        sa=small, sar=small16, sb2=small, sbr=small8, t1=v((1, 128), f32),
        t2r=v((128, 1, 128), f32),
    )
    for p in PARTS:
        w = WIDTH[p]
        named["ag" + p] = v((128, 16, w), bf16)
        named["sb" + p] = v((64, 16, w), bf16)
        named["ra" + p] = v((3, N_SEQ, 16, w), bf16)
        named["mid" + p] = v((N_SEQ, 16, w), bf16)
        named["rb" + p] = v((N_SEQ, 16, w), bf16)
    for name, count in dict(s_ps=4, s_pr=4, g1s=3, g1r=3, g2s=3, g2r=3, g3s=3, g3r=3, r1s=3, r1r=3, r2s=3, r2r=3).items():
        named[name] = dma((count,))
    named["s_send"] = dma((9, 2))
    named["s_recv"] = dma((9, 2))
    return named


def kernel(*refs):
    names = INPUTS + OUTPUTS + tuple(scratch())
    assert len(names) == len(refs)
    program(**dict(zip(names, refs)))


def program(
    x_in, z_in, bc_in, raw_hbm, ids_hbm, cnt_hbm, tgt_in, w_hbm, dec_hbm, bias_hbm, skip_hbm, gain_hbm,
    packed_out, raw_in, ids_ref, cnt_ref, dec_in, bias_in, skip_in, x_ref, z_ref, bc_ref, tgt_ref, s_in, act, gat, dnf, gdn, invs,
    ex, red, tri, par, gain, wown, rawt, wid, dec_s, ent, chain, fcol, sc,
    xw, wtd, yin, eexp, gstate, hst, apart, normb, ogb, gb, q2a, ds1, accs,
    hs, hr, hp, hi, gs, gr, gp, gi, cs, cr, wfull, wgp, pr, sa, sar, sb2, sbr, t1, t2r,
    s_send, s_recv, s_ps, s_pr, g1s, g1r, g2s, g2r, g3s, g3r, r1s, r1r, r2s, r2r, **part,
):
    dp, seq = lax.axis_index(DP), lax.axis_index(SEQ)
    yy, core = dp // 2, dp % 2
    partner = dp + 1 - 2 * core
    own_b = dp * N_SEQ + seq
    xx, zz = seq // 4, seq % 4
    place = {"y": yy, "x": xx, "z": zz}
    MESH = pl.DeviceIdType.MESH

    def at(d, s):
        return {DP: d, SEQ: s}

    def remote(src, dst, ss, rs, d, s):
        return pltpu.make_async_remote_copy(
            src_ref=src, dst_ref=dst, send_sem=ss, recv_sem=rs, device_id=at(d, s), device_id_type=MESH
        )

    incoming = (
        (dec_hbm, dec_in), (bias_hbm, bias_in), (skip_hbm, skip_in), (raw_hbm, raw_in), (ids_hbm, ids_ref), (bc_in, bc_ref),
        (x_in, x_ref), (w_hbm, wown), (gain_hbm, gain), (z_in, z_ref), (tgt_in, tgt_ref), (cnt_hbm, cnt_ref),
    )
    loads = [pltpu.make_async_copy(source, target, s_in.at[n]) for n, (source, target) in enumerate(incoming)]
    for load in loads:
        load.start()

    barrier = pltpu.get_barrier_semaphore()

    dps = [((yy + k) % 4) * 2 + core for k in range(4)]
    seqs = {(a, b): ((xx + a) % 4) * 4 + (zz + b) % 4 for a in range(4) for b in range(4)}

    def hops(offset):
        return sum(min(k, 4 - k) for k in offset)

    chips = [(a, b, c) for a in range(4) for b in range(4) for c in range(4)]
    far_first = sorted(chips[1:], key=lambda offset: -hops(offset))
    everyone = []
    for a, b, c in far_first + chips[:1]:
        for flip in (0, 1):
            if (a, b, c, flip) != (0, 0, 0, 0):
                everyone.append((dps[a] + flip * (1 - 2 * core), seqs[b, c]))
    for d, s in everyone:
        pl.semaphore_signal(barrier, 1, device_id=at(d, s), device_id_type=MESH)

    row = iota((CHUNK, WIDE), 0)
    col = iota((CHUNK, WIDE), 1)
    ex[...] = jnp.where(((row & 15) == (col >> 6)) & (row < 48), 1.0, 0.0).astype(bf16)
    rrow = iota((WIDE, 128), 0)
    rcol = iota((WIDE, 128), 1)
    ti, tj = iota((CHUNK, CHUNK), 0), iota((CHUNK, CHUNK), 1)
    tri[...] = jnp.where(ti >= tj, 1.0, 0.0)
    rep = jnp.where(iota((HEADS, 128), 0) == (iota((HEADS, 128), 1) & 15), 1.0, 0.0)

    spread = jnp.where((iota((128, 128), 0) & 15) == (iota((128, 128), 1) & 15), 1.0, 0.0)

    def tiled(ref):
        return jnp.dot(jnp.broadcast_to(ref[...], (8, HEADS)), rep, precision=highest, preferred_element_type=f32)

    for load in loads[:5]:
        load.wait()
    par[0] = tiled(dec_in)
    par[1] = tiled(bias_in)
    par[2] = tiled(skip_in)
    rawt[...] = lax.dot_general(
        raw_in[...], rep, (((0,), (0,)), ((), ())), precision=highest, preferred_element_type=f32
    )
    loads[5].wait()
    loads[11].wait()

    def expand(v):
        return dot(three_parts(v), ex[...])

    def head_sum(v):
        high = v.astype(bf16)
        low = (v - high.astype(f32)).astype(bf16)
        return dot(high, red[...]) + dot(low, red[...])

    lane = iota((1, 128), 1)
    low_half = jnp.where(lane < HEAD, 1.0, 0.0).astype(bf16)
    high_half = jnp.where(lane < HEAD, 0.0, 1.0).astype(bf16)

    total = cnt_ref[0]
    for k in range(1, N_DP):
        total = total + cnt_ref[k]
    total_f = total.astype(f32)
    own_count = cnt_ref[dp]

    def rows(c):
        return pl.ds(pl.multiple_of(c * CHUNK, CHUNK), CHUNK)

    def prepare(c, carry):
        flag = jnp.where(ids_ref[0:1, rows(c)] == 0, 1.0, 0.0)
        flag_col = jnp.broadcast_to(flag, (CHUNK, CHUNK)).T
        seg = dot(tri[...], flag_col)
        fcol[c] = seg
        return carry

    lax.fori_loop(0, CHUNKS, prepare, 0)
    loads[6].wait()
    loads[7].wait()
    loads[8].wait()

    def index_in(p, y, x, z):
        return {"y": y * 16 + x * 4 + z, "x": x * 16 + y * 4 + z, "z": z * 16 + x * 4 + y}[p]

    plane_far = sorted([(a, b) for a in range(4) for b in range(4)][1:], key=lambda offset: -hops(offset))

    def plane_peer(p, a, b):
        if p == "y":
            return dp, seqs[a, b], seqs[a, b]
        if p == "x":
            return dps[a], seqs[0, b], ((yy + a) % 4) * 4 + (zz + b) % 4
        return dps[b], seqs[a, 0], ((xx + a) % 4) * 4 + (yy + b) % 4

    def line_peer(p, k):
        c = (place[p] + k) % 4
        if p == "y":
            return c * 2 + core, seq, c
        if p == "x":
            return dp, c * 4 + zz, c
        return dp, xx * 4 + c, c

    mine_in = {p: index_in(p, yy, xx, zz) for p in PARTS}

    def ag_start():
        for n, p in enumerate(PARTS):
            buf = part["ag" + p]
            lanes = slice(FIRST[p], FIRST[p] + WIDTH[p])
            right = slice(HALF + FIRST[p], HALF + FIRST[p] + WIDTH[p])
            own = core * 64 + mine_in[p]
            buf[own] = jnp.concatenate([wown[:, lanes], wown[:, right]], axis=0).astype(bf16)

            for a, b in plane_far:
                d, s, _ = plane_peer(p, a, b)
                remote(buf.at[own], buf.at[own], g1s.at[n], g1r.at[n], d, s).start()

    def ag_line():
        for n, p in enumerate(PARTS):
            buf = part["ag" + p]
            piece = buf.at[pl.ds(0, 15)]
            remote(piece, piece, g1s.at[n], g1r.at[n], partner, seq).wait_recv()
            slab = buf.at[pl.ds(core * 64 + place[p] * 16, 16)]
            for k in range(1, 4):
                d, s, _ = line_peer(p, k)
                remote(slab, slab, g2s.at[n], g2r.at[n], d, s).start()

    def unpack(p, its_core):
        buf, w, base = part["ag" + p], WIDTH[p], its_core * 64

        def one(y, carry):
            d = y * 2 + its_core
            if p == "y":
                blocks = [buf[pl.ds(base + y * 16, 16)].astype(f32)]
            elif p == "x":
                blocks = [buf[pl.ds(base + x * 16 + y * 4, 4)].astype(f32) for x in range(4)]
            else:
                blocks = [buf[pl.ds(base + z * 16 + x * 4 + y, 1)].astype(f32) for x in range(4) for z in range(4)]
            tops, lows = [], []
            for block in blocks:
                split = block.reshape(block.shape[0], 2, 8, w)
                tops.append(split[:, 0].reshape(-1, w))
                lows.append(split[:, 1].reshape(-1, w))
            wfull[rows(d), FIRST[p] : FIRST[p] + w] = jnp.concatenate(tops, axis=0).astype(bf16)
            wfull[rows(d), HALF + FIRST[p] : HALF + FIRST[p] + w] = jnp.concatenate(lows, axis=0).astype(bf16)
            return carry

        lax.fori_loop(0, N_Y, one, 0)

    def ag_finish():
        for p in "xzy":
            n, buf = PARTS.index(p), part["ag" + p]
            piece = buf.at[pl.ds(0, 48)]
            remote(piece, piece, g2s.at[n], g2r.at[n], partner, seq).wait_recv()
            ours = buf.at[pl.ds(core * 64, 64)]
            remote(ours, ours, g3s.at[n], g3r.at[n], partner, seq).start()
            unpack(p, core)
        for p in "xzy":
            n, buf = PARTS.index(p), part["ag" + p]
            piece = buf.at[pl.ds((1 - core) * 64, 64)]
            remote(piece, piece, g3s.at[n], g3r.at[n], partner, seq).wait_recv()
            unpack(p, 1 - core)

    def ag_sent():
        for n, p in enumerate(PARTS):
            buf = part["ag" + p]
            for count, ss, rs in ((15, g1s, g1r), (48, g2s, g2r), (64, g3s, g3r)):
                piece = buf.at[pl.ds(0, count)]
                remote(piece, piece, ss.at[n], rs.at[n], partner, seq).wait_send()

    def exchange_start(src, dst, n, h):
        for a, b in plane_far:
            peer = seqs[a, b]
            remote(src.at[h, peer], dst.at[h, seq], s_send.at[n, h], s_recv.at[n, h], dp, peer).start()
        dst[h, seq] = src[h, seq]

    def spread_start(src, dst, n):
        for a, b in plane_far:
            remote(src, dst.at[seq], s_send.at[n, 0], s_recv.at[n, 0], dp, seqs[a, b]).start()
        dst[seq] = src[...]

    def cross_start(src, dst, n):
        for k in range(1, N_DP):
            remote(src, dst.at[dp], s_send.at[n, 0], s_recv.at[n, 0], (dp + k) % N_DP, seq).start()
        dst[dp] = src[...]

    def recv_wait(dst, n, count, h=0):
        piece = dst.at[pl.ds(0, count)]
        remote(piece, piece, s_send.at[n, h], s_recv.at[n, h], partner, seq).wait_recv()

    def send_wait(dst, n, count, h=0):
        piece = dst.at[pl.ds(0, count)]
        remote(piece, piece, s_send.at[n, h], s_recv.at[n, h], partner, seq).wait_send()

    def one_step(step, losses):
        dec_t, bias_t, skip_t = par[0, 0:1], par[1, 0:1], par[2, 0:1]
        rate = jnp.exp(dec_t)

        pre = rawt[...] + bias_t
        u = jnp.exp(-jnp.abs(pre))
        v = 1.0 + u
        log1p = jnp.where(v == 1.0, u, jnp.log(v) * u / jnp.where(v == 1.0, 1.0, v - 1.0))
        widths = jnp.maximum(pre, 0.0) + log1p
        wid[...] = widths
        sub8, lane8 = iota((8, 128), 0), iota((8, 128), 1)
        through = jnp.zeros((8, 128), f32)
        carried = jnp.ones((1, 128), f32)
        for c in range(CHUNKS):
            span = slice(c * CHUNK, (c + 1) * CHUNK)
            seg = fcol[c]
            width = widths[span]
            s = jnp.dot(tri[...], -rate * width, precision=highest, preferred_element_type=f32)
            last = s[CHUNK - 1 : CHUNK]
            seg_last = seg[CHUNK - 1 : CHUNK]
            leaving = jnp.exp(last - s) * jnp.where(seg == seg_last, 1.0, 0.0)
            passing = jnp.exp(last) * jnp.where(seg_last == 0.0, 1.0, 0.0)
            dec_s[span] = s
            ent[span] = jnp.exp(s) * jnp.where(seg == 0.0, 1.0, 0.0)
            weighted = (x_ref[span].astype(f32) * expand(width * leaving)).astype(bf16)
            wtd[span] = weighted
            gstate[c] = dot_tn(bc_ref[span, :STATE], weighted)
            through = jnp.where(sub8 == c, passing, through)
            carried = carried * passing
        chain[...] = expand(through)
        wide8 = jnp.broadcast_to(carried, (8, 128))
        even = jnp.sum(jnp.where(lane8 == 2 * sub8, wide8, 0.0), axis=1, keepdims=True)
        odd = jnp.sum(jnp.where(lane8 == 2 * sub8 + 1, wide8, 0.0), axis=1, keepdims=True)
        cs[...] = jnp.where(lane8 < HEAD, even, odd)
        hst[0] = gstate[2] + chain[2:3] * (gstate[1] + chain[1:2] * gstate[0])

        def to_blocks(state, out):
            for r in range(8):
                for h in range(2):
                    for q in range(2):
                        first = HALF * h + 256 * q
                        out[q, 2 * r + h] = state[16 * r : 16 * r + 16, first : first + 256].astype(bf16)

        def from_blocks(source, put):
            for q in range(2):
                for r in range(8):
                    for h in range(2):
                        first = HALF * h + 256 * q
                        put(slice(16 * r, 16 * r + 16), slice(first, first + 256), source[q, 2 * r + h].astype(f32))

        to_blocks(hst[0], hs)

        @pl.when(step == 0)
        def _():
            pl.semaphore_wait(barrier, 127)
            ag_start()

        exchange_start(hs, hr, 0, 0)
        spread_start(cs, cr, 1)
        exchange_start(hs, hr, 0, 1)

        @pl.when(step == 0)
        def _():
            loads[9].wait()
            red[...] = jnp.where((rrow >> 6) == (rcol & 15), 1.0, 0.0).astype(bf16)

            def once(c, carry):
                z_f = z_ref[rows(c)].astype(f32)
                act[rows(c)] = z_f / (1.0 + jnp.exp(-z_f))
                scores = dot_nt(bc_ref[rows(c), STATE:], bc_ref[rows(c), :STATE])
                sc[c] = jnp.where((fcol[c] == fcol[c].T) & (ti >= tj), scores, 0.0)
                return carry

            lax.fori_loop(0, CHUNKS, once, 0)
            loads[10].wait()

        skip_e = expand(jnp.broadcast_to(skip_t, (8, 128)))[0:1]
        gain_e = gain[...]

        def inside(c, carry):
            s = dec_s[rows(c)]
            s_t = s.T
            scores = sc[c]
            xw[rows(c)] = (x_ref[rows(c)].astype(f32) * expand(wid[rows(c)])).astype(bf16)
            eexp[rows(c)] = expand(ent[rows(c)])
            for p in range(PAIRS):
                parts = []
                for h in (2 * p, 2 * p + 1):
                    gap = jnp.minimum(s[:, h : h + 1] - s_t[h : h + 1, :], 0.0)
                    parts.append((jnp.exp(gap) * scores).astype(bf16))
                mine = xw[rows(c), 128 * p : 128 * (p + 1)]
                both = jnp.concatenate([mine * low_half, mine * high_half], axis=0)
                lanes = slice(128 * p, 128 * (p + 1))
                direct = skip_e[:, lanes] * x_ref[rows(c), lanes].astype(f32)
                yin[rows(c), lanes] = dot(jnp.concatenate(parts, axis=1), both) + direct
            return carry

        lax.fori_loop(0, CHUNKS, inside, 0)
        ag_line()

        half = seq % 2

        def scan(source, out, h, order):
            state = [jnp.zeros((16, 128), f32) for _ in range(2)]
            for i in order:
                for m in range(2):
                    lanes = slice(128 * m, 128 * (m + 1))
                    out[h, i, :, lanes] = state[m].astype(bf16)
                    factor = cr[i, pl.ds(4 * half + 2 * h + m, 1), :]
                    state[m] = factor * state[m] + source[h, i, :, lanes].astype(f32)

        recv_wait(cr, 1, 15)
        for h in range(2):
            recv_wait(hr.at[h], 0, 15, h)
            scan(hr, hp, h, range(N_SEQ))
            exchange_start(hp, hi, 2, h)
        ag_finish()
        for h in range(2):
            recv_wait(hi.at[h], 2, 15, h)

        def put_state(at_rows, lanes, value):
            hst[0, at_rows, lanes] = value

        from_blocks(hi, put_state)

        scale = 2.0 / (WIDE * total_f)
        accs[...] = jnp.zeros(accs.shape, f32)

        for c in range(CHUNKS):
            span = slice(c * CHUNK, (c + 1) * CHUNK)
            state = hst[c]
            y = yin[span] + eexp[span] * dot(bc_ref[span, STATE:], state.astype(bf16))
            yin[span] = y
            gated = y * act[span]
            gat[span] = gated
            inv = lax.rsqrt(jnp.sum(gated * gated, axis=1, keepdims=True) * (1.0 / WIDE) + norm_floor)
            invs[span] = jnp.broadcast_to(inv, (CHUNK, 128))
            normb[span] = (gated * gain_e * inv).astype(bf16)
            hst[c + 1] = chain[c : c + 1] * state + gstate[c]
        block = 1024
        position = seq * TOK + iota((TOK, block), 0)
        scored = jnp.where(position < own_count, 1.0, 0.0)
        losses_8 = jnp.zeros((8, block), f32)
        for first in range(0, WIDE, block):
            lanes = slice(first, first + block)
            res = (dot(normb[...], wfull[:, lanes]) - tgt_ref[:, lanes].astype(f32)) * scored
            losses_8 = losses_8 + jnp.sum((res * res).reshape(TOK // 8, 8, block), axis=0)
            ogb[:, lanes] = (res * scale).astype(bf16)
        loss = jnp.sum(jnp.sum(losses_8, axis=1, keepdims=True), axis=0, keepdims=True)
        inner_l = jnp.zeros((TOK, 128), f32)
        for first in range(0, WIDE, block):
            lanes = slice(first, first + block)
            d_norm = dot_nt(ogb[...], wfull[lanes, :])
            dnf[:, lanes] = d_norm
            d_gain = d_norm * gain_e[:, lanes]
            gdn[:, lanes] = d_gain
            term = d_gain * gat[:, lanes]
            for k in range(0, block, 128):
                inner_l = inner_l + term[:, k : k + 128]
        inner = jnp.sum(inner_l, axis=1, keepdims=True) * (1.0 / WIDE)
        for c in range(CHUNKS):
            span = slice(c * CHUNK, (c + 1) * CHUNK)
            inv = invs[span, 0:1]
            g = (gdn[span] - gat[span] * (inv * inv * inner[span])) * inv * act[span]
            gb[span] = g.astype(bf16)
            apart[c] = dot_tn(bc_ref[span, STATE:], (g * eexp[span]).astype(bf16))
        entry = apart[0] + chain[0:1] * (apart[1] + chain[1:2] * apart[2])
        to_blocks(entry, gs)
        for h in range(2):
            exchange_start(gs, gr, 3, h)
        def grad_rows(first, second):
            lanes = [normb[:, pl.ds(pl.multiple_of(d * 128, 128), 128)] for d in (first, second)]
            both = dot_tn(jnp.concatenate(lanes, axis=1), ogb[...])
            return blocks_of(both[:128]), blocks_of(both[128:])

        def group(k, c):
            return ((yy + k) % N_Y) * 2 + c

        for pair in ((1, 2), (3, 0)):
            pieces = grad_rows(*[group(k, 1 - core) for k in pair])
            for k, piece in zip(pair, pieces):
                wgp[k] = piece.astype(bf16)
                remote(wgp.at[k], pr.at[k], s_ps.at[k], s_pr.at[k], partner, seq).start()
        for pair in ((1, 2), (3, 0)):
            pieces = grad_rows(*[group(k, core) for k in pair])
            for k, mine in zip(pair, pieces):
                y_k = (yy + k) % N_Y
                remote(wgp.at[k], pr.at[k], s_ps.at[k], s_pr.at[k], partner, seq).wait_recv()
                both = (mine + pr[k].astype(f32)).astype(bf16)
                part["sby"][pl.ds(y_k * 16, 16)] = both[:, :, : WIDTH["y"]]
                if k > 0:
                    slab = part["sby"].at[pl.ds(y_k * 16, 16)]
                    remote(slab, part["ray"].at[k - 1], r1s.at[0], r1r.at[0], y_k * 2 + core, seq).start()
                for p in "xz":
                    piece = both[:, :, FIRST[p] : FIRST[p] + WIDTH[p]]
                    for x in range(4):
                        if p == "x":
                            part["sbx"][pl.ds(x * 16 + y_k * 4, 4)] = piece[4 * x : 4 * x + 4]
                        else:
                            for z in range(4):
                                part["sbz"][z * 16 + x * 4 + y_k] = piece[4 * x + z]
        for n, p in ((1, "x"), (2, "z")):
            for k in range(1, 4):
                d, s, c = line_peer(p, k)
                slab = part["sb" + p].at[pl.ds(c * 16, 16)]
                remote(slab, part["ra" + p].at[k - 1], r1s.at[n], r1r.at[n], d, s).start()

        def small_sums(c, carry):
            x_f, inv = x_ref[rows(c)].astype(f32), invs[rows(c), 0:1]
            accs[0] += jnp.sum((dnf[rows(c)] * gat[rows(c)] * inv).reshape(16, 8, WIDE), axis=0)
            accs[1] += jnp.sum((gb[rows(c)].astype(f32) * x_f).reshape(16, 8, WIDE), axis=0)
            return carry

        lax.fori_loop(0, CHUNKS, small_sums, 0)
        gain_g = jnp.sum(accs[0], axis=0, keepdims=True)
        for r in range(8):
            sa[r : r + 1, :] = gain_g[:, 128 * r : 128 * (r + 1)]
        skip_g = head_sum(jnp.broadcast_to(jnp.sum(accs[1], axis=0, keepdims=True), (8, WIDE)))
        sub = iota((8, 128), 0)
        sa[8:16, :] = jnp.where(sub == 0, skip_g, jnp.where(sub == 1, jnp.broadcast_to(loss, (8, 128)), 0.0))
        spread_start(sa, sar, 4)

        def scatter_plane():
            for p in "xzy":
                n = PARTS.index(p)
                got, mid, dst = part["ra" + p], part["mid" + p], part["rb" + p]
                remote(got, got, r1s.at[n], r1r.at[n], partner, seq).wait_recv()
                value = part["sb" + p][pl.ds(place[p] * 16, 16)].astype(f32)
                for k in range(3):
                    value = value + got[k].astype(f32)
                mid[...] = value.astype(bf16)
                here = mine_in[p] % 16
                for a, b in plane_far:
                    d, s, q = plane_peer(p, a, b)
                    remote(mid.at[q], dst.at[here], r2s.at[n], r2r.at[n], d, s).start()
                dst[here] = mid[here]

        def inside_back(c, carry):
            s = dec_s[rows(c)]
            s_t = s.T
            scores = sc[c].T
            for p in range(PAIRS):
                parts = []
                for h in (2 * p, 2 * p + 1):
                    gap = jnp.minimum(s_t[h : h + 1, :] - s[:, h : h + 1], 0.0)
                    parts.append((jnp.exp(gap) * scores).astype(bf16))
                mine = gb[rows(c), 128 * p : 128 * (p + 1)]
                both = jnp.concatenate([mine * low_half, mine * high_half], axis=0)
                lanes = slice(128 * p, 128 * (p + 1))
                eexp[rows(c), lanes] = dot(jnp.concatenate(parts, axis=1), both)
            g_f, x_f = gb[rows(c)].astype(f32), x_ref[rows(c)].astype(f32)
            ds1[rows(c)] = head_sum(g_f * (yin[rows(c)] - skip_e * x_f))
            q2a[rows(c)] = head_sum(xw[rows(c)].astype(f32) * eexp[rows(c)])
            return carry

        lax.fori_loop(0, CHUNKS - 1, inside_back, 0)

        for h in range(2):
            recv_wait(gr.at[h], 3, 15, h)
            scan(gr, gp, h, range(N_SEQ - 1, -1, -1))
            exchange_start(gp, gi, 5, h)
        lax.fori_loop(CHUNKS - 1, CHUNKS, inside_back, 0)

        scatter_plane()

        def summed(ref, count):
            value = ref[0]
            for k in range(1, count):
                value = value + ref[k]
            return value

        recv_wait(sar, 4, 15)
        sb2[...] = summed(sar, N_SEQ)
        cross_start(sb2, sbr, 6)

        for h in range(2):
            recv_wait(gi.at[h], 5, 15, h)

        def put_after(at_rows, lanes, value):
            apart[3, at_rows, lanes] = value

        from_blocks(gi, put_after)
        apart[2] = apart[2] + chain[2:3] * apart[3]
        apart[1] = apart[1] + chain[1:2] * apart[2]

        dec_g = bias_g = jnp.zeros((1, 128), f32)
        sig = 1.0 / (1.0 + jnp.exp(-(rawt[...] + bias_t)))
        for c in range(CHUNKS):
            span = slice(c * CHUNK, (c + 1) * CHUNK)
            after = apart[c + 1]
            width = wid[span]
            z_t = dot(bc_ref[span, :STATE], after.astype(bf16))
            q2 = q2a[span] + head_sum(wtd[span].astype(f32) * z_t)
            ends = jnp.sum((after * hst[c + 1]).reshape(16, 8, WIDE), axis=0)
            end_h = jnp.sum(head_sum(ends), axis=0, keepdims=True)
            d_a = lax.dot_general(
                tri[...], ds1[span] - q2, (((0,), (0,)), ((), ())), precision=highest, preferred_element_type=f32
            ) + end_h
            d_w = q2 / width - rate * d_a
            dec_g = dec_g - jnp.sum(d_a * (rate * width), axis=0, keepdims=True)
            bias_g = bias_g + jnp.sum(d_w * sig[span], axis=0, keepdims=True)

        recv_wait(sbr, 6, 7)
        sums_a = summed(sbr, N_DP)

        ag_sent()

        grad, square = {}, jnp.zeros((1, 1), f32)
        for n, p in enumerate(PARTS):
            dst = part["rb" + p]
            got = dst.at[pl.ds(0, 15)]
            remote(got, got, r2s.at[n], r2r.at[n], partner, seq).wait_recv()
            value = dst[0].astype(f32)
            for q in range(1, 16):
                value = value + dst[q].astype(f32)
            grad[p] = value
            square = square + jnp.sum(jnp.sum(value * value, axis=1, keepdims=True), axis=0, keepdims=True)
        t1[...] = jnp.where(lane < 16, dec_g, jnp.where(lane < 32, bias_g, jnp.where(lane == 32, square, 0.0)))
        for d, q in everyone:
            remote(t1, t2r.at[own_b], s_send.at[8, 0], s_recv.at[8, 0], d, q).start()
        t2r[own_b] = t1[...]
        recv_wait(t2r, 8, 127)
        sums_b = jnp.sum(t2r[...], axis=0)

        picked = jnp.where(sub8 == (lane8 >> 4), jnp.broadcast_to(sums_b, (8, 128)), 0.0)
        heads = jnp.dot(picked, spread, precision=highest, preferred_element_type=f32)
        dec_g, bias_g = heads[0:1], heads[1:2]
        squares = jnp.sum(jnp.where(lane == 32, sums_b, 0.0), axis=1, keepdims=True)
        gain_rows, skip_g, loss_all = sums_a[0:8], sums_a[8:9], sums_a[9:10]
        small = jnp.sum(
            jnp.where(lane < HEADS, dec_g * dec_g + bias_g * bias_g + skip_g * skip_g, 0.0), axis=1, keepdims=True
        )
        gains = jnp.sum(jnp.sum(gain_rows * gain_rows, axis=1, keepdims=True), axis=0, keepdims=True)
        norm = jnp.sqrt(squares + (small + gains))
        move = learn_rate * (clip_limit / jnp.maximum(norm, clip_limit))
        par[0] = jnp.broadcast_to(dec_t - move * dec_g, (8, 128))
        par[1] = jnp.broadcast_to(bias_t - move * bias_g, (8, 128))
        par[2] = jnp.broadcast_to(skip_t - move * skip_g, (8, 128))
        for r in range(8):
            lanes = slice(128 * r, 128 * (r + 1))
            gain[:, lanes] = gain[:, lanes] - move * gain_rows[r : r + 1]
        for p in PARTS:
            for h in range(2):
                lanes = slice(HALF * h + FIRST[p], HALF * h + FIRST[p] + WIDTH[p])
                wown[:, lanes] = wown[:, lanes] - move * grad[p][8 * h : 8 * h + 8]

        for h in range(2):
            send_wait(hr.at[h], 0, 15, h)
        send_wait(cr, 1, 15)
        for h in range(2):
            send_wait(hi.at[h], 2, 15, h)
        for h in range(2):
            send_wait(gr.at[h], 3, 15, h)
        send_wait(sar, 4, 15)
        for h in range(2):
            send_wait(gi.at[h], 5, 15, h)
        send_wait(sbr, 6, 7)
        send_wait(t2r, 8, 127)
        for k in range(N_Y):
            remote(wgp.at[k], pr.at[k], s_ps.at[k], s_pr.at[k], partner, seq).wait_send()
        for n, p in enumerate(PARTS):
            got, dst = part["ra" + p], part["rb" + p].at[pl.ds(0, 15)]
            remote(got, got, r1s.at[n], r1r.at[n], partner, seq).wait_send()
            remote(dst, dst, r2s.at[n], r2r.at[n], partner, seq).wait_send()

        @pl.when(step == 0)
        def _():
            ag_start()

        step_loss = loss_all[:, 0:1] * (1.0 / WIDE) / total_f
        return jnp.where(iota((1, STEPS), 1) == step, step_loss, losses)

    losses = lax.fori_loop(0, STEPS, one_step, jnp.zeros((1, STEPS), f32))
    packed_out[0:8] = wown[...]
    packed_out[8:9] = gain[...]
    packed_out[9:10, :] = jnp.zeros((1, WIDE), f32)
    for n in range(3):
        packed_out[9:10, 128 * n : 128 * (n + 1)] = par[n, 0:1]
    packed_out[9:10, 384 : 384 + STEPS] = losses


def split_kernel(packed, loss_out, w_out, dec_out, bias_out, skip_out, gain_out):
    w_out[...] = packed[0:8]
    gain_out[...] = packed[8:9]
    dec_out[...] = packed[9:10, 0:HEADS]
    bias_out[...] = packed[9:10, 128 : 128 + HEADS]
    skip_out[...] = packed[9:10, 256 : 256 + HEADS]
    loss_out[...] = packed[9:10, 384 : 384 + STEPS]


def per_device(x, z, bc, raw, ids, counts, target, weight, dec, bias, skip, gain):
    vmem = pl.BlockSpec(memory_space=pltpu.VMEM)
    in_hbm = pl.BlockSpec(memory_space=pltpu.HBM)
    shape = jax.ShapeDtypeStruct
    packed = pl.pallas_call(
        kernel,
        out_shape=shape((16, WIDE), f32),
        in_specs=[in_hbm] * 12,
        out_specs=vmem,
        scratch_shapes=list(scratch().values()),
        compiler_params=pltpu.CompilerParams(
            collective_id=0, has_side_effects=True, vmem_limit_bytes=62 * 1024 * 1024
        ),
    )(
        x[0], z[0], bc[0], raw[0].T, ids, counts, target[0], weight,
        dec.reshape(1, HEADS), bias.reshape(1, HEADS), skip.reshape(1, HEADS), gain.reshape(1, WIDE),
    )
    losses, weight, dec, bias, skip, gain = pl.pallas_call(
        split_kernel,
        out_shape=(
            shape((1, STEPS), f32), shape((8, WIDE), f32), shape((1, HEADS), f32), shape((1, HEADS), f32),
            shape((1, HEADS), f32), shape((1, WIDE), f32),
        ),
        in_specs=[vmem],
        out_specs=(vmem,) * 6,
    )(packed)
    return (
        losses.reshape(STEPS), weight, dec.reshape(HEADS), bias.reshape(HEADS), skip.reshape(HEADS), gain.reshape(WIDE)
    )


def solution(mesh):
    tokens = P(DP, SEQ, None)
    return jax.shard_map(
        per_device,
        mesh=mesh,
        in_specs=(
            tokens, tokens, tokens, tokens, P(DP, SEQ), P(), tokens, P((DP, SEQ), None), P(), P(), P(), P(),
        ),
        out_specs=(P(), P((DP, SEQ), None), P(), P(), P(), P()),
        check_vma=False,
    )
```

```python
import jax
import jax.numpy as jnp
from jax import lax
from jax.experimental import pallas as pl
from jax.experimental.pallas import tpu as pltpu
from jax.sharding import PartitionSpec as P

STEPS = 2
DP, SEQ = "dp", "seq"
N_DP, N_SEQ, N_Y = 8, 16, 4
TOK, WIDE, STATE, HEADS, HEAD = 384, 1024, 128, 16, 64
CHUNK, CHUNKS, PAIRS = 128, 3, 8
HALF = WIDE // 2

norm_floor = 1.0
clip_limit = 1.0
learn_rate = 8.0
f32, bf16 = jnp.float32, jnp.bfloat16
highest = lax.Precision.HIGHEST


def dot(a, b):
    return jnp.dot(a, b, preferred_element_type=f32)


def dot_tn(a, b):
    return lax.dot_general(a, b, (((0,), (0,)), ((), ())), preferred_element_type=f32)


def dot_nt(a, b):
    return lax.dot_general(a, b, (((1,), (1,)), ((), ())), preferred_element_type=f32)


def iota(shape, dim):
    return lax.broadcasted_iota(jnp.int32, shape, dim)


def three_parts(v):
    high = v.astype(bf16).astype(f32)
    rest = v - high
    mid = rest.astype(bf16).astype(f32)
    low = rest - mid
    group = (iota(v.shape, 1) >> 4) & 3
    zero = jnp.zeros_like(v)
    return jnp.where(
        group == 0, high, jnp.where(group == 1, mid, jnp.where(group == 2, low, zero))
    ).astype(bf16)


def blocks_of(rows):
    left = rows[:, :HALF].reshape(N_SEQ, 1, 8, HALF)
    right = rows[:, HALF:].reshape(N_SEQ, 1, 8, HALF)
    return jnp.concatenate([left, right], axis=1).reshape(N_SEQ, 16, HALF)


def rows_of(blocks):
    count = blocks.shape[0]
    split = blocks.reshape(count, 2, 8, HALF)
    return split[:, 0].reshape(count * 8, HALF), split[:, 1].reshape(count * 8, HALF)


INPUTS = (
    "x_in", "z_in", "bc_in", "raw_hbm", "ids_hbm", "cnt_hbm", "tgt_in", "w_hbm", "dec_hbm", "bias_hbm", "skip_hbm", "gain_hbm",
)
OUTPUTS = ("packed_out",)
PARTS = "yxz"
WIDTH = {"y": 256, "x": 128, "z": 128}
FIRST = {"y": 0, "x": 256, "z": 384}


def scratch():
    dma, v = pltpu.SemaphoreType.DMA, pltpu.VMEM
    rows_f, wide_f, wide_b = v((TOK, 128), f32), v((TOK, WIDE), f32), v((TOK, WIDE), bf16)
    states, sixteen = v((CHUNKS + 1, STATE, WIDE), f32), v((2, N_SEQ, 16, HALF // 2), bf16)
    small, small16, small8 = v((16, 128), f32), v((N_SEQ, 16, 128), f32), v((N_DP, 16, 128), f32)
    named = dict(
        raw_in=v((HEADS, TOK), f32), ids_ref=v((1, TOK), jnp.int32), cnt_ref=pltpu.SMEM((N_DP,), jnp.int32),
        dec_in=v((1, HEADS), f32), bias_in=v((1, HEADS), f32), skip_in=v((1, HEADS), f32),
        x_ref=wide_b, z_ref=wide_b, bc_ref=v((TOK, 2 * STATE), bf16), tgt_ref=wide_b, s_in=dma((12,)),
        act=wide_f, gat=wide_f, dnf=wide_f, gdn=wide_f, invs=rows_f,
        ex=v((128, WIDE), bf16), red=v((WIDE, 128), bf16), tri=v((CHUNK, CHUNK), f32), par=v((3, 8, 128), f32),
        gain=v((1, WIDE), f32), wown=v((8, WIDE), f32), rawt=rows_f, wid=rows_f, dec_s=rows_f, ent=rows_f,
        chain=v((8, WIDE), f32), fcol=v((CHUNKS, CHUNK, CHUNK), f32), sc=v((CHUNKS, CHUNK, CHUNK), f32),
        xw=wide_b, wtd=wide_b, yin=wide_f, eexp=wide_f, gstate=v((CHUNKS, STATE, WIDE), f32), hst=states, apart=states,
        normb=wide_b, ogb=wide_b, gb=wide_b, q2a=rows_f, ds1=rows_f, accs=v((2, 8, WIDE), f32),
        hs=sixteen, hr=sixteen, hp=sixteen, hi=sixteen, gs=sixteen, gr=sixteen, gp=sixteen, gi=sixteen,
        cs=v((8, 128), f32), cr=v((N_SEQ, 8, 128), f32), wfull=v((WIDE, WIDE), bf16),
        wgp=v((N_Y, N_SEQ, 16, HALF), bf16), pr=v((N_Y, N_SEQ, 16, HALF), bf16),
        sa=small, sar=small16, sb2=small, sbr=small8, t1=v((1, 128), f32),
        t2r=v((128, 1, 128), f32),
    )
    for p in PARTS:
        w = WIDTH[p]
        named["ag" + p] = v((128, 16, w), bf16)
        named["sb" + p] = v((64, 16, w), bf16)
        named["ra" + p] = v((3, N_SEQ, 16, w), bf16)
        named["mid" + p] = v((N_SEQ, 16, w), bf16)
        named["rb" + p] = v((N_SEQ, 16, w), bf16)
    for name, count in dict(s_ps=4, s_pr=4, g1s=3, g1r=3, g2s=3, g2r=3, g3s=3, g3r=3, r1s=3, r1r=3, r2s=3, r2r=3).items():
        named[name] = dma((count,))
    named["s_send"] = dma((9, 2))
    named["s_recv"] = dma((9, 2))
    return named


def kernel(*refs):
    names = INPUTS + OUTPUTS + tuple(scratch())
    assert len(names) == len(refs)
    program(**dict(zip(names, refs)))


def program(
    x_in, z_in, bc_in, raw_hbm, ids_hbm, cnt_hbm, tgt_in, w_hbm, dec_hbm, bias_hbm, skip_hbm, gain_hbm,
    packed_out, raw_in, ids_ref, cnt_ref, dec_in, bias_in, skip_in, x_ref, z_ref, bc_ref, tgt_ref, s_in, act, gat, dnf, gdn, invs,
    ex, red, tri, par, gain, wown, rawt, wid, dec_s, ent, chain, fcol, sc,
    xw, wtd, yin, eexp, gstate, hst, apart, normb, ogb, gb, q2a, ds1, accs,
    hs, hr, hp, hi, gs, gr, gp, gi, cs, cr, wfull, wgp, pr, sa, sar, sb2, sbr, t1, t2r,
    s_send, s_recv, s_ps, s_pr, g1s, g1r, g2s, g2r, g3s, g3r, r1s, r1r, r2s, r2r, **part,
):
    dp, seq = lax.axis_index(DP), lax.axis_index(SEQ)
    yy, core = dp // 2, dp % 2
    partner = dp + 1 - 2 * core
    own_b = dp * N_SEQ + seq
    xx, zz = seq // 4, seq % 4
    place = {"y": yy, "x": xx, "z": zz}
    MESH = pl.DeviceIdType.MESH

    def at(d, s):
        return {DP: d, SEQ: s}

    def remote(src, dst, ss, rs, d, s):
        return pltpu.make_async_remote_copy(
            src_ref=src, dst_ref=dst, send_sem=ss, recv_sem=rs, device_id=at(d, s), device_id_type=MESH
        )

    incoming = (
        (dec_hbm, dec_in), (bias_hbm, bias_in), (skip_hbm, skip_in), (raw_hbm, raw_in), (ids_hbm, ids_ref), (bc_in, bc_ref),
        (x_in, x_ref), (w_hbm, wown), (gain_hbm, gain), (z_in, z_ref), (tgt_in, tgt_ref), (cnt_hbm, cnt_ref),
    )
    loads = [pltpu.make_async_copy(source, target, s_in.at[n]) for n, (source, target) in enumerate(incoming)]
    for load in loads:
        load.start()

    barrier = pltpu.get_barrier_semaphore()

    dps = [((yy + k) % 4) * 2 + core for k in range(4)]
    seqs = {(a, b): ((xx + a) % 4) * 4 + (zz + b) % 4 for a in range(4) for b in range(4)}

    def hops(offset):
        return sum(min(k, 4 - k) for k in offset)

    chips = [(a, b, c) for a in range(4) for b in range(4) for c in range(4)]
    far_first = sorted(chips[1:], key=lambda offset: -hops(offset))
    everyone = []
    for a, b, c in far_first + chips[:1]:
        for flip in (0, 1):
            if (a, b, c, flip) != (0, 0, 0, 0):
                everyone.append((dps[a] + flip * (1 - 2 * core), seqs[b, c]))
    for d, s in everyone:
        pl.semaphore_signal(barrier, 1, device_id=at(d, s), device_id_type=MESH)

    row = iota((CHUNK, WIDE), 0)
    col = iota((CHUNK, WIDE), 1)
    ex[...] = jnp.where(((row & 15) == (col >> 6)) & (row < 48), 1.0, 0.0).astype(bf16)
    rrow = iota((WIDE, 128), 0)
    rcol = iota((WIDE, 128), 1)
    ti, tj = iota((CHUNK, CHUNK), 0), iota((CHUNK, CHUNK), 1)
    tri[...] = jnp.where(ti >= tj, 1.0, 0.0)
    rep = jnp.where(iota((HEADS, 128), 0) == (iota((HEADS, 128), 1) & 15), 1.0, 0.0)

    spread = jnp.where((iota((128, 128), 0) & 15) == (iota((128, 128), 1) & 15), 1.0, 0.0)

    def tiled(ref):
        return jnp.dot(jnp.broadcast_to(ref[...], (8, HEADS)), rep, precision=highest, preferred_element_type=f32)

    for load in loads[:5]:
        load.wait()
    par[0] = tiled(dec_in)
    par[1] = tiled(bias_in)
    par[2] = tiled(skip_in)
    rawt[...] = lax.dot_general(
        raw_in[...], rep, (((0,), (0,)), ((), ())), precision=highest, preferred_element_type=f32
    )
    loads[5].wait()
    loads[11].wait()

    def expand(v):
        return dot(three_parts(v), ex[...])

    def head_sum(v):
        high = v.astype(bf16)
        low = (v - high.astype(f32)).astype(bf16)
        return dot(high, red[...]) + dot(low, red[...])

    lane = iota((1, 128), 1)
    low_half = jnp.where(lane < HEAD, 1.0, 0.0).astype(bf16)
    high_half = jnp.where(lane < HEAD, 0.0, 1.0).astype(bf16)

    total = cnt_ref[0]
    for k in range(1, N_DP):
        total = total + cnt_ref[k]
    total_f = total.astype(f32)
    own_count = cnt_ref[dp]

    def rows(c):
        return pl.ds(pl.multiple_of(c * CHUNK, CHUNK), CHUNK)

    def prepare(c, carry):
        flag = jnp.where(ids_ref[0:1, rows(c)] == 0, 1.0, 0.0)
        flag_col = jnp.broadcast_to(flag, (CHUNK, CHUNK)).T
        seg = dot(tri[...], flag_col)
        fcol[c] = seg
        return carry

    lax.fori_loop(0, CHUNKS, prepare, 0)
    loads[6].wait()
    loads[7].wait()
    loads[8].wait()

    def index_in(p, y, x, z):
        return {"y": y * 16 + x * 4 + z, "x": x * 16 + y * 4 + z, "z": z * 16 + x * 4 + y}[p]

    plane_far = sorted([(a, b) for a in range(4) for b in range(4)][1:], key=lambda offset: -hops(offset))

    def plane_peer(p, a, b):
        if p == "y":
            return dp, seqs[a, b], seqs[a, b]
        if p == "x":
            return dps[a], seqs[0, b], ((yy + a) % 4) * 4 + (zz + b) % 4
        return dps[b], seqs[a, 0], ((xx + a) % 4) * 4 + (yy + b) % 4

    def line_peer(p, k):
        c = (place[p] + k) % 4
        if p == "y":
            return c * 2 + core, seq, c
        if p == "x":
            return dp, c * 4 + zz, c
        return dp, xx * 4 + c, c

    mine_in = {p: index_in(p, yy, xx, zz) for p in PARTS}

    def ag_start():
        for n, p in enumerate(PARTS):
            buf = part["ag" + p]
            lanes = slice(FIRST[p], FIRST[p] + WIDTH[p])
            right = slice(HALF + FIRST[p], HALF + FIRST[p] + WIDTH[p])
            own = core * 64 + mine_in[p]
            buf[own] = jnp.concatenate([wown[:, lanes], wown[:, right]], axis=0).astype(bf16)

            for a, b in plane_far:
                d, s, _ = plane_peer(p, a, b)
                remote(buf.at[own], buf.at[own], g1s.at[n], g1r.at[n], d, s).start()

    def ag_line():
        for n, p in enumerate(PARTS):
            buf = part["ag" + p]
            piece = buf.at[pl.ds(0, 15)]
            remote(piece, piece, g1s.at[n], g1r.at[n], partner, seq).wait_recv()
            slab = buf.at[pl.ds(core * 64 + place[p] * 16, 16)]
            for k in range(1, 4):
                d, s, _ = line_peer(p, k)
                remote(slab, slab, g2s.at[n], g2r.at[n], d, s).start()

    def unpack(p, its_core):
        buf, w, base = part["ag" + p], WIDTH[p], its_core * 64

        def one(y, carry):
            d = y * 2 + its_core
            if p == "y":
                blocks = [buf[pl.ds(base + y * 16, 16)].astype(f32)]
            elif p == "x":
                blocks = [buf[pl.ds(base + x * 16 + y * 4, 4)].astype(f32) for x in range(4)]
            else:
                blocks = [buf[pl.ds(base + z * 16 + x * 4 + y, 1)].astype(f32) for x in range(4) for z in range(4)]
            tops, lows = [], []
            for block in blocks:
                split = block.reshape(block.shape[0], 2, 8, w)
                tops.append(split[:, 0].reshape(-1, w))
                lows.append(split[:, 1].reshape(-1, w))
            wfull[rows(d), FIRST[p] : FIRST[p] + w] = jnp.concatenate(tops, axis=0).astype(bf16)
            wfull[rows(d), HALF + FIRST[p] : HALF + FIRST[p] + w] = jnp.concatenate(lows, axis=0).astype(bf16)
            return carry

        lax.fori_loop(0, N_Y, one, 0)

    def ag_finish():
        for p in "xzy":
            n, buf = PARTS.index(p), part["ag" + p]
            piece = buf.at[pl.ds(0, 48)]
            remote(piece, piece, g2s.at[n], g2r.at[n], partner, seq).wait_recv()
            ours = buf.at[pl.ds(core * 64, 64)]
            remote(ours, ours, g3s.at[n], g3r.at[n], partner, seq).start()
            unpack(p, core)
        for p in "xzy":
            n, buf = PARTS.index(p), part["ag" + p]
            piece = buf.at[pl.ds((1 - core) * 64, 64)]
            remote(piece, piece, g3s.at[n], g3r.at[n], partner, seq).wait_recv()
            unpack(p, 1 - core)

    def ag_sent():
        for n, p in enumerate(PARTS):
            buf = part["ag" + p]
            for count, ss, rs in ((15, g1s, g1r), (48, g2s, g2r), (64, g3s, g3r)):
                piece = buf.at[pl.ds(0, count)]
                remote(piece, piece, ss.at[n], rs.at[n], partner, seq).wait_send()

    def exchange_start(src, dst, n, h):
        for a, b in plane_far:
            peer = seqs[a, b]
            remote(src.at[h, peer], dst.at[h, seq], s_send.at[n, h], s_recv.at[n, h], dp, peer).start()
        dst[h, seq] = src[h, seq]

    def spread_start(src, dst, n):
        for a, b in plane_far:
            remote(src, dst.at[seq], s_send.at[n, 0], s_recv.at[n, 0], dp, seqs[a, b]).start()
        dst[seq] = src[...]

    def cross_start(src, dst, n):
        for k in range(1, N_DP):
            remote(src, dst.at[dp], s_send.at[n, 0], s_recv.at[n, 0], (dp + k) % N_DP, seq).start()
        dst[dp] = src[...]

    def recv_wait(dst, n, count, h=0):
        piece = dst.at[pl.ds(0, count)]
        remote(piece, piece, s_send.at[n, h], s_recv.at[n, h], partner, seq).wait_recv()

    def send_wait(dst, n, count, h=0):
        piece = dst.at[pl.ds(0, count)]
        remote(piece, piece, s_send.at[n, h], s_recv.at[n, h], partner, seq).wait_send()

    def one_step(step, losses):
        dec_t, bias_t, skip_t = par[0, 0:1], par[1, 0:1], par[2, 0:1]
        rate = jnp.exp(dec_t)

        pre = rawt[...] + bias_t
        u = jnp.exp(-jnp.abs(pre))
        v = 1.0 + u
        log1p = jnp.where(v == 1.0, u, jnp.log(v) * u / jnp.where(v == 1.0, 1.0, v - 1.0))
        widths = jnp.maximum(pre, 0.0) + log1p
        wid[...] = widths
        sub8, lane8 = iota((8, 128), 0), iota((8, 128), 1)
        through = jnp.zeros((8, 128), f32)
        carried = jnp.ones((1, 128), f32)
        for c in range(CHUNKS):
            span = slice(c * CHUNK, (c + 1) * CHUNK)
            seg = fcol[c]
            width = widths[span]
            s = jnp.dot(tri[...], -rate * width, precision=highest, preferred_element_type=f32)
            last = s[CHUNK - 1 : CHUNK]
            seg_last = seg[CHUNK - 1 : CHUNK]
            leaving = jnp.exp(last - s) * jnp.where(seg == seg_last, 1.0, 0.0)
            passing = jnp.exp(last) * jnp.where(seg_last == 0.0, 1.0, 0.0)
            dec_s[span] = s
            ent[span] = jnp.exp(s) * jnp.where(seg == 0.0, 1.0, 0.0)
            weighted = (x_ref[span].astype(f32) * expand(width * leaving)).astype(bf16)
            wtd[span] = weighted
            gstate[c] = dot_tn(bc_ref[span, :STATE], weighted)
            through = jnp.where(sub8 == c, passing, through)
            carried = carried * passing
        chain[...] = expand(through)
        wide8 = jnp.broadcast_to(carried, (8, 128))
        even = jnp.sum(jnp.where(lane8 == 2 * sub8, wide8, 0.0), axis=1, keepdims=True)
        odd = jnp.sum(jnp.where(lane8 == 2 * sub8 + 1, wide8, 0.0), axis=1, keepdims=True)
        cs[...] = jnp.where(lane8 < HEAD, even, odd)
        hst[0] = gstate[2] + chain[2:3] * (gstate[1] + chain[1:2] * gstate[0])

        def to_blocks(state, out):
            for r in range(8):
                for h in range(2):
                    for q in range(2):
                        first = HALF * h + 256 * q
                        out[q, 2 * r + h] = state[16 * r : 16 * r + 16, first : first + 256].astype(bf16)

        def from_blocks(source, put):
            for q in range(2):
                for r in range(8):
                    for h in range(2):
                        first = HALF * h + 256 * q
                        put(slice(16 * r, 16 * r + 16), slice(first, first + 256), source[q, 2 * r + h].astype(f32))

        to_blocks(hst[0], hs)

        @pl.when(step == 0)
        def _():
            pl.semaphore_wait(barrier, 127)
            ag_start()

        exchange_start(hs, hr, 0, 0)
        spread_start(cs, cr, 1)
        exchange_start(hs, hr, 0, 1)

        @pl.when(step == 0)
        def _():
            loads[9].wait()
            red[...] = jnp.where((rrow >> 6) == (rcol & 15), 1.0, 0.0).astype(bf16)

            def once(c, carry):
                z_f = z_ref[rows(c)].astype(f32)
                act[rows(c)] = z_f / (1.0 + jnp.exp(-z_f))
                scores = dot_nt(bc_ref[rows(c), STATE:], bc_ref[rows(c), :STATE])
                sc[c] = jnp.where((fcol[c] == fcol[c].T) & (ti >= tj), scores, 0.0)
                return carry

            lax.fori_loop(0, CHUNKS, once, 0)
            loads[10].wait()

        skip_e = expand(jnp.broadcast_to(skip_t, (8, 128)))[0:1]
        gain_e = gain[...]

        def inside(c, carry):
            s = dec_s[rows(c)]
            s_t = s.T
            scores = sc[c]
            xw[rows(c)] = (x_ref[rows(c)].astype(f32) * expand(wid[rows(c)])).astype(bf16)
            eexp[rows(c)] = expand(ent[rows(c)])
            for p in range(PAIRS):
                parts = []
                for h in (2 * p, 2 * p + 1):
                    gap = jnp.minimum(s[:, h : h + 1] - s_t[h : h + 1, :], 0.0)
                    parts.append((jnp.exp(gap) * scores).astype(bf16))
                mine = xw[rows(c), 128 * p : 128 * (p + 1)]
                both = jnp.concatenate([mine * low_half, mine * high_half], axis=0)
                lanes = slice(128 * p, 128 * (p + 1))
                direct = skip_e[:, lanes] * x_ref[rows(c), lanes].astype(f32)
                yin[rows(c), lanes] = dot(jnp.concatenate(parts, axis=1), both) + direct
            return carry

        lax.fori_loop(0, CHUNKS, inside, 0)
        ag_line()

        half = seq % 2

        def scan(source, out, h, order):
            state = [jnp.zeros((16, 128), f32) for _ in range(2)]
            for i in order:
                for m in range(2):
                    lanes = slice(128 * m, 128 * (m + 1))
                    out[h, i, :, lanes] = state[m].astype(bf16)
                    factor = cr[i, pl.ds(4 * half + 2 * h + m, 1), :]
                    state[m] = factor * state[m] + source[h, i, :, lanes].astype(f32)

        recv_wait(cr, 1, 15)
        for h in range(2):
            recv_wait(hr.at[h], 0, 15, h)
            scan(hr, hp, h, range(N_SEQ))
            exchange_start(hp, hi, 2, h)
        ag_finish()
        for h in range(2):
            recv_wait(hi.at[h], 2, 15, h)

        def put_state(at_rows, lanes, value):
            hst[0, at_rows, lanes] = value

        from_blocks(hi, put_state)

        scale = 2.0 / (WIDE * total_f)

        for c in range(CHUNKS):
            span = slice(c * CHUNK, (c + 1) * CHUNK)
            state = hst[c]
            y = yin[span] + eexp[span] * dot(bc_ref[span, STATE:], state.astype(bf16))
            yin[span] = y
            gated = y * act[span]
            gat[span] = gated
            inv = lax.rsqrt(jnp.sum(gated * gated, axis=1, keepdims=True) * (1.0 / WIDE) + norm_floor)
            invs[span] = jnp.broadcast_to(inv, (CHUNK, 128))
            normb[span] = (gated * gain_e * inv).astype(bf16)
            hst[c + 1] = chain[c : c + 1] * state + gstate[c]
        block = 512
        position = seq * TOK + iota((TOK, block), 0)
        scored = jnp.where(position < own_count, 1.0, 0.0)
        losses_8 = jnp.zeros((8, block), f32)
        for first in range(0, WIDE, block):
            lanes = slice(first, first + block)
            res = (dot(normb[...], wfull[:, lanes]) - tgt_ref[:, lanes].astype(f32)) * scored
            losses_8 = losses_8 + jnp.sum((res * res).reshape(TOK // 8, 8, block), axis=0)
            ogb[:, lanes] = (res * scale).astype(bf16)
        loss = jnp.sum(jnp.sum(losses_8, axis=1, keepdims=True), axis=0, keepdims=True)
        inner_l = jnp.zeros((TOK, 128), f32)
        for first in range(0, WIDE, block):
            lanes = slice(first, first + block)
            d_norm = dot_nt(ogb[...], wfull[lanes, :])
            dnf[:, lanes] = d_norm
            d_gain = d_norm * gain_e[:, lanes]
            gdn[:, lanes] = d_gain
            term = d_gain * gat[:, lanes]
            for k in range(0, block, 128):
                inner_l = inner_l + term[:, k : k + 128]
        inner = jnp.sum(inner_l, axis=1, keepdims=True) * (1.0 / WIDE)
        for c in range(CHUNKS):
            span = slice(c * CHUNK, (c + 1) * CHUNK)
            inv = invs[span, 0:1]
            g = (gdn[span] - gat[span] * (inv * inv * inner[span])) * inv * act[span]
            gb[span] = g.astype(bf16)
            apart[c] = dot_tn(bc_ref[span, STATE:], (g * eexp[span]).astype(bf16))
        entry = apart[0] + chain[0:1] * (apart[1] + chain[1:2] * apart[2])
        to_blocks(entry, gs)
        for h in range(2):
            exchange_start(gs, gr, 3, h)
        def grad_rows(first, second):
            lanes = [normb[:, pl.ds(pl.multiple_of(d * 128, 128), 128)] for d in (first, second)]
            both = dot_tn(jnp.concatenate(lanes, axis=1), ogb[...])
            return blocks_of(both[:128]), blocks_of(both[128:])

        def group(k, c):
            return ((yy + k) % N_Y) * 2 + c

        for pair in ((1, 2), (3, 0)):
            pieces = grad_rows(*[group(k, 1 - core) for k in pair])
            for k, piece in zip(pair, pieces):
                wgp[k] = piece.astype(bf16)
                remote(wgp.at[k], pr.at[k], s_ps.at[k], s_pr.at[k], partner, seq).start()
        for pair in ((1, 2), (3, 0)):
            pieces = grad_rows(*[group(k, core) for k in pair])
            for k, mine in zip(pair, pieces):
                y_k = (yy + k) % N_Y
                remote(wgp.at[k], pr.at[k], s_ps.at[k], s_pr.at[k], partner, seq).wait_recv()
                both = (mine + pr[k].astype(f32)).astype(bf16)
                part["sby"][pl.ds(y_k * 16, 16)] = both[:, :, : WIDTH["y"]]
                if k > 0:
                    slab = part["sby"].at[pl.ds(y_k * 16, 16)]
                    remote(slab, part["ray"].at[k - 1], r1s.at[0], r1r.at[0], y_k * 2 + core, seq).start()
                for p in "xz":
                    piece = both[:, :, FIRST[p] : FIRST[p] + WIDTH[p]]
                    for x in range(4):
                        if p == "x":
                            part["sbx"][pl.ds(x * 16 + y_k * 4, 4)] = piece[4 * x : 4 * x + 4]
                        else:
                            for z in range(4):
                                part["sbz"][z * 16 + x * 4 + y_k] = piece[4 * x + z]
        for n, p in ((1, "x"), (2, "z")):
            for k in range(1, 4):
                d, s, c = line_peer(p, k)
                slab = part["sb" + p].at[pl.ds(c * 16, 16)]
                remote(slab, part["ra" + p].at[k - 1], r1s.at[n], r1r.at[n], d, s).start()

        accs[...] = jnp.zeros(accs.shape, f32)

        def small_sums(c, carry):
            x_f, inv = x_ref[rows(c)].astype(f32), invs[rows(c), 0:1]
            accs[0] += jnp.sum((dnf[rows(c)] * gat[rows(c)] * inv).reshape(16, 8, WIDE), axis=0)
            accs[1] += jnp.sum((gb[rows(c)].astype(f32) * x_f).reshape(16, 8, WIDE), axis=0)
            return carry

        lax.fori_loop(0, CHUNKS, small_sums, 0)
        gain_g = jnp.sum(accs[0], axis=0, keepdims=True)
        for r in range(8):
            sa[r : r + 1, :] = gain_g[:, 128 * r : 128 * (r + 1)]
        skip_g = head_sum(jnp.broadcast_to(jnp.sum(accs[1], axis=0, keepdims=True), (8, WIDE)))
        sub = iota((8, 128), 0)
        sa[8:16, :] = jnp.where(sub == 0, skip_g, jnp.where(sub == 1, jnp.broadcast_to(loss, (8, 128)), 0.0))
        spread_start(sa, sar, 4)

        def scatter_plane():
            for p in "xzy":
                n = PARTS.index(p)
                got, mid, dst = part["ra" + p], part["mid" + p], part["rb" + p]
                remote(got, got, r1s.at[n], r1r.at[n], partner, seq).wait_recv()
                value = part["sb" + p][pl.ds(place[p] * 16, 16)].astype(f32)
                for k in range(3):
                    value = value + got[k].astype(f32)
                mid[...] = value.astype(bf16)
                here = mine_in[p] % 16
                for a, b in plane_far:
                    d, s, q = plane_peer(p, a, b)
                    remote(mid.at[q], dst.at[here], r2s.at[n], r2r.at[n], d, s).start()
                dst[here] = mid[here]

        def inside_back(c, carry):
            s = dec_s[rows(c)]
            s_t = s.T
            scores = sc[c].T
            for p in range(PAIRS):
                parts = []
                for h in (2 * p, 2 * p + 1):
                    gap = jnp.minimum(s_t[h : h + 1, :] - s[:, h : h + 1], 0.0)
                    parts.append((jnp.exp(gap) * scores).astype(bf16))
                mine = gb[rows(c), 128 * p : 128 * (p + 1)]
                both = jnp.concatenate([mine * low_half, mine * high_half], axis=0)
                lanes = slice(128 * p, 128 * (p + 1))
                eexp[rows(c), lanes] = dot(jnp.concatenate(parts, axis=1), both)
            g_f, x_f = gb[rows(c)].astype(f32), x_ref[rows(c)].astype(f32)
            ds1[rows(c)] = head_sum(g_f * (yin[rows(c)] - skip_e * x_f))
            q2a[rows(c)] = head_sum(xw[rows(c)].astype(f32) * eexp[rows(c)])
            return carry

        lax.fori_loop(0, CHUNKS - 1, inside_back, 0)

        for h in range(2):
            recv_wait(gr.at[h], 3, 15, h)
            scan(gr, gp, h, range(N_SEQ - 1, -1, -1))
            exchange_start(gp, gi, 5, h)
        lax.fori_loop(CHUNKS - 1, CHUNKS, inside_back, 0)

        scatter_plane()

        def summed(ref, count):
            value = ref[0]
            for k in range(1, count):
                value = value + ref[k]
            return value

        recv_wait(sar, 4, 15)
        sb2[...] = summed(sar, N_SEQ)
        cross_start(sb2, sbr, 6)

        for h in range(2):
            recv_wait(gi.at[h], 5, 15, h)

        def put_after(at_rows, lanes, value):
            apart[3, at_rows, lanes] = value

        from_blocks(gi, put_after)
        apart[2] = apart[2] + chain[2:3] * apart[3]
        apart[1] = apart[1] + chain[1:2] * apart[2]

        dec_g = bias_g = jnp.zeros((1, 128), f32)
        sig = 1.0 / (1.0 + jnp.exp(-(rawt[...] + bias_t)))
        for c in range(CHUNKS):
            span = slice(c * CHUNK, (c + 1) * CHUNK)
            after = apart[c + 1]
            width = wid[span]
            z_t = dot(bc_ref[span, :STATE], after.astype(bf16))
            q2 = q2a[span] + head_sum(wtd[span].astype(f32) * z_t)
            ends = jnp.sum((after * hst[c + 1]).reshape(16, 8, WIDE), axis=0)
            end_h = jnp.sum(head_sum(ends), axis=0, keepdims=True)
            d_a = lax.dot_general(
                tri[...], ds1[span] - q2, (((0,), (0,)), ((), ())), precision=highest, preferred_element_type=f32
            ) + end_h
            d_w = q2 / width - rate * d_a
            dec_g = dec_g - jnp.sum(d_a * (rate * width), axis=0, keepdims=True)
            bias_g = bias_g + jnp.sum(d_w * sig[span], axis=0, keepdims=True)

        recv_wait(sbr, 6, 7)
        sums_a = summed(sbr, N_DP)

        ag_sent()

        grad, square = {}, jnp.zeros((1, 1), f32)
        for n, p in enumerate(PARTS):
            dst = part["rb" + p]
            got = dst.at[pl.ds(0, 15)]
            remote(got, got, r2s.at[n], r2r.at[n], partner, seq).wait_recv()
            value = dst[0].astype(f32)
            for q in range(1, 16):
                value = value + dst[q].astype(f32)
            grad[p] = value
            square = square + jnp.sum(jnp.sum(value * value, axis=1, keepdims=True), axis=0, keepdims=True)
        t1[...] = jnp.where(lane < 16, dec_g, jnp.where(lane < 32, bias_g, jnp.where(lane == 32, square, 0.0)))
        for d, q in everyone:
            remote(t1, t2r.at[own_b], s_send.at[8, 0], s_recv.at[8, 0], d, q).start()
        t2r[own_b] = t1[...]
        recv_wait(t2r, 8, 127)
        sums_b = jnp.sum(t2r[...], axis=0)

        picked = jnp.where(sub8 == (lane8 >> 4), jnp.broadcast_to(sums_b, (8, 128)), 0.0)
        heads = jnp.dot(picked, spread, precision=highest, preferred_element_type=f32)
        dec_g, bias_g = heads[0:1], heads[1:2]
        squares = jnp.sum(jnp.where(lane == 32, sums_b, 0.0), axis=1, keepdims=True)
        gain_rows, skip_g, loss_all = sums_a[0:8], sums_a[8:9], sums_a[9:10]
        small = jnp.sum(
            jnp.where(lane < HEADS, dec_g * dec_g + bias_g * bias_g + skip_g * skip_g, 0.0), axis=1, keepdims=True
        )
        gains = jnp.sum(jnp.sum(gain_rows * gain_rows, axis=1, keepdims=True), axis=0, keepdims=True)
        norm = jnp.sqrt(squares + (small + gains))
        move = learn_rate * (clip_limit / jnp.maximum(norm, clip_limit))
        par[0] = jnp.broadcast_to(dec_t - move * dec_g, (8, 128))
        par[1] = jnp.broadcast_to(bias_t - move * bias_g, (8, 128))
        par[2] = jnp.broadcast_to(skip_t - move * skip_g, (8, 128))
        for r in range(8):
            lanes = slice(128 * r, 128 * (r + 1))
            gain[:, lanes] = gain[:, lanes] - move * gain_rows[r : r + 1]
        for p in PARTS:
            for h in range(2):
                lanes = slice(HALF * h + FIRST[p], HALF * h + FIRST[p] + WIDTH[p])
                wown[:, lanes] = wown[:, lanes] - move * grad[p][8 * h : 8 * h + 8]

        for h in range(2):
            send_wait(hr.at[h], 0, 15, h)
        send_wait(cr, 1, 15)
        for h in range(2):
            send_wait(hi.at[h], 2, 15, h)
        for h in range(2):
            send_wait(gr.at[h], 3, 15, h)
        send_wait(sar, 4, 15)
        for h in range(2):
            send_wait(gi.at[h], 5, 15, h)
        send_wait(sbr, 6, 7)
        send_wait(t2r, 8, 127)
        for k in range(N_Y):
            remote(wgp.at[k], pr.at[k], s_ps.at[k], s_pr.at[k], partner, seq).wait_send()
        for n, p in enumerate(PARTS):
            got, dst = part["ra" + p], part["rb" + p].at[pl.ds(0, 15)]
            remote(got, got, r1s.at[n], r1r.at[n], partner, seq).wait_send()
            remote(dst, dst, r2s.at[n], r2r.at[n], partner, seq).wait_send()

        @pl.when(step == 0)
        def _():
            ag_start()

        step_loss = loss_all[:, 0:1] * (1.0 / WIDE) / total_f
        return jnp.where(iota((1, STEPS), 1) == step, step_loss, losses)

    losses = lax.fori_loop(0, STEPS, one_step, jnp.zeros((1, STEPS), f32))
    packed_out[0:8] = wown[...]
    packed_out[8:9] = gain[...]
    packed_out[9:10, :] = jnp.zeros((1, WIDE), f32)
    for n in range(3):
        packed_out[9:10, 128 * n : 128 * (n + 1)] = par[n, 0:1]
    packed_out[9:10, 384 : 384 + STEPS] = losses


def split_kernel(packed, loss_out, w_out, dec_out, bias_out, skip_out, gain_out):
    w_out[...] = packed[0:8]
    gain_out[...] = packed[8:9]
    dec_out[...] = packed[9:10, 0:HEADS]
    bias_out[...] = packed[9:10, 128 : 128 + HEADS]
    skip_out[...] = packed[9:10, 256 : 256 + HEADS]
    loss_out[...] = packed[9:10, 384 : 384 + STEPS]


def per_device(x, z, bc, raw, ids, counts, target, weight, dec, bias, skip, gain):
    vmem = pl.BlockSpec(memory_space=pltpu.VMEM)
    in_hbm = pl.BlockSpec(memory_space=pltpu.HBM)
    shape = jax.ShapeDtypeStruct
    packed = pl.pallas_call(
        kernel,
        out_shape=shape((16, WIDE), f32),
        in_specs=[in_hbm] * 12,
        out_specs=vmem,
        scratch_shapes=list(scratch().values()),
        compiler_params=pltpu.CompilerParams(
            collective_id=0, has_side_effects=True, vmem_limit_bytes=62 * 1024 * 1024
        ),
    )(
        x[0], z[0], bc[0], raw[0].T, ids, counts, target[0], weight,
        dec.reshape(1, HEADS), bias.reshape(1, HEADS), skip.reshape(1, HEADS), gain.reshape(1, WIDE),
    )
    losses, weight, dec, bias, skip, gain = pl.pallas_call(
        split_kernel,
        out_shape=(
            shape((1, STEPS), f32), shape((8, WIDE), f32), shape((1, HEADS), f32), shape((1, HEADS), f32),
            shape((1, HEADS), f32), shape((1, WIDE), f32),
        ),
        in_specs=[vmem],
        out_specs=(vmem,) * 6,
    )(packed)
    return (
        losses.reshape(STEPS), weight, dec.reshape(HEADS), bias.reshape(HEADS), skip.reshape(HEADS), gain.reshape(WIDE)
    )


def solution(mesh):
    tokens = P(DP, SEQ, None)
    return jax.shard_map(
        per_device,
        mesh=mesh,
        in_specs=(
            tokens, tokens, tokens, tokens, P(DP, SEQ), P(), tokens, P((DP, SEQ), None), P(), P(), P(), P(),
        ),
        out_specs=(P(), P((DP, SEQ), None), P(), P(), P(), P()),
        check_vma=False,
    )
```
